128 devices in a mesh: row: 16 (over x_hi, y, core), col: 4 (over z), dp: 2 (over x_lo).
Axes of the slice: x: 4 (x_hi: 2, x_lo: 2; x = x_hi * 2 + x_lo), y: 4, z: 4, core: 2. Of those that a mesh axis runs over, the one named last changes fastest.
Arguments:
- slides: bfloat16 [2, 256, 128, 512], P('dp', 'row', 'col'), may hold values from -6 to 6
- cotangent: bfloat16 [2, 256, 128, 512], P('dp', 'row', 'col'), may hold values from -6 to 6
- kernel: float32 [2, 7, 7, 512], replicated, may hold values from -0.875 to 0.875
- kernel_bias: float32 [2, 512], replicated, may hold values from -3 to 3
- norm_gain: float32 [2, 512], replicated, may hold values from 0.1 to 1.9
- norm_bias: float32 [2, 512], replicated, may hold values from -3 to 3
- weight_in: bfloat16 [2, 512, 2048], P(None, 'dp'), may hold values from -0.25 to 0.25
- bias_in: float32 [2, 2048], replicated, may hold values from -3 to 3
- weight_out: bfloat16 [2, 2048, 512], P(None, None, 'dp'), may hold values from -0.125 to 0.125
- bias_out: float32 [2, 512], replicated, may hold values from -3 to 3
- layer_scale: float32 [2, 512], replicated, may hold values from 0.3 to 1.5
Outputs:
- output: bfloat16 [2, 256, 128, 512], P('dp', 'row', 'col')
- grad_slides: bfloat16 [2, 256, 128, 512], P('dp', 'row', 'col')
- grad_weight_in: float32 [2, 512, 2048], P(None, 'dp')
- grad_weight_out: float32 [2, 2048, 512], P(None, None, 'dp')
- grad_kernel: float32 [2, 7, 7, 512], replicated
- grad_channel: float32 [2, 5, 512], replicated
- grad_bias_in: float32 [2, 2048], replicated
The draws below stay inside these ranges and needn't reach their ends.
All inputs are finite; a program needn't handle non-finite values.
Results may differ from the reference program's by a relative error of at most 0.01.
Values may be sent and summed in bfloat16 or wider, within the bound.
No kernel may reach another device: no remote copies, remote signals or barrier semaphores. Data moves between devices by JAX's collectives and lax.ppermute only.
A program may use at most 128 MiB of HBM per device.

```python
import math
import jax
import jax.numpy as jnp
from jax import lax

D = 512
FF = 2048
LAYERS = 2
SLIDES = 2
HEIGHT = 256
WIDTH = 128


def shard_levels(rng, shape, pieces, smallest, high):
    def one(position, blocks):
        steps = jax.random.uniform(jax.random.fold_in(jax.random.fold_in(rng, 6), position), (blocks,), jnp.float32, smallest / len(pieces), high / len(pieces))
        return jnp.repeat(jnp.exp(steps), shape[position] // blocks).reshape((-1,) + (1,) * (len(shape) - position - 1))

    loudness = one(*pieces[0])
    for cut in pieces[1:]:
        loudness = loudness * one(*cut)
    return loudness


def normal_values(key, dims, spread, reach, cuts=(), held_as=jnp.bfloat16):
    factor_of = shard_levels(key, dims, cuts, -0.22, 0.18) if cuts else 1.0
    entries = jax.random.normal(key, dims, jnp.float32) * spread * factor_of
    return jnp.minimum(jnp.maximum(entries, -reach), reach).astype(held_as)


def setup_inputs(seed: int = 0) -> dict:
    key_list = jax.random.split(jax.random.key(seed), 12)
    slides = normal_values(key_list[0], (SLIDES, HEIGHT, WIDTH, D), 1.0, 6.0, ((0, 2), (1, 16), (2, 4)))
    cotangent = normal_values(key_list[1], (SLIDES, HEIGHT, WIDTH, D), 1.0, 6.0, ((0, 2), (1, 16), (2, 4)))
    kernel = normal_values(key_list[2], (LAYERS, 7, 7, D), 49 ** -0.5, 0.875, (), jnp.float32)
    kernel_bias = normal_values(key_list[3], (LAYERS, D), 0.5, 3.0, (), jnp.float32)
    norm_gain = jnp.clip(1.0 + 0.18 * jax.random.normal(key_list[4], (LAYERS, D), jnp.float32), 0.1, 1.9)
    norm_bias = normal_values(key_list[5], (LAYERS, D), 0.5, 3.0, (), jnp.float32)
    weight_in = normal_values(key_list[6], (LAYERS, D, FF), D ** -0.5, 0.25, ((1, 2),))
    bias_in = normal_values(key_list[7], (LAYERS, FF), 0.5, 3.0, (), jnp.float32)
    weight_out = normal_values(key_list[8], (LAYERS, FF, D), FF ** -0.5, 0.125, ((2, 2),))
    bias_out = normal_values(key_list[9], (LAYERS, D), 0.5, 3.0, (), jnp.float32)
    layer_scale = jnp.clip(jnp.exp(jax.random.uniform(key_list[10], (LAYERS, D), jnp.float32, math.log(0.3), math.log(1.5))), 0.3, 1.5)
    return dict(slides=slides, cotangent=cotangent, kernel=kernel, kernel_bias=kernel_bias, norm_gain=norm_gain, norm_bias=norm_bias, weight_in=weight_in, bias_in=bias_in, weight_out=weight_out, bias_out=bias_out, layer_scale=layer_scale)


COEF = 0.7978845608028654
CUBIC = 0.044715
EPSILON = 1e-06

def gelu_tanh(values):
    inner = COEF * (values + CUBIC * values * values * values)
    return 0.5 * values * (1.0 + jnp.tanh(inner))

def gelu_slope(values):
    tangent = jnp.tanh(COEF * (values + CUBIC * values * values * values))
    return 0.5 * (1.0 + tangent) + 0.5 * values * (1.0 - tangent * tangent) * COEF * (1.0 + 3.0 * CUBIC * values * values)

def depthwise(padded, taps):
    height = padded.shape[1] - 6
    width = padded.shape[2] - 6
    total = jnp.zeros((padded.shape[0], height, width, padded.shape[3]), jnp.float32)
    for row_tap in range(7):
        for col_tap in range(7):
            window = padded[:, row_tap:row_tap + height, col_tap:col_tap + width, :].astype(jnp.float32)
            total = total + window * taps[row_tap, col_tap]
    return total

def tap_grads(padded, upstream):
    height = upstream.shape[1]
    width = upstream.shape[2]
    rows_out = []
    for row_tap in range(7):
        line = []
        for col_tap in range(7):
            window = padded[:, row_tap:row_tap + height, col_tap:col_tap + width, :].astype(jnp.float32)
            line.append(lax.optimization_barrier(jnp.sum(window * upstream, axis=(0, 1, 2))))
        rows_out.append(jnp.stack(line))
    return jnp.stack(rows_out)

def forward_layer(padded, current, taps, tap_bias, gain, shift, weight_in, bias_in, weight_out, bias_out, scale):
    channels = current.shape[-1]
    mixed = (depthwise(padded, taps) + tap_bias).reshape(-1, channels)
    center = mixed - lax.optimization_barrier(jnp.mean(mixed, -1, keepdims=True))
    rstd = lax.rsqrt(lax.optimization_barrier(jnp.mean(center * center, -1, keepdims=True)) + EPSILON)
    normed = center * rstd
    normal_low = (normed * gain + shift).astype(jnp.bfloat16)
    hidden = jnp.dot(normal_low, weight_in, preferred_element_type=jnp.float32) + bias_in
    activated = gelu_tanh(hidden).astype(jnp.bfloat16)
    branch = jnp.dot(activated, weight_out, preferred_element_type=jnp.float32) + bias_out
    result = current.reshape(-1, channels).astype(jnp.float32) + scale * branch
    result = result.astype(jnp.bfloat16).reshape(current.shape)
    return (result, (normed, rstd, normal_low, hidden, activated, branch))

def backward_layer(upstream, saved, gain, weight_in, weight_out, scale):
    normed, rstd, normal_low, hidden, activated, branch = saved
    contract_rows = (((0,), (0,)), ((), ()))
    contract_cols = (((1,), (1,)), ((), ()))
    grad_scale = lax.optimization_barrier(jnp.sum(upstream * branch, 0))
    grad_branch = upstream * scale
    grad_bias_out = lax.optimization_barrier(jnp.sum(grad_branch, 0))
    branch_low = grad_branch.astype(jnp.bfloat16)
    grad_weight_out = lax.dot_general(activated, branch_low, contract_rows, preferred_element_type=jnp.float32)
    grad_act = lax.dot_general(branch_low, weight_out, contract_cols, preferred_element_type=jnp.float32)
    grad_hidden = grad_act * gelu_slope(hidden)
    grad_bias_in = lax.optimization_barrier(jnp.sum(grad_hidden, 0))
    hidden_low = grad_hidden.astype(jnp.bfloat16)
    grad_weight_in = lax.dot_general(normal_low, hidden_low, contract_rows, preferred_element_type=jnp.float32)
    grad_normal = lax.dot_general(hidden_low, weight_in, contract_cols, preferred_element_type=jnp.float32)
    grad_gain = lax.optimization_barrier(jnp.sum(grad_normal * normed, 0))
    grad_shift = lax.optimization_barrier(jnp.sum(grad_normal, 0))
    scaled = grad_normal * gain
    grad_mixed = rstd * (scaled - lax.optimization_barrier(jnp.mean(scaled, -1, keepdims=True)) - normed * lax.optimization_barrier(jnp.mean(scaled * normed, -1, keepdims=True)))
    grad_tap_bias = lax.optimization_barrier(jnp.sum(grad_mixed, 0))
    channel_grads = jnp.stack([grad_tap_bias, grad_gain, grad_shift, grad_bias_out, grad_scale])
    return (grad_mixed, grad_weight_in, grad_weight_out, grad_bias_in, channel_grads)

def pad_map(values):
    return jnp.pad(values, ((0, 0), (3, 3), (3, 3), (0, 0)))

def reference(slides, cotangent, kernel, kernel_bias, norm_gain, norm_bias, weight_in, bias_in, weight_out, bias_out, layer_scale):
    layers = weight_in.shape[0]
    channels = slides.shape[-1]
    current = slides
    caches = []
    paddings = []
    for which in range(layers):
        padded = pad_map(current)
        current, cache = forward_layer(padded, current, kernel[which], kernel_bias[which], norm_gain[which], norm_bias[which], weight_in[which], bias_in[which], weight_out[which], bias_out[which], layer_scale[which])
        caches.append(cache)
        paddings.append(padded)
    output = current
    upstream = cotangent.astype(jnp.float32).reshape(-1, channels)
    grads_in = [None] * layers
    grads_out = [None] * layers
    grads_kernel = [None] * layers
    grads_channel = [None] * layers
    grads_bias = [None] * layers
    for which in reversed(range(layers)):
        grad_mixed, grad_in, grad_out, grad_bias, channel_grads = backward_layer(upstream, caches[which], norm_gain[which], weight_in[which], weight_out[which], layer_scale[which])
        shaped = grad_mixed.reshape(slides.shape)
        grads_kernel[which] = tap_grads(paddings[which], shaped)
        back = depthwise(pad_map(shaped), kernel[which][::-1, ::-1])
        upstream = upstream + back.reshape(-1, channels)
        grads_in[which] = grad_in
        grads_out[which] = grad_out
        grads_channel[which] = channel_grads
        grads_bias[which] = grad_bias
    grad_slides = upstream.astype(jnp.bfloat16).reshape(slides.shape)
    return (output, grad_slides, jnp.stack(grads_in), jnp.stack(grads_out), jnp.stack(grads_kernel), jnp.stack(grads_channel), jnp.stack(grads_bias))
```

```python
import jax
import jax.numpy as jnp
from jax import lax
from jax.sharding import PartitionSpec as P

COEF = 0.7978845608028654
CUBIC = 0.044715
EPSILON = 1e-06


SPACE = ("xh", "y", "z")
HALF = 1024


def chips_along_x(step):
    def target(pos):
        x = (pos + step) % 4
        return x

    return [(pos, target(pos)) for pos in range(4)]


def swapped(value, axis):
    return lax.ppermute(value, axis, [(0, 1), (1, 0)])


def fetch_weights(own_in, own_out):
    core = lax.axis_index("core")
    part = lax.axis_index("dp")
    send_in = lax.dynamic_slice_in_dim(own_in, core * 128, 128, 0)
    send_out = lax.dynamic_slice_in_dim(own_out, core * 1024, 1024, 0)
    got_in = lax.ppermute(send_in, ("xh", "dp"), chips_along_x(1))
    got_out = lax.ppermute(send_out, ("xh", "dp"), chips_along_x(-1))
    mate_in = swapped(got_in, "core")
    mate_out = swapped(got_out, "core")
    first = core == 0
    other_in = jnp.concatenate(
        [jnp.where(first, got_in, mate_in), jnp.where(first, mate_in, got_in)], 0
    )
    other_out = jnp.concatenate(
        [jnp.where(first, got_out, mate_out), jnp.where(first, mate_out, got_out)], 0
    )
    low = part == 0
    full_in = jnp.concatenate(
        [jnp.where(low, own_in, other_in), jnp.where(low, other_in, own_in)], 0
    )
    full_out = jnp.concatenate(
        [jnp.where(low, own_out, other_out), jnp.where(low, other_out, own_out)], 1
    )
    return full_in, full_out


def with_halo(block, sides, width):
    for axis, dim in sides:
        count = lax.axis_size(axis)
        forward = [(i, i + 1) for i in range(count - 1)]
        backward = [(target, source) for source, target in forward]
        low = lax.ppermute(
            lax.slice_in_dim(block, block.shape[dim] - width, None, axis=dim), axis, forward
        )
        high = lax.ppermute(lax.slice_in_dim(block, 0, width, axis=dim), axis, backward)
        block = jnp.concatenate([low, block, high], axis=dim)
    return block


def gelu_tanh(values):
    inner = COEF * (values + CUBIC * values * values * values)
    return 0.5 * values * (1.0 + jnp.tanh(inner))


def gelu_slope(values):
    tangent = jnp.tanh(COEF * (values + CUBIC * values * values * values))
    return 0.5 * (1.0 + tangent) + 0.5 * values * (1.0 - tangent * tangent) * COEF * (
        1.0 + 3.0 * CUBIC * values * values
    )


def depthwise(padded, taps):
    height = padded.shape[1] - 6
    width = padded.shape[2] - 6
    total = jnp.zeros((padded.shape[0], height, width, padded.shape[3]), jnp.float32)
    for row_tap in range(7):
        for col_tap in range(7):
            window = padded[:, row_tap : row_tap + height, col_tap : col_tap + width, :].astype(
                jnp.float32
            )
            total = total + window * taps[row_tap, col_tap]
    return total


def tap_grads(padded, upstream):
    height = upstream.shape[1]
    width = upstream.shape[2]
    rows_out = []
    for row_tap in range(7):
        line = []
        for col_tap in range(7):
            window = padded[:, row_tap : row_tap + height, col_tap : col_tap + width, :].astype(
                jnp.float32
            )
            line.append(jnp.sum(window * upstream, axis=(0, 1, 2)))
        rows_out.append(jnp.stack(line))
    return jnp.stack(rows_out)


def forward_layer(
    padded, current, taps, tap_bias, gain, shift, weight_in, bias_in, weight_out, bias_out, scale
):
    channels = current.shape[-1]
    mixed = (depthwise(padded, taps) + tap_bias).reshape(-1, channels)
    center = mixed - jnp.mean(mixed, -1, keepdims=True)
    rstd = lax.rsqrt(jnp.mean(center * center, -1, keepdims=True) + EPSILON)
    normed = center * rstd
    normal_low = (normed * gain + shift).astype(jnp.bfloat16)
    hidden = jnp.dot(normal_low, weight_in, preferred_element_type=jnp.float32) + bias_in
    activated = gelu_tanh(hidden).astype(jnp.bfloat16)
    branch = jnp.dot(activated, weight_out, preferred_element_type=jnp.float32) + bias_out
    result = current.reshape(-1, channels).astype(jnp.float32) + scale * branch
    result = result.astype(jnp.bfloat16).reshape(current.shape)
    return (result, (normed, rstd, normal_low, hidden, activated, branch))


def backward_layer(upstream, saved, gain, weight_in, weight_out, scale):
    normed, rstd, normal_low, hidden, activated, branch = saved
    contract_rows = (((0,), (0,)), ((), ()))
    contract_cols = (((1,), (1,)), ((), ()))
    grad_scale = jnp.sum(upstream * branch, 0)
    grad_branch = upstream * scale
    grad_bias_out = jnp.sum(grad_branch, 0)
    branch_low = grad_branch.astype(jnp.bfloat16)
    grad_weight_out = lax.dot_general(
        branch_low, activated, contract_rows, preferred_element_type=jnp.float32
    )
    grad_act = lax.dot_general(
        branch_low, weight_out, contract_cols, preferred_element_type=jnp.float32
    )
    grad_hidden = grad_act * gelu_slope(hidden)
    grad_bias_in = jnp.sum(grad_hidden, 0)
    hidden_low = grad_hidden.astype(jnp.bfloat16)
    grad_weight_in = lax.dot_general(
        normal_low, hidden_low, contract_rows, preferred_element_type=jnp.float32
    )
    grad_normal = lax.dot_general(
        hidden_low, weight_in, contract_cols, preferred_element_type=jnp.float32
    )
    grad_gain = jnp.sum(grad_normal * normed, 0)
    grad_shift = jnp.sum(grad_normal, 0)
    scaled = grad_normal * gain
    grad_mixed = rstd * (
        scaled
        - jnp.mean(scaled, -1, keepdims=True)
        - normed * jnp.mean(scaled * normed, -1, keepdims=True)
    )
    grad_tap_bias = jnp.sum(grad_mixed, 0)
    channel_grads = jnp.stack([grad_tap_bias, grad_gain, grad_shift, grad_bias_out, grad_scale])
    return (grad_mixed, grad_weight_in, grad_weight_out, grad_bias_in, channel_grads)


def reduce_weights(grad_in, grad_out):
    core = lax.axis_index("core")
    both = jnp.stack([grad_in, grad_out], 1).astype(jnp.bfloat16)
    keep = lax.dynamic_slice_in_dim(both, core * HALF, HALF, 2)
    give = lax.dynamic_slice_in_dim(both, (1 - core) * HALF, HALF, 2)
    pair = keep.astype(jnp.float32) + swapped(give, "core").astype(jnp.float32)
    pair = pair.astype(jnp.bfloat16).reshape(64, 8, 2, HALF)
    pieces = lax.all_to_all(pair, ("dp", *SPACE), 0, 0, tiled=True)
    mine = jnp.sum(pieces.astype(jnp.float32), 0).astype(jnp.bfloat16)
    copies = jnp.broadcast_to(mine, (32, *mine.shape))
    whole = lax.all_to_all(copies, SPACE, 0, 0, tiled=True).reshape(256, 2, HALF)
    mate = swapped(whole, "core")
    first = core == 0
    full = jnp.concatenate(
        [jnp.where(first, whole, mate), jnp.where(first, mate, whole)], 2
    ).astype(jnp.float32)
    return full[:, 0], full[:, 1].T


def reduce_small(parts):
    axes = ("xh", "y", "core", "z", "dp")
    lines = jnp.concatenate([p.reshape(-1) for p in parts])
    count = lines.shape[0]
    spare = -count % (128 * 128)
    lines = jnp.pad(lines, (0, spare)).astype(jnp.bfloat16).reshape(128, -1)
    pieces = lax.all_to_all(lines, axes, 0, 0, tiled=True)
    mine = jnp.sum(pieces.astype(jnp.float32), 0, keepdims=True)
    whole = lax.all_gather(mine, axes, axis=0, tiled=True).reshape(-1)
    outs = []
    start = 0
    for p in parts:
        outs.append(whole[start : start + p.size].reshape(p.shape))
        start += p.size
    return outs


def per_device(
    slides,
    cotangent,
    kernel,
    kernel_bias,
    norm_gain,
    norm_bias,
    weight_in,
    bias_in,
    weight_out,
    bias_out,
    layer_scale,
):
    layers = weight_in.shape[0]
    channels = slides.shape[-1]
    current = slides
    caches = []
    paddings = []
    fetched = []
    for which in range(layers):
        full_in, full_out = fetch_weights(weight_in[which], weight_out[which])
        fetched.append((full_in, full_out))
        padded = with_halo(current, ((("xh", "y", "core"), 1), ("z", 2)), 3)
        current, cache = forward_layer(
            padded,
            current,
            kernel[which],
            kernel_bias[which],
            norm_gain[which],
            norm_bias[which],
            full_in,
            bias_in[which],
            full_out,
            bias_out[which],
            layer_scale[which],
        )
        caches.append(cache)
        paddings.append(padded)
    upstream = cotangent.astype(jnp.float32).reshape(-1, channels)
    grads_in = [None] * layers
    grads_out = [None] * layers
    grads_kernel = [None] * layers
    grads_channel = [None] * layers
    grads_bias = [None] * layers
    for which in reversed(range(layers)):
        full_in, full_out = fetched[which]
        grad_mixed, grad_in, grad_out, grad_bias, channel_grads = backward_layer(
            upstream, caches[which], norm_gain[which], full_in, full_out, layer_scale[which]
        )
        shaped = grad_mixed.reshape(slides.shape)
        rim = with_halo(shaped.astype(jnp.bfloat16), ((("xh", "y", "core"), 1), ("z", 2)), 3).astype(
            shaped.dtype
        )
        local_taps = tap_grads(paddings[which], shaped)
        back = depthwise(rim, kernel[which][::-1, ::-1])
        upstream = upstream + back.reshape(-1, channels)
        grads_in[which], grads_out[which] = reduce_weights(grad_in, grad_out)
        grads_kernel[which], grads_channel[which], grads_bias[which] = (
            local_taps,
            channel_grads,
            grad_bias,
        )
    grad_slides = upstream.astype(jnp.bfloat16).reshape(slides.shape)
    small = reduce_small(
        [jnp.stack(grads_kernel), jnp.stack(grads_channel), jnp.stack(grads_bias)]
    )
    return (current, grad_slides, jnp.stack(grads_in), jnp.stack(grads_out), *small)


def solution(mesh):
    fine = jax.sharding.Mesh(
        mesh.devices.reshape(2, 4, 2, 4, 2), ("xh", "y", "core", "z", "dp")
    )
    rows = ("xh", "y", "core")
    return jax.shard_map(
        per_device,
        mesh=fine,
        in_specs=(
            P("dp", rows, "z", None),
            P("dp", rows, "z", None),
            P(),
            P(),
            P(),
            P(),
            P(None, "dp", None),
            P(),
            P(None, None, "dp"),
            P(),
            P(),
        ),
        out_specs=(
            P("dp", rows, "z", None),
            P("dp", rows, "z", None),
            P(None, "dp", None),
            P(None, None, "dp"),
            P(),
            P(),
            P(),
        ),
        check_vma=False,
    )
```

```python
import jax
import jax.numpy as jnp
from jax import lax
from jax.experimental import pallas as pl
from jax.experimental.pallas import tpu as pltpu
from jax.sharding import PartitionSpec as P

COEF = 0.7978845608028654
CUBIC = 0.044715
EPSILON = 1e-06

PIX = 512
CH = 512
FF = 2048
HALF = 1024
ROWS, COLS = 16, 32
WIDE = 40
DEEP = 14
SLAB = DEEP * WIDE * 8
SPACE = ("xh", "y", "z")
F32, BF16 = jnp.float32, jnp.bfloat16

VM = pl.BlockSpec(memory_space=pltpu.VMEM)
SM = pl.BlockSpec(memory_space=pltpu.SMEM)


def call(body, outs, count, flops, scratch=(), scalars=0):
    shapes = [jax.ShapeDtypeStruct(s, d) for s, d in outs]
    return pl.pallas_call(
        body,
        out_shape=shapes,
        in_specs=[SM] * scalars + [VM] * (count - scalars),
        out_specs=[VM] * len(outs),
        scratch_shapes=list(scratch),
        compiler_params=pltpu.CompilerParams(vmem_limit_bytes=56 * 1024 * 1024),
        cost_estimate=pl.CostEstimate(
            flops=flops, bytes_accessed=4_000_000, transcendentals=0
        ),
    )


def at(row, col):
    return (row * WIDE + col) * 8


def homes(row):
    found = []
    if row < DEEP:
        found.append((0, row))
    if row >= 8:
        found.append((1, row - 8))
    return found


def put_row(slab, row, line):
    for block, inner in homes(row):
        for group in range(4):
            slab[pl.ds(at(inner, 3) + block * 4 + group, COLS, stride=8), :] = line[
                :, group * 128 : (group + 1) * 128
            ]


def put_edges(slab, top, bottom):
    for k in range(3):
        put_row(slab, k, top[k * COLS : (k + 1) * COLS, :].astype(F32))
        put_row(slab, 19 + k, bottom[k * COLS : (k + 1) * COLS, :].astype(F32))


def put_columns(slab, left, right):
    for row in range(DEEP):
        a, b = row * 24, (row + 1) * 24
        slab[pl.ds(at(row, 0), 24), :] = left[a:b, :].astype(F32)
        slab[pl.ds(at(row, 35), 24), :] = right[a:b, :].astype(F32)


def take_columns(slab, to_low, to_high):
    for row in range(DEEP):
        a, b = row * 24, (row + 1) * 24
        to_low[a:b, :] = slab[pl.ds(at(row, 3), 24), :].astype(BF16)
        to_high[a:b, :] = slab[pl.ds(at(row, 32), 24), :].astype(BF16)


def filtered(slab, taps, store):
    def step(n, carry):
        row = n // 4
        col = (n % 4) * 8
        sums = [None] * 8
        for p in range(7):
            base = pl.multiple_of(((row + p) * WIDE + col) * 8, 8)
            seen = [slab[pl.ds(base + 8 * k, 8), :] for k in range(14)]
            for q in range(7):
                weight = taps[(p * 7 + q) * 8 : (p * 7 + q + 1) * 8, :]
                for m in range(8):
                    term = seen[m + q] * weight
                    sums[m] = term if sums[m] is None else sums[m] + term
        base = pl.multiple_of((row * COLS + col) * 8, 8)
        for m in range(8):
            store[pl.ds(base + 8 * m, 8), :] = sums[m]
        return carry

    lax.fori_loop(0, 32, step, 0)


def line_of(store, row):
    block, inner = row // 8, row % 8
    return jnp.concatenate(
        [
            store[pl.ds(inner * COLS * 8 + block * 4 + group, COLS, stride=8), :]
            for group in range(4)
        ],
        axis=1,
    )


def pack_body(x, top, bottom, slab, to_low, to_high):
    for row in range(ROWS):
        put_row(slab, row + 3, x[row * COLS : (row + 1) * COLS, :].astype(F32))
    put_edges(slab, top, bottom)
    take_columns(slab, to_low, to_high)


def edge_body(old, top, bottom, slab, to_low, to_high):
    slab[...] = old[...]
    put_edges(slab, top, bottom)
    take_columns(slab, to_low, to_high)


def norm_body(old, left, right, taps, bias, gain, shift, slab, normal, normed, rstd, store):
    slab[...] = old[...]
    put_columns(slab, left, right)
    filtered(slab, taps, store)
    for row in range(ROWS):
        a, b = row * COLS, (row + 1) * COLS
        mixed = line_of(store, row) + bias[...]
        center = mixed - jnp.mean(mixed, -1, keepdims=True)
        scale = lax.rsqrt(jnp.mean(center * center, -1, keepdims=True) + EPSILON)
        value = center * scale
        normed[a:b, :] = value
        rstd[a:b, :] = jnp.broadcast_to(scale, (COLS, 128))
        normal[a:b, :] = (value * gain[...] + shift[...]).astype(BF16)


def mlp_body(
    place, a, normal, own_in, got_in, mate_in, own_out, got_out, mate_out,
    bias_in, bias_out, scale,
    out, top, bottom, act, slope, branch, full_in, full_out,
):
    core, part = place[0], place[1]
    mine = pl.multiple_of(part * 256, 256)
    theirs = pl.multiple_of((1 - part) * 256, 256)
    full_in[pl.ds(mine, 256), :] = own_in[...]
    full_in[pl.ds(pl.multiple_of(theirs + core * 128, 128), 128), :] = got_in[...]
    full_in[pl.ds(pl.multiple_of(theirs + (1 - core) * 128, 128), 128), :] = mate_in[...]
    full_out[:, pl.ds(mine, 256)] = own_out[...]
    full_out[pl.ds(pl.multiple_of(core * HALF, HALF), HALF), pl.ds(theirs, 256)] = got_out[...]
    full_out[pl.ds(pl.multiple_of((1 - core) * HALF, HALF), HALF), pl.ds(theirs, 256)] = mate_out[...]
    for c in range(8):
        cols = slice(c * 256, (c + 1) * 256)
        hidden = jnp.dot(normal[...], full_in[:, cols], preferred_element_type=F32)
        v = hidden + bias_in[:, cols]
        square = v * v
        tangent = jnp.tanh(v * (COEF + (COEF * CUBIC) * square))
        half = 0.5 * v
        act[:, cols] = (half + half * tangent).astype(BF16)
        slope[:, cols] = (
            0.5
            + 0.5 * tangent
            + half * (1.0 - tangent * tangent) * (COEF + (3.0 * COEF * CUBIC) * square)
        ).astype(BF16)
    for c in range(2):
        cols = slice(c * 256, (c + 1) * 256)
        value = jnp.dot(act[...], full_out[:, cols], preferred_element_type=F32)
        value = value + bias_out[:, cols]
        branch[:, cols] = value
        result = (a[:, cols].astype(F32) + scale[:, cols] * value).astype(BF16)
        out[:, cols] = result
        top[:, cols] = result[:96, :]
        bottom[:, cols] = result[416:, :]


def back_body(
    place, u, branch, act, slope, normal, normed, rstd, full_in, full_out, gain, scale,
    keep, give, slab, top, bottom, channel, bias, low, gh, gn,
):
    core = place[0]
    rows_first = (((0,), (0,)), ((), ()))
    cols_last = (((1,), (1,)), ((), ()))
    up = u[...].astype(F32)
    channel[4:5, :] = jnp.sum(up * branch[...], 0, keepdims=True)
    gb = up * scale[...]
    channel[3:4, :] = jnp.sum(gb, 0, keepdims=True)
    low[...] = gb.astype(BF16)
    for c in range(8):
        cols = slice(c * 256, (c + 1) * 256)
        ga = lax.dot_general(
            low[...], full_out[cols, :], cols_last, preferred_element_type=F32
        )
        value = ga * slope[:, cols].astype(F32)
        bias[:, cols] = jnp.sum(value, 0, keepdims=True)
        gh[:, cols] = value.astype(BF16)
    for side, ref in ((core, keep), (1 - core, give)):
        for c in range(4):
            cols = pl.ds(pl.multiple_of(side * HALF + c * 256, 256), 256)
            ref[:, c * 256 : (c + 1) * 256] = lax.dot_general(
                normal[...], gh[:, cols], rows_first, preferred_element_type=F32
            ).astype(BF16)
            ref[:, HALF + c * 256 : HALF + (c + 1) * 256] = lax.dot_general(
                low[...], act[:, cols], rows_first, preferred_element_type=F32
            ).astype(BF16)
    for c in range(2):
        cols = slice(c * 256, (c + 1) * 256)
        gn[:, cols] = lax.dot_general(
            gh[...], full_in[cols, :], cols_last, preferred_element_type=F32
        )
    sums = [jnp.zeros((8, CH), F32) for _ in range(3)]

    def folded(value):
        return value[0:8] + value[8:16] + value[16:24] + value[24:32]

    for row in range(ROWS):
        a, b = row * COLS, (row + 1) * COLS
        grad = gn[a:b, :]
        value = normed[a:b, :]
        sums[1] += folded(grad * value)
        sums[2] += folded(grad)
        gs = grad * gain[...]
        gm = rstd[a:b, 0:1] * (
            gs
            - jnp.mean(gs, -1, keepdims=True)
            - value * jnp.mean(gs * value, -1, keepdims=True)
        )
        sums[0] += folded(gm)
        put_row(slab, row + 3, gm)
        if row < 3:
            top[a:b, :] = gm.astype(BF16)
        if row >= 13:
            bottom[a - 416 : b - 416, :] = gm.astype(BF16)
    for k in range(3):
        channel[k : k + 1, :] = jnp.sum(sums[k], 0, keepdims=True)


def taps_body(seen, grads, out):
    for p in range(7):

        def step(n, sums, p=p):
            row = n // 4
            col = (n % 4) * 8
            base = pl.multiple_of(((row + p) * WIDE + col) * 8, 8)
            home = pl.multiple_of(((row + 3) * WIDE + col + 3) * 8, 8)
            near = [seen[pl.ds(base + 8 * k, 8), :] for k in range(14)]
            sums = list(sums)
            for m in range(8):
                grad = grads[pl.ds(home + 8 * m, 8), :]
                for q in range(7):
                    sums[q] = sums[q] + near[m + q] * grad
            return tuple(sums)

        sums = lax.fori_loop(0, 32, step, tuple(jnp.zeros((8, 128), F32) for _ in range(7)))
        for q in range(7):
            out[(p * 7 + q) * 8 : (p * 7 + q + 1) * 8, :] = sums[q]


def up_body(old, left, right, taps, u, out, slab, store):
    slab[...] = old[...]
    put_columns(slab, left, right)
    filtered(slab, taps, store)
    for row in range(ROWS):
        a, b = row * COLS, (row + 1) * COLS
        out[a:b, :] = (u[a:b, :].astype(F32) + line_of(store, row)).astype(out.dtype)


STORE = pltpu.VMEM((ROWS * COLS * 4 + 16, 128), F32)
STRIP = ((DEEP * 24, 128), BF16)
EDGE = ((96, CH), BF16)


def pack(x, top, bottom):
    return call(pack_body, [((SLAB, 128), F32), STRIP, STRIP], 3, 10_000_000)(x, top, bottom)


def pack_edges(slab, top, bottom):
    return call(edge_body, [((SLAB, 128), F32), STRIP, STRIP], 3, 10_000_000)(slab, top, bottom)


def normalise(slab, left, right, taps, bias, gain, shift):
    outs = [((SLAB, 128), F32), ((PIX, CH), BF16), ((PIX, CH), F32), ((PIX, 128), F32)]
    return call(norm_body, outs, 7, 40_000_000, [STORE])(
        slab, left, right, taps, bias, gain, shift
    )


def mlp(place, a, normal, weights, bias_in, bias_out, scale):
    outs = [
        ((PIX, CH), BF16), EDGE, EDGE, ((PIX, FF), BF16), ((PIX, FF), BF16),
        ((PIX, CH), F32), ((CH, FF), BF16), ((FF, CH), BF16),
    ]
    return call(mlp_body, outs, 12, 60_000_000, scalars=1)(
        place, a, normal, *weights, bias_in, bias_out, scale
    )


def backward(place, u, saved, gain, scale):
    outs = [
        ((CH, FF), BF16), ((CH, FF), BF16), ((SLAB, 128), F32), EDGE, EDGE,
        ((8, CH), F32), ((1, FF), F32),
    ]
    scratch = [
        pltpu.VMEM((PIX, CH), BF16), pltpu.VMEM((PIX, FF), BF16), pltpu.VMEM((PIX, CH), F32),
    ]
    return call(back_body, outs, 12, 100_000_000, scratch, scalars=1)(
        place, u, *saved, gain, scale
    )


def tap_grads(seen, grads):
    return call(taps_body, [((49 * 8, 128), F32)], 2, 40_000_000)(seen, grads)[0]


def upstream(slab, left, right, taps, u, dtype):
    scratch = [pltpu.VMEM((SLAB, 128), F32), STORE]
    return call(up_body, [((PIX, CH), dtype)], 5, 40_000_000, scratch)(
        slab, left, right, taps, u
    )[0]


def spread(taps):
    lines = taps.reshape(49, 1, 4, 128)
    return jnp.broadcast_to(lines, (49, 2, 4, 128)).reshape(49 * 8, 128)


def finish_body(place, whole, mate, *refs):
    grad_in, grad_out = refs[-2:]
    core = place[0]
    for side, ref in ((core, whole), (1 - core, mate)):
        span = pl.ds(pl.multiple_of(side * HALF, HALF), HALF)
        grad_in[0, :, span] = ref[:, :HALF].astype(F32)
        grad_out[0, span, :] = ref[:, HALF:].astype(F32).T


def finish(place, whole, mate, layer, buffers):
    block = pl.BlockSpec((128, FF), lambda i: (i, 0))
    held = [pl.BlockSpec(memory_space=pl.ANY)] * len(buffers)
    return pl.pallas_call(
        finish_body,
        grid=(2,),
        out_shape=[
            jax.ShapeDtypeStruct((2, 256, FF), F32),
            jax.ShapeDtypeStruct((2, FF, 256), F32),
        ],
        in_specs=[SM, block, block, *held],
        out_specs=[
            pl.BlockSpec((1, 128, FF), lambda i: (layer, i, 0)),
            pl.BlockSpec((1, FF, 128), lambda i: (layer, 0, i)),
        ],
        input_output_aliases={3: 0, 4: 1} if buffers else {},
        cost_estimate=pl.CostEstimate(
            flops=10_000_000, bytes_accessed=6_000_000, transcendentals=0
        ),
    )(place, whole, mate, *buffers)


RANKS = ("xh", "y", "core")
FORWARD = {"rows": [(i, i + 1) for i in range(15)], "z": [(i, i + 1) for i in range(3)]}
BACKWARD = {k: [(b, a) for a, b in v] for k, v in FORWARD.items()}


def from_rows(top, bottom):
    return (
        lax.ppermute(bottom, RANKS, FORWARD["rows"]),
        lax.ppermute(top, RANKS, BACKWARD["rows"]),
    )


def from_columns(to_low, to_high):
    return (
        lax.ppermute(to_high, "z", FORWARD["z"]),
        lax.ppermute(to_low, "z", BACKWARD["z"]),
    )


def swapped(value, axis):
    return lax.ppermute(value, axis, [(0, 1), (1, 0)])


def around_x(value, step):
    return lax.ppermute(value, ("xh", "dp"), [(i, (i + step) % 4) for i in range(4)])


def fetch_weights(core, own_in, own_out):
    got_in = around_x(lax.dynamic_slice_in_dim(own_in, core * 128, 128, 0), 1)
    got_out = around_x(lax.dynamic_slice_in_dim(own_out, core * HALF, HALF, 0), -1)
    mate_in, mate_out = swapped(got_in, "core"), swapped(got_out, "core")
    return own_in, got_in, mate_in, own_out, got_out, mate_out


def reduce_weights(keep, give):
    pair = keep.astype(F32) + swapped(give, "core").astype(F32)
    pieces = lax.all_to_all(
        pair.astype(BF16).reshape(64, 8, FF), ("dp", *SPACE), 0, 0, tiled=True
    )
    mine = jnp.sum(pieces.astype(F32), 0).astype(BF16)
    copies = jnp.broadcast_to(mine, (32, 8, FF))
    whole = lax.all_to_all(copies, SPACE, 0, 0, tiled=True).reshape(256, FF)
    return whole, swapped(whole, "core")


def reduce_small(parts):
    axes = ("xh", "y", "core", "z", "dp")
    lines = jnp.concatenate([p.reshape(-1, 128) for p in parts])
    count = lines.shape[0]
    lines = jnp.pad(lines, ((0, -count % 512), (0, 0))).reshape(128, -1, 128)
    mine = jnp.sum(lax.all_to_all(lines, axes, 0, 0, tiled=True), 0)
    copies = jnp.broadcast_to(mine, lines.shape)
    whole = lax.all_to_all(copies, axes, 0, 0, tiled=True).reshape(-1, 128)
    outs = []
    start = 0
    for p in parts:
        size = p.size // 128
        outs.append(whole[start : start + size].reshape(p.shape))
        start += size
    return outs


def per_device(
    slides,
    cotangent,
    kernel,
    kernel_bias,
    norm_gain,
    norm_bias,
    weight_in,
    bias_in,
    weight_out,
    bias_out,
    layer_scale,
):
    core, part = lax.axis_index("core"), lax.axis_index("dp")
    place = jnp.stack([core, part]).astype(jnp.int32)
    one = lambda table, which: table[which][None]
    weights = [fetch_weights(core, weight_in[k], weight_out[k]) for k in range(2)]
    current = slides.reshape(PIX, CH)
    top, bottom = current[:96], current[416:]
    saved = []
    slabs = []
    for k in range(2):
        above, below = from_rows(top, bottom)
        slab, to_low, to_high = pack(current, above, below)
        left, right = from_columns(to_low, to_high)
        slab, normal, normed, rstd = normalise(
            slab, left, right, spread(kernel[k]),
            one(kernel_bias, k), one(norm_gain, k), one(norm_bias, k),
        )
        current, top, bottom, act, slope, branch, full_in, full_out = mlp(
            place, current, normal, weights[k],
            one(bias_in, k), one(bias_out, k), one(layer_scale, k),
        )
        slabs.append(slab)
        saved.append((branch, act, slope, normal, normed, rstd, full_in, full_out))
    up = cotangent.reshape(PIX, CH)
    buffers = ()
    taps, channels, biases = [None] * 2, [None] * 2, [None] * 2
    for k in (1, 0):
        keep, give, grads, top, bottom, channel, biases[k] = backward(
            place, up, saved[k], one(norm_gain, k), one(layer_scale, k)
        )
        above, below = from_rows(top, bottom)
        taps[k] = tap_grads(slabs[k], grads)
        slab, to_low, to_high = pack_edges(grads, above, below)
        left, right = from_columns(to_low, to_high)
        up = upstream(slab, left, right, spread(kernel[k][::-1, ::-1]), up, F32 if k else BF16)
        channels[k] = channel[:5]
        whole, mate = reduce_weights(keep, give)
        buffers = finish(place, whole, mate, k, buffers)
    summed = [t.reshape(49, 2, 4, 128).sum(1).reshape(7, 7, CH) for t in taps]
    small = reduce_small([jnp.stack(summed), jnp.stack(channels), jnp.concatenate(biases)])
    return (
        current.reshape(slides.shape),
        up.reshape(slides.shape),
        *buffers,
        *small,
    )


def solution(mesh):
    fine = jax.sharding.Mesh(
        mesh.devices.reshape(2, 4, 2, 4, 2), ("xh", "y", "core", "z", "dp")
    )
    maps = P("dp", RANKS, "z", None)
    split_in, split_out = P(None, "dp", None), P(None, None, "dp")
    whole = P()
    return jax.shard_map(
        per_device,
        mesh=fine,
        in_specs=(
            maps, maps, whole, whole, whole, whole, split_in, whole, split_out, whole, whole,
        ),
        out_specs=(maps, maps, split_in, split_out, whole, whole, whole),
        check_vma=False,
    )
```

```python
import jax
import jax.numpy as jnp
from jax import lax
from jax.experimental import pallas as pl
from jax.experimental.pallas import tpu as pltpu
from jax.sharding import PartitionSpec as P

COEF = 0.7978845608028654
CUBIC = 0.044715
EPSILON = 1e-06

PIX = 512
CH = 512
FF = 2048
HALF = 1024
WIRE = FF + 128
ROWS, COLS = 16, 32
WIDE = 40
DEEP = 14
SLAB = DEEP * WIDE * 8
SPACE = ("xh", "y", "z")
F32, BF16 = jnp.float32, jnp.bfloat16

VM = pl.BlockSpec(memory_space=pltpu.VMEM)
SM = pl.BlockSpec(memory_space=pltpu.SMEM)


def call(body, outs, count, flops, scratch=(), scalars=0):
    shapes = [jax.ShapeDtypeStruct(s, d) for s, d in outs]
    return pl.pallas_call(
        body,
        out_shape=shapes,
        in_specs=[SM] * scalars + [VM] * (count - scalars),
        out_specs=[VM] * len(outs),
        scratch_shapes=list(scratch),
        compiler_params=pltpu.CompilerParams(vmem_limit_bytes=56 * 1024 * 1024),
        cost_estimate=pl.CostEstimate(
            flops=flops, bytes_accessed=4_000_000, transcendentals=0
        ),
    )


def at(row, col):
    return (row * WIDE + col) * 8


def homes(row):
    found = []
    if row < DEEP:
        found.append((0, row))
    if row >= 8:
        found.append((1, row - 8))
    return found


def put_row(slab, row, line):
    for block, inner in homes(row):
        for group in range(4):
            slab[pl.ds(at(inner, 3) + block * 4 + group, COLS, stride=8), :] = line[
                :, group * 128 : (group + 1) * 128
            ]


def put_edges(slab, top, bottom):
    for k in range(3):
        put_row(slab, k, top[k * COLS : (k + 1) * COLS, :].astype(F32))
        put_row(slab, 19 + k, bottom[k * COLS : (k + 1) * COLS, :].astype(F32))


def put_columns(slab, left, right):
    for row in range(DEEP):
        a, b = row * 24, (row + 1) * 24
        slab[pl.ds(at(row, 0), 24), :] = left[a:b, :].astype(F32)
        slab[pl.ds(at(row, 35), 24), :] = right[a:b, :].astype(F32)


def take_columns(slab, to_low, to_high):
    for row in range(DEEP):
        a, b = row * 24, (row + 1) * 24
        to_low[a:b, :] = slab[pl.ds(at(row, 3), 24), :].astype(BF16)
        to_high[a:b, :] = slab[pl.ds(at(row, 32), 24), :].astype(BF16)


def filtered(slab, taps, store):
    def step(n, carry):
        row = n // 4
        col = (n % 4) * 8
        sums = [None] * 8
        for p in range(7):
            base = pl.multiple_of(((row + p) * WIDE + col) * 8, 8)
            seen = [slab[pl.ds(base + 8 * k, 8), :] for k in range(14)]
            for q in range(7):
                weight = taps[(p * 7 + q) * 8 : (p * 7 + q + 1) * 8, :]
                for m in range(8):
                    term = seen[m + q] * weight
                    sums[m] = term if sums[m] is None else sums[m] + term
        base = pl.multiple_of((row * COLS + col) * 8, 8)
        for m in range(8):
            store[pl.ds(base + 8 * m, 8), :] = sums[m]
        return carry

    lax.fori_loop(0, 32, step, 0)


def line_of(store, row):
    block, inner = row // 8, row % 8
    return jnp.concatenate(
        [
            store[pl.ds(inner * COLS * 8 + block * 4 + group, COLS, stride=8), :]
            for group in range(4)
        ],
        axis=1,
    )


def pack_body(x, top, bottom, slab, to_low, to_high):
    for row in range(ROWS):
        put_row(slab, row + 3, x[row * COLS : (row + 1) * COLS, :].astype(F32))
    put_edges(slab, top, bottom)
    take_columns(slab, to_low, to_high)


def edge_body(old, top, bottom, slab, to_low, to_high):
    slab[...] = old[...]
    put_edges(slab, top, bottom)
    take_columns(slab, to_low, to_high)


def norm_body(old, left, right, taps, bias, gain, shift, slab, normal, normed, rstd, store):
    slab[...] = old[...]
    put_columns(slab, left, right)
    filtered(slab, taps, store)
    for row in range(ROWS):
        a, b = row * COLS, (row + 1) * COLS
        mixed = line_of(store, row) + bias[...]
        center = mixed - jnp.mean(mixed, -1, keepdims=True)
        scale = lax.rsqrt(jnp.mean(center * center, -1, keepdims=True) + EPSILON)
        value = center * scale
        normed[a:b, :] = value
        rstd[a:b, :] = jnp.broadcast_to(scale, (COLS, 128))
        normal[a:b, :] = (value * gain[...] + shift[...]).astype(BF16)


def mlp_body(
    place, a, normal, own_in, got_in, mate_in, own_out, got_out, mate_out,
    bias_in, bias_out, scale,
    out, top, bottom, act, slope, branch, full_in, full_out,
):
    core, part = place[0], place[1]
    mine = pl.multiple_of(part * 256, 256)
    theirs = pl.multiple_of((1 - part) * 256, 256)
    full_in[pl.ds(mine, 256), :] = own_in[...]
    full_in[pl.ds(pl.multiple_of(theirs + core * 128, 128), 128), :] = got_in[...]
    full_in[pl.ds(pl.multiple_of(theirs + (1 - core) * 128, 128), 128), :] = mate_in[...]
    full_out[:, pl.ds(mine, 256)] = own_out[...]
    full_out[pl.ds(pl.multiple_of(core * HALF, HALF), HALF), pl.ds(theirs, 256)] = got_out[...]
    full_out[pl.ds(pl.multiple_of((1 - core) * HALF, HALF), HALF), pl.ds(theirs, 256)] = mate_out[...]
    for c in range(8):
        cols = slice(c * 256, (c + 1) * 256)
        hidden = jnp.dot(normal[...], full_in[:, cols], preferred_element_type=F32)
        v = hidden + bias_in[:, cols]
        square = v * v
        tangent = jnp.tanh(v * (COEF + (COEF * CUBIC) * square))
        half = 0.5 * v
        act[:, cols] = (half + half * tangent).astype(BF16)
        slope[:, cols] = (
            0.5
            + 0.5 * tangent
            + half * (1.0 - tangent * tangent) * (COEF + (3.0 * COEF * CUBIC) * square)
        ).astype(BF16)
    for c in range(2):
        cols = slice(c * 256, (c + 1) * 256)
        value = jnp.dot(act[...], full_out[:, cols], preferred_element_type=F32)
        value = value + bias_out[:, cols]
        branch[:, cols] = value
        result = (a[:, cols].astype(F32) + scale[:, cols] * value).astype(BF16)
        out[:, cols] = result
        top[:, cols] = result[:96, :]
        bottom[:, cols] = result[416:, :]


def back_body(
    place, u, branch, act, slope, normal, normed, rstd, full_in, full_out, gain, scale,
    keep, give, slab, top, bottom, channel, bias, low, gh, gn,
):
    core = place[0]
    rows_first = (((0,), (0,)), ((), ()))
    cols_last = (((1,), (1,)), ((), ()))
    up = u[...].astype(F32)
    channel[4:5, :] = jnp.sum(up * branch[...], 0, keepdims=True)
    gb = up * scale[...]
    channel[3:4, :] = jnp.sum(gb, 0, keepdims=True)
    low[...] = gb.astype(BF16)
    for c in range(8):
        cols = slice(c * 256, (c + 1) * 256)
        ga = lax.dot_general(
            low[...], full_out[cols, :], cols_last, preferred_element_type=F32
        )
        value = ga * slope[:, cols].astype(F32)
        bias[:, cols] = jnp.sum(value, 0, keepdims=True)
        gh[:, cols] = value.astype(BF16)
    for side, ref in ((core, keep), (1 - core, give)):
        for c in range(4):
            cols = pl.ds(pl.multiple_of(side * HALF + c * 256, 256), 256)
            ref[:, c * 256 : (c + 1) * 256] = lax.dot_general(
                normal[...], gh[:, cols], rows_first, preferred_element_type=F32
            ).astype(BF16)
            ref[:, HALF + c * 256 : HALF + (c + 1) * 256] = lax.dot_general(
                low[...], act[:, cols], rows_first, preferred_element_type=F32
            ).astype(BF16)
    for c in range(2):
        cols = slice(c * 256, (c + 1) * 256)
        gn[:, cols] = lax.dot_general(
            gh[...], full_in[cols, :], cols_last, preferred_element_type=F32
        )
    sums = [jnp.zeros((8, CH), F32) for _ in range(3)]

    def folded(value):
        return value[0:8] + value[8:16] + value[16:24] + value[24:32]

    for row in range(ROWS):
        a, b = row * COLS, (row + 1) * COLS
        grad = gn[a:b, :]
        value = normed[a:b, :]
        sums[1] += folded(grad * value)
        sums[2] += folded(grad)
        gs = grad * gain[...]
        gm = rstd[a:b, 0:1] * (
            gs
            - jnp.mean(gs, -1, keepdims=True)
            - value * jnp.mean(gs * value, -1, keepdims=True)
        )
        sums[0] += folded(gm)
        put_row(slab, row + 3, gm)
        if row < 3:
            top[a:b, :] = gm.astype(BF16)
        if row >= 13:
            bottom[a - 416 : b - 416, :] = gm.astype(BF16)
    for k in range(3):
        channel[k : k + 1, :] = jnp.sum(sums[k], 0, keepdims=True)


def taps_body(seen, grads, out):
    for p in range(7):

        def step(n, sums, p=p):
            row = n // 4
            col = (n % 4) * 8
            base = pl.multiple_of(((row + p) * WIDE + col) * 8, 8)
            home = pl.multiple_of(((row + 3) * WIDE + col + 3) * 8, 8)
            near = [seen[pl.ds(base + 8 * k, 8), :] for k in range(14)]
            sums = list(sums)
            for m in range(8):
                grad = grads[pl.ds(home + 8 * m, 8), :]
                for q in range(7):
                    sums[q] = sums[q] + near[m + q] * grad
            return tuple(sums)

        sums = lax.fori_loop(0, 32, step, tuple(jnp.zeros((8, 128), F32) for _ in range(7)))
        for q in range(7):
            out[(p * 7 + q) * 4 : (p * 7 + q + 1) * 4, :] = sums[q][0:4] + sums[q][4:8]


def up_body(old, left, right, taps, u, out, slab, store):
    slab[...] = old[...]
    put_columns(slab, left, right)
    filtered(slab, taps, store)
    for row in range(ROWS):
        a, b = row * COLS, (row + 1) * COLS
        out[a:b, :] = (u[a:b, :].astype(F32) + line_of(store, row)).astype(out.dtype)


def pair_body(keep, got, taps, channel, bias, out, lines):
    lines[0:196, :] = taps[...]
    spot = 196
    for kind in range(5):
        for group in range(4):
            lines[spot : spot + 1, :] = channel[
                kind : kind + 1, group * 128 : (group + 1) * 128
            ]
            spot += 1
    for group in range(16):
        lines[spot : spot + 1, :] = bias[:, group * 128 : (group + 1) * 128]
        spot += 1
    lines[spot:256, :] = jnp.zeros((256 - spot, 128), F32)

    def step(n, carry):
        rows = pl.ds(pl.multiple_of(n * 32, 32), 32)
        total = keep[rows, :].astype(F32) + got[rows, :].astype(F32)
        out[pl.ds(n * 4, 4), :, :FF] = total.reshape(4, 8, FF).astype(BF16)
        rows = pl.ds(pl.multiple_of((n % 8) * 32, 32), 32)
        out[pl.ds(n * 4, 4), :, FF:] = lines[rows, :].reshape(4, 8, 128).astype(BF16)
        return carry

    lax.fori_loop(0, 16, step, 0)


def merge_body(pieces0, pieces1, out):
    for k, pieces in ((0, pieces0), (1, pieces1)):
        for a, b in ((0, 512), (512, 1024), (1024, 1536), (1536, 2176)):
            def step(n, total, a=a, b=b, pieces=pieces):
                for m in range(4):
                    total = total + pieces[n * 4 + m, :, a:b].astype(F32)
                return total

            total = lax.fori_loop(0, 16, step, jnp.zeros((8, b - a), F32)).astype(BF16)
            for n in range(32):
                out[n, :, k * WIRE + a : k * WIRE + b] = total


def small_body(whole0, whole1, mate0, mate1, taps, channel, bias, lines):
    for k, whole, mate in ((0, whole0, mate0), (1, whole1, mate1)):
        lines[0:256, :] = (whole[...].astype(F32) + mate[...].astype(F32)).reshape(256, 128)
        for group in range(4):
            cols = slice(group * 128, (group + 1) * 128)
            taps[k, :, cols] = lines[pl.ds(group, 49, stride=4), :]
            channel[k, :, cols] = lines[pl.ds(196 + group, 5, stride=4), :]
        for group in range(16):
            bias[k : k + 1, group * 128 : (group + 1) * 128] = lines[216 + group : 217 + group, :]


def finish_body(place, whole, mate, grad_in, grad_out):
    core = place[0]
    for side, ref in ((core, whole), (1 - core, mate)):
        span = pl.ds(pl.multiple_of(side * HALF, HALF), HALF)
        value = ref[:, :, :FF].astype(F32).reshape(128, FF)
        grad_in[0, :, span] = value[:, :HALF]
        grad_out[0, span, :] = value[:, HALF:].T


STORE = pltpu.VMEM((ROWS * COLS * 4 + 16, 128), F32)
STRIP = ((DEEP * 24, 128), BF16)
EDGE = ((96, CH), BF16)


def pack(x, top, bottom):
    return call(pack_body, [((SLAB, 128), F32), STRIP, STRIP], 3, 10_000_000)(x, top, bottom)


def pack_edges(slab, top, bottom):
    return call(edge_body, [((SLAB, 128), F32), STRIP, STRIP], 3, 10_000_000)(slab, top, bottom)


def normalise(slab, left, right, taps, bias, gain, shift):
    outs = [((SLAB, 128), F32), ((PIX, CH), BF16), ((PIX, CH), F32), ((PIX, 128), F32)]
    return call(norm_body, outs, 7, 40_000_000, [STORE])(
        slab, left, right, taps, bias, gain, shift
    )


def mlp(place, a, normal, weights, bias_in, bias_out, scale):
    outs = [
        ((PIX, CH), BF16), EDGE, EDGE, ((PIX, FF), BF16), ((PIX, FF), BF16),
        ((PIX, CH), F32), ((CH, FF), BF16), ((FF, CH), BF16),
    ]
    return call(mlp_body, outs, 12, 60_000_000, scalars=1)(
        place, a, normal, *weights, bias_in, bias_out, scale
    )


def backward(place, u, saved, gain, scale):
    outs = [
        ((CH, FF), BF16), ((CH, FF), BF16), ((SLAB, 128), F32), EDGE, EDGE,
        ((8, CH), F32), ((1, FF), F32),
    ]
    scratch = [
        pltpu.VMEM((PIX, CH), BF16), pltpu.VMEM((PIX, FF), BF16), pltpu.VMEM((PIX, CH), F32),
    ]
    return call(back_body, outs, 12, 100_000_000, scratch, scalars=1)(
        place, u, *saved, gain, scale
    )


def tap_grads(seen, grads):
    return call(taps_body, [((49 * 4, 128), F32)], 2, 40_000_000)(seen, grads)[0]


def upstream(slab, left, right, taps, u, dtype):
    scratch = [pltpu.VMEM((SLAB, 128), F32), STORE]
    return call(up_body, [((PIX, CH), dtype)], 5, 40_000_000, scratch)(
        slab, left, right, taps, u
    )[0]


def spread(taps):
    lines = taps.reshape(49, 1, 4, 128)
    return jnp.broadcast_to(lines, (49, 2, 4, 128)).reshape(49 * 8, 128)


def finish(place, whole, mate):
    block = pl.BlockSpec((16, 8, WIRE), lambda layer, i: (i, 0, layer))
    return pl.pallas_call(
        finish_body,
        grid=(2, 2),
        out_shape=[
            jax.ShapeDtypeStruct((2, 256, FF), F32),
            jax.ShapeDtypeStruct((2, FF, 256), F32),
        ],
        in_specs=[SM, block, block],
        out_specs=[
            pl.BlockSpec((1, 128, FF), lambda layer, i: (layer, i, 0)),
            pl.BlockSpec((1, FF, 128), lambda layer, i: (layer, 0, i)),
        ],
        cost_estimate=pl.CostEstimate(
            flops=10_000_000, bytes_accessed=12_000_000, transcendentals=0
        ),
    )(place, whole, mate)


def finish_small(whole, mate):
    first = pl.BlockSpec((32, 8, 128), lambda i: (0, 0, FF // 128))
    second = pl.BlockSpec((32, 8, 128), lambda i: (0, 0, (WIRE + FF) // 128))
    shapes = [(2, 49, CH), (2, 5, CH), (2, FF)]
    return pl.pallas_call(
        small_body,
        grid=(1,),
        out_shape=[jax.ShapeDtypeStruct(s, F32) for s in shapes],
        in_specs=[first, second, first, second],
        out_specs=[
            pl.BlockSpec((2, 49, CH), lambda i: (0, 0, 0)),
            pl.BlockSpec((2, 5, CH), lambda i: (0, 0, 0)),
            pl.BlockSpec((2, FF), lambda i: (0, 0)),
        ],
        scratch_shapes=[pltpu.VMEM((256 + 8, 128), F32)],
        cost_estimate=pl.CostEstimate(
            flops=1_000_000, bytes_accessed=1_000_000, transcendentals=0
        ),
    )(whole, whole, mate, mate)


RANKS = ("xh", "y", "core")
FORWARD = {"rows": [(i, i + 1) for i in range(15)], "z": [(i, i + 1) for i in range(3)]}
BACKWARD = {k: [(b, a) for a, b in v] for k, v in FORWARD.items()}


def from_rows(top, bottom):
    above = lax.ppermute(bottom, RANKS, FORWARD["rows"])
    below = lax.ppermute(top, RANKS, BACKWARD["rows"])
    return above, below


def from_columns(to_low, to_high):
    left = lax.ppermute(to_high, "z", FORWARD["z"])
    right = lax.ppermute(to_low, "z", BACKWARD["z"])
    return left, right


def swapped(value, axis):
    return lax.ppermute(value, axis, [(0, 1), (1, 0)])


def around_x(value, step):
    return lax.ppermute(value, ("xh", "dp"), [(i, (i + step) % 4) for i in range(4)])


def fetch_weights(core, weight_in, weight_out, k):
    half_in = lax.dynamic_slice(weight_in, (k, core * 128, 0), (1, 128, FF))[0]
    half_out = lax.dynamic_slice(weight_out, (k, core * HALF, 0), (1, HALF, 256))[0]
    got_in = around_x(half_in, 1)
    got_out = around_x(half_out, -1)
    mate_in = swapped(got_in, "core")
    mate_out = swapped(got_out, "core")
    return weight_in[k], got_in, mate_in, weight_out[k], got_out, mate_out


def send_grads(keep, got, taps, channel, bias):
    scratch = [pltpu.VMEM((256, 128), F32)]
    pair = call(pair_body, [((64, 8, WIRE), BF16)], 5, 2_000_000, scratch)(
        keep, got, taps, channel, bias
    )[0]
    return lax.all_to_all(pair, ("dp", *SPACE), 0, 0, tiled=True)


def per_device(
    slides,
    cotangent,
    kernel,
    kernel_bias,
    norm_gain,
    norm_bias,
    weight_in,
    bias_in,
    weight_out,
    bias_out,
    layer_scale,
):
    core, part = lax.axis_index("core"), lax.axis_index("dp")
    place = jnp.stack([core, part]).astype(jnp.int32)
    one = lambda table, which: table[which][None]
    current = slides.reshape(PIX, CH)
    top, bottom = current[:96], current[416:]
    saved = []
    slabs = []
    weights = fetch_weights(core, weight_in, weight_out, 0)
    for k in range(2):
        above, below = from_rows(top, bottom)
        slab, to_low, to_high = pack(current, above, below)
        left, right = from_columns(to_low, to_high)
        slab, normal, normed, rstd = normalise(
            slab, left, right, spread(kernel[k]),
            one(kernel_bias, k), one(norm_gain, k), one(norm_bias, k),
        )
        current, top, bottom, act, slope, branch, full_in, full_out = mlp(
            place, current, normal, weights,
            one(bias_in, k), one(bias_out, k), one(layer_scale, k),
        )
        slabs.append(slab)
        saved.append((branch, act, slope, normal, normed, rstd, full_in, full_out))
        if k == 0:
            later_in, later_out, _ = lax.optimization_barrier((weight_in, weight_out, left))
            weights = fetch_weights(core, later_in, later_out, 1)
    up = cotangent.reshape(PIX, CH)
    pieces = [None] * 2
    for k in (1, 0):
        keep, give, grads, top, bottom, channel, bias = backward(
            place, up, saved[k], one(norm_gain, k), one(layer_scale, k)
        )
        got = swapped(give, "core")
        above, below = from_rows(top, bottom)
        taps = tap_grads(slabs[k], grads)
        pieces[k] = send_grads(keep, got, taps, channel, bias)
        slab, to_low, to_high = pack_edges(grads, above, below)
        left, right = from_columns(to_low, to_high)
        up = upstream(
            slab, left, right, spread(kernel[k][::-1, ::-1]), up, F32 if k else BF16
        )
    copies = call(merge_body, [((32, 8, 2 * WIRE), BF16)], 2, 5_000_000)(*pieces)[0]
    whole = lax.all_to_all(copies, SPACE, 0, 0, tiled=True)
    mate = swapped(whole, "core")
    grad_in, grad_out = finish(place, whole, mate)
    grad_taps, grad_channel, grad_bias = finish_small(whole, mate)
    return (
        current.reshape(slides.shape),
        up.reshape(slides.shape),
        grad_in,
        grad_out,
        grad_taps.reshape(2, 7, 7, CH),
        grad_channel,
        grad_bias,
    )


def solution(mesh):
    fine = jax.sharding.Mesh(
        mesh.devices.reshape(2, 4, 2, 4, 2), ("xh", "y", "core", "z", "dp")
    )
    maps = P("dp", RANKS, "z", None)
    split_in, split_out = P(None, "dp", None), P(None, None, "dp")
    whole = P()
    return jax.shard_map(
        per_device,
        mesh=fine,
        in_specs=(
            maps, maps, whole, whole, whole, whole, split_in, whole, split_out, whole, whole,
        ),
        out_specs=(maps, maps, split_in, split_out, whole, whole, whole),
        check_vma=False,
    )
```

```python
import functools

import jax
import jax.numpy as jnp
from jax import lax
from jax.experimental import pallas as pl
from jax.experimental.pallas import tpu as pltpu
from jax.sharding import PartitionSpec as P

COEF = 0.7978845608028654
CUBIC = 0.044715
EPSILON = 1e-06

PIX = 512
CH = 512
FF = 2048
HALF = 1024
WIRE = FF + 128
ROWS, COLS = 16, 32
WIDE = 40
DEEP = 14
SLAB = DEEP * WIDE * 8
SPACE = ("xh", "y", "z")
F32, BF16 = jnp.float32, jnp.bfloat16

VM = pl.BlockSpec(memory_space=pltpu.VMEM)
SM = pl.BlockSpec(memory_space=pltpu.SMEM)


def call(body, outs, count, flops, scratch=(), scalars=0, grant=12):
    shapes = [jax.ShapeDtypeStruct(s, d) for s, d in outs]
    return pl.pallas_call(
        body,
        out_shape=shapes,
        in_specs=[SM] * scalars + [VM] * (count - scalars),
        out_specs=[VM] * len(outs),
        scratch_shapes=list(scratch),
        compiler_params=pltpu.CompilerParams(vmem_limit_bytes=grant * 1024 * 1024),
        cost_estimate=pl.CostEstimate(
            flops=flops, bytes_accessed=4_000_000, transcendentals=0
        ),
    )


def at(row, col):
    return (row * WIDE + col) * 8


def homes(row):
    found = []
    if row < DEEP:
        found.append((0, row))
    if row >= 8:
        found.append((1, row - 8))
    return found


def put_row(slab, row, line):
    for block, inner in homes(row):
        for group in range(4):
            slab[pl.ds(at(inner, 3) + block * 4 + group, COLS, stride=8), :] = line[
                :, group * 128 : (group + 1) * 128
            ]


def put_edges(slab, top, bottom):
    for k in range(3):
        put_row(slab, k, top[k * COLS : (k + 1) * COLS, :].astype(F32))
        put_row(slab, 19 + k, bottom[k * COLS : (k + 1) * COLS, :].astype(F32))


def put_columns(slab, left, right):
    for row in range(DEEP):
        a, b = row * 24, (row + 1) * 24
        slab[pl.ds(at(row, 0), 24), :] = left[a:b, :].astype(F32)
        slab[pl.ds(at(row, 35), 24), :] = right[a:b, :].astype(F32)


def take_columns(slab, to_low, to_high):
    for row in range(DEEP):
        a, b = row * 24, (row + 1) * 24
        to_low[a:b, :] = slab[pl.ds(at(row, 3), 24), :].astype(BF16)
        to_high[a:b, :] = slab[pl.ds(at(row, 32), 24), :].astype(BF16)


def spread(kernel, k, taps):
    for tap in range(49):
        line = kernel[tap // 7, tap % 7, k : k + 1, :]
        for part in range(8):
            group = part % 4
            taps[tap * 8 + part : tap * 8 + part + 1, :] = line[
                :, group * 128 : (group + 1) * 128
            ]


def filtered(slab, taps, store, turned):
    def step(n, carry):
        row = n // 4
        col = (n % 4) * 8
        sums = [None] * 8
        for p in range(7):
            base = pl.multiple_of(((row + p) * WIDE + col) * 8, 8)
            seen = [slab[pl.ds(base + 8 * k, 8), :] for k in range(14)]
            for q in range(7):
                tap = 48 - p * 7 - q if turned else p * 7 + q
                weight = taps[tap * 8 : tap * 8 + 8, :]
                for m in range(8):
                    term = seen[m + q] * weight
                    sums[m] = term if sums[m] is None else sums[m] + term
        base = pl.multiple_of((row * COLS + col) * 8, 8)
        for m in range(8):
            store[pl.ds(base + 8 * m, 8), :] = sums[m]
        return carry

    lax.fori_loop(0, 32, step, 0)


def line_of(store, row):
    block, inner = row // 8, row % 8
    return jnp.concatenate(
        [
            store[pl.ds(inner * COLS * 8 + block * 4 + group, COLS, stride=8), :]
            for group in range(4)
        ],
        axis=1,
    )


def pack_body(x, top, bottom, slab, to_low, to_high):
    for row in range(ROWS):
        put_row(slab, row + 3, x[row * COLS : (row + 1) * COLS, :].astype(F32))
    put_edges(slab, top, bottom)
    take_columns(slab, to_low, to_high)


def edge_body(old, top, bottom, slab, to_low, to_high):
    slab[...] = old[...]
    put_edges(slab, top, bottom)
    take_columns(slab, to_low, to_high)


def norm_body(
    k, old, left, right, kernel, bias, gain, shift, slab, normal, normed, rstd, store, taps
):
    one = slice(k, k + 1)
    spread(kernel, k, taps)
    slab[...] = old[...]
    put_columns(slab, left, right)
    filtered(slab, taps, store, False)
    for row in range(ROWS):
        a, b = row * COLS, (row + 1) * COLS
        mixed = line_of(store, row) + bias[one, :]
        center = mixed - jnp.mean(mixed, -1, keepdims=True)
        scale = lax.rsqrt(jnp.mean(center * center, -1, keepdims=True) + EPSILON)
        value = center * scale
        normed[a:b, :] = value
        rstd[a:b, :] = jnp.broadcast_to(scale, (COLS, 128))
        normal[a:b, :] = (value * gain[one, :] + shift[one, :]).astype(BF16)


def mlp_body(
    k, place, a, normal, own_in, got_in, mate_in, own_out, got_out, mate_out,
    bias_in, bias_out, scale,
    out, top, bottom, act, slope, branch, full_in, full_out,
):
    one = slice(k, k + 1)
    core, part = place[0], place[1]
    mine = pl.multiple_of(part * 256, 256)
    theirs = pl.multiple_of((1 - part) * 256, 256)
    full_in[pl.ds(mine, 256), :] = own_in[k]
    full_in[pl.ds(pl.multiple_of(theirs + core * 128, 128), 128), :] = got_in[...]
    full_in[pl.ds(pl.multiple_of(theirs + (1 - core) * 128, 128), 128), :] = mate_in[...]
    full_out[:, pl.ds(mine, 256)] = own_out[k]
    full_out[pl.ds(pl.multiple_of(core * HALF, HALF), HALF), pl.ds(theirs, 256)] = got_out[...]
    full_out[pl.ds(pl.multiple_of((1 - core) * HALF, HALF), HALF), pl.ds(theirs, 256)] = mate_out[...]
    for c in range(8):
        cols = slice(c * 256, (c + 1) * 256)
        hidden = jnp.dot(normal[...], full_in[:, cols], preferred_element_type=F32)
        v = hidden + bias_in[one, cols]
        square = v * v
        tangent = jnp.tanh(v * (COEF + (COEF * CUBIC) * square))
        half = 0.5 * v
        act[:, cols] = (half + half * tangent).astype(BF16)
        slope[:, cols] = (
            0.5
            + 0.5 * tangent
            + half * (1.0 - tangent * tangent) * (COEF + (3.0 * COEF * CUBIC) * square)
        ).astype(BF16)
    for c in range(2):
        cols = slice(c * 256, (c + 1) * 256)
        value = jnp.dot(act[...], full_out[:, cols], preferred_element_type=F32)
        value = value + bias_out[one, cols]
        branch[:, cols] = value
        result = (a[:, cols].astype(F32) + scale[one, cols] * value).astype(BF16)
        out[:, cols] = result
        top[:, cols] = result[:96, :]
        bottom[:, cols] = result[416:, :]


def back_body(
    k, u, branch, slope, normed, rstd, full_in, full_out, gain, scale,
    low, gh, slab, top, bottom, channel, bias, gn,
):
    one = slice(k, k + 1)
    cols_last = (((1,), (1,)), ((), ()))
    up = u[...].astype(F32)
    channel[4:5, :] = jnp.sum(up * branch[...], 0, keepdims=True)
    gb = up * scale[one, :]
    channel[3:4, :] = jnp.sum(gb, 0, keepdims=True)
    low[...] = gb.astype(BF16)
    for c in range(8):
        cols = slice(c * 256, (c + 1) * 256)
        ga = lax.dot_general(
            low[...], full_out[cols, :], cols_last, preferred_element_type=F32
        )
        value = ga * slope[:, cols].astype(F32)
        bias[:, cols] = jnp.sum(value, 0, keepdims=True)
        gh[:, cols] = value.astype(BF16)
    for c in range(2):
        cols = slice(c * 256, (c + 1) * 256)
        gn[:, cols] = lax.dot_general(
            gh[...], full_in[cols, :], cols_last, preferred_element_type=F32
        )
    sums = [jnp.zeros((8, CH), F32) for _ in range(3)]

    def folded(value):
        return value[0:8] + value[8:16] + value[16:24] + value[24:32]

    for row in range(ROWS):
        a, b = row * COLS, (row + 1) * COLS
        grad = gn[a:b, :]
        value = normed[a:b, :]
        sums[1] += folded(grad * value)
        sums[2] += folded(grad)
        gs = grad * gain[one, :]
        gm = rstd[a:b, 0:1] * (
            gs
            - jnp.mean(gs, -1, keepdims=True)
            - value * jnp.mean(gs * value, -1, keepdims=True)
        )
        sums[0] += folded(gm)
        put_row(slab, row + 3, gm)
        if row < 3:
            top[a:b, :] = gm.astype(BF16)
        if row >= 13:
            bottom[a - 416 : b - 416, :] = gm.astype(BF16)
    for n in range(3):
        channel[n : n + 1, :] = jnp.sum(sums[n], 0, keepdims=True)


def grads_body(place, normal, low, act, gh, keep, give):
    core = place[0]
    rows_first = (((0,), (0,)), ((), ()))
    for side, ref in ((1 - core, give), (core, keep)):
        for c in range(4):
            cols = pl.ds(pl.multiple_of(side * HALF + c * 256, 256), 256)
            ref[:, c * 256 : (c + 1) * 256] = lax.dot_general(
                normal[...], gh[:, cols], rows_first, preferred_element_type=F32
            ).astype(BF16)
            ref[:, HALF + c * 256 : HALF + (c + 1) * 256] = lax.dot_general(
                low[...], act[:, cols], rows_first, preferred_element_type=F32
            ).astype(BF16)


def taps_body(seen, grads, out):
    for p in range(7):

        def step(n, sums, p=p):
            row = n // 4
            col = (n % 4) * 8
            base = pl.multiple_of(((row + p) * WIDE + col) * 8, 8)
            home = pl.multiple_of(((row + 3) * WIDE + col + 3) * 8, 8)
            near = [seen[pl.ds(base + 8 * k, 8), :] for k in range(14)]
            sums = list(sums)
            for m in range(8):
                grad = grads[pl.ds(home + 8 * m, 8), :]
                for q in range(7):
                    sums[q] = sums[q] + near[m + q] * grad
            return tuple(sums)

        sums = lax.fori_loop(0, 32, step, tuple(jnp.zeros((8, 128), F32) for _ in range(7)))
        for q in range(7):
            out[(p * 7 + q) * 4 : (p * 7 + q + 1) * 4, :] = sums[q][0:4] + sums[q][4:8]


def up_body(k, old, left, right, kernel, u, out, slab, store, taps):
    spread(kernel, k, taps)
    slab[...] = old[...]
    put_columns(slab, left, right)
    filtered(slab, taps, store, True)
    for row in range(ROWS):
        a, b = row * COLS, (row + 1) * COLS
        out[a:b, :] = (u[a:b, :].astype(F32) + line_of(store, row)).astype(out.dtype)


def pair_body(keep, got, taps, channel, bias, out, lines):
    lines[0:196, :] = taps[...]
    spot = 196
    for kind in range(5):
        for group in range(4):
            lines[spot : spot + 1, :] = channel[
                kind : kind + 1, group * 128 : (group + 1) * 128
            ]
            spot += 1
    for group in range(16):
        lines[spot : spot + 1, :] = bias[:, group * 128 : (group + 1) * 128]
        spot += 1
    lines[spot:256, :] = jnp.zeros((256 - spot, 128), F32)

    def step(n, carry):
        rows = pl.ds(pl.multiple_of(n * 32, 32), 32)
        total = keep[rows, :].astype(F32) + got[rows, :].astype(F32)
        out[pl.ds(n * 4, 4), :, :FF] = total.reshape(4, 8, FF).astype(BF16)
        rows = pl.ds(pl.multiple_of((n % 8) * 32, 32), 32)
        out[pl.ds(n * 4, 4), :, FF:] = lines[rows, :].reshape(4, 8, 128).astype(BF16)
        return carry

    lax.fori_loop(0, 16, step, 0)


def merge_body(pieces0, pieces1, out):
    for k, pieces in ((0, pieces0), (1, pieces1)):
        for a, b in ((0, 512), (512, 1024), (1024, 1536), (1536, 2176)):
            def step(n, total, a=a, b=b, pieces=pieces):
                for m in range(4):
                    total = total + pieces[n * 4 + m, :, a:b].astype(F32)
                return total

            total = lax.fori_loop(0, 16, step, jnp.zeros((8, b - a), F32)).astype(BF16)
            for n in range(32):
                out[n, :, k * WIRE + a : k * WIRE + b] = total


def small_body(whole0, whole1, mate0, mate1, taps, channel, bias, lines):
    for k, whole, mate in ((0, whole0, mate0), (1, whole1, mate1)):
        lines[0:256, :] = (whole[...].astype(F32) + mate[...].astype(F32)).reshape(256, 128)
        for group in range(4):
            cols = slice(group * 128, (group + 1) * 128)
            for tap in range(49):
                line = tap * 4 + group
                taps[tap // 7, tap % 7, k : k + 1, cols] = lines[line : line + 1, :]
            for kind in range(5):
                line = 196 + kind * 4 + group
                channel[kind, k : k + 1, cols] = lines[line : line + 1, :]
        for group in range(16):
            bias[k : k + 1, group * 128 : (group + 1) * 128] = lines[216 + group : 217 + group, :]


def finish_body(place, whole, mate, grad_in, grad_out):
    core = place[0]
    for side, ref in ((core, whole), (1 - core, mate)):
        span = pl.ds(pl.multiple_of(side * HALF, HALF), HALF)
        value = ref[:, :, :FF].astype(F32).reshape(128, FF)
        grad_in[0, :, span] = value[:, :HALF]
        grad_out[0, span, :] = value[:, HALF:].T


STORE = pltpu.VMEM((ROWS * COLS * 4 + 16, 128), F32)
TAPS = pltpu.VMEM((400, 128), F32)
STRIP = ((DEEP * 24, 128), BF16)
EDGE = ((96, CH), BF16)


def pack(x, top, bottom):
    return call(pack_body, [((SLAB, 128), F32), STRIP, STRIP], 3, 10_000_000)(x, top, bottom)


def pack_edges(slab, top, bottom):
    return call(edge_body, [((SLAB, 128), F32), STRIP, STRIP], 3, 10_000_000)(slab, top, bottom)


def normalise(k, slab, left, right, kernel, bias, gain, shift):
    outs = [((SLAB, 128), F32), ((PIX, CH), BF16), ((PIX, CH), F32), ((PIX, 128), F32)]
    return call(functools.partial(norm_body, k), outs, 7, 40_000_000, [STORE, TAPS])(
        slab, left, right, kernel, bias, gain, shift
    )


def mlp(k, place, a, normal, weights, bias_in, bias_out, scale):
    outs = [
        ((PIX, CH), BF16), EDGE, EDGE, ((PIX, FF), BF16), ((PIX, FF), BF16),
        ((PIX, CH), F32), ((CH, FF), BF16), ((FF, CH), BF16),
    ]
    return call(functools.partial(mlp_body, k), outs, 12, 60_000_000, scalars=1)(
        place, a, normal, *weights, bias_in, bias_out, scale
    )


def backward(k, u, saved, gain, scale):
    outs = [
        ((PIX, CH), BF16), ((PIX, FF), BF16), ((SLAB, 128), F32), EDGE, EDGE,
        ((8, CH), F32), ((1, FF), F32),
    ]
    scratch = [pltpu.VMEM((PIX, CH), F32)]
    return call(functools.partial(back_body, k), outs, 9, 60_000_000, scratch)(
        u, *saved, gain, scale
    )


def weight_grads(place, normal, low, act, gh):
    outs = [((CH, FF), BF16), ((CH, FF), BF16)]
    return call(grads_body, outs, 5, 50_000_000, scalars=1)(place, normal, low, act, gh)


def tap_grads(seen, grads):
    return call(taps_body, [((49 * 4, 128), F32)], 2, 40_000_000)(seen, grads)[0]


def upstream(k, slab, left, right, kernel, u, dtype):
    scratch = [pltpu.VMEM((SLAB, 128), F32), STORE, TAPS]
    return call(functools.partial(up_body, k), [((PIX, CH), dtype)], 5, 40_000_000, scratch)(
        slab, left, right, kernel, u
    )[0]


def finish(place, whole, mate):
    block = pl.BlockSpec((16, 8, WIRE), lambda layer, i: (i, 0, layer))
    return pl.pallas_call(
        finish_body,
        grid=(2, 2),
        out_shape=[
            jax.ShapeDtypeStruct((2, 256, FF), F32),
            jax.ShapeDtypeStruct((2, FF, 256), F32),
        ],
        in_specs=[SM, block, block],
        out_specs=[
            pl.BlockSpec((1, 128, FF), lambda layer, i: (layer, i, 0)),
            pl.BlockSpec((1, FF, 128), lambda layer, i: (layer, 0, i)),
        ],
        cost_estimate=pl.CostEstimate(
            flops=10_000_000, bytes_accessed=12_000_000, transcendentals=0
        ),
    )(place, whole, mate)


def finish_small(whole, mate):
    first = pl.BlockSpec((32, 8, 128), lambda i: (0, 0, FF // 128))
    second = pl.BlockSpec((32, 8, 128), lambda i: (0, 0, (WIRE + FF) // 128))
    shapes = [(7, 7, 2, CH), (5, 2, CH), (2, FF)]
    return pl.pallas_call(
        small_body,
        grid=(1,),
        out_shape=[jax.ShapeDtypeStruct(s, F32) for s in shapes],
        in_specs=[first, second, first, second],
        out_specs=[
            pl.BlockSpec((7, 7, 2, CH), lambda i: (0, 0, 0, 0)),
            pl.BlockSpec((5, 2, CH), lambda i: (0, 0, 0)),
            pl.BlockSpec((2, FF), lambda i: (0, 0)),
        ],
        scratch_shapes=[pltpu.VMEM((256 + 8, 128), F32)],
        cost_estimate=pl.CostEstimate(
            flops=1_000_000, bytes_accessed=1_000_000, transcendentals=0
        ),
    )(whole, whole, mate, mate)


RANKS = ("xh", "y", "core")
FORWARD = {"rows": [(i, i + 1) for i in range(15)], "z": [(i, i + 1) for i in range(3)]}
BACKWARD = {k: [(b, a) for a, b in v] for k, v in FORWARD.items()}


def from_rows(top, bottom):
    above = lax.ppermute(bottom, RANKS, FORWARD["rows"])
    below = lax.ppermute(top, RANKS, BACKWARD["rows"])
    return above, below


def from_columns(to_low, to_high):
    left = lax.ppermute(to_high, "z", FORWARD["z"])
    right = lax.ppermute(to_low, "z", BACKWARD["z"])
    return left, right


def swapped(value, axis):
    return lax.ppermute(value, axis, [(0, 1), (1, 0)])


def around_x(value, step):
    return lax.ppermute(value, ("xh", "dp"), [(i, (i + step) % 4) for i in range(4)])


def fetch_weights(core, weight_in, weight_out, k):
    half_in = lax.dynamic_slice(weight_in, (k, core * 128, 0), (1, 128, FF))[0]
    half_out = lax.dynamic_slice(weight_out, (k, core * HALF, 0), (1, HALF, 256))[0]
    got_in = around_x(half_in, 1)
    got_out = around_x(half_out, -1)
    mate_in = swapped(got_in, "core")
    mate_out = swapped(got_out, "core")
    return got_in, mate_in, got_out, mate_out


def send_grads(keep, got, taps, channel, bias):
    scratch = [pltpu.VMEM((256, 128), F32)]
    pair = call(pair_body, [((64, 8, WIRE), BF16)], 5, 2_000_000, scratch)(
        keep, got, taps, channel, bias
    )[0]
    return lax.all_to_all(pair, ("dp", *SPACE), 0, 0, tiled=True)


def per_device(
    slides,
    cotangent,
    kernel,
    kernel_bias,
    norm_gain,
    norm_bias,
    weight_in,
    bias_in,
    weight_out,
    bias_out,
    layer_scale,
):
    core, part = lax.axis_index("core"), lax.axis_index("dp")
    place = jnp.stack([core, part]).astype(jnp.int32)
    kernel = jnp.transpose(kernel, (1, 2, 0, 3))
    current = slides.reshape(PIX, CH)
    top, bottom = current[:96], current[416:]
    saved = []
    fetched = fetch_weights(core, weight_in, weight_out, 0)
    for k in range(2):
        above, below = from_rows(top, bottom)
        slab, to_low, to_high = pack(current, above, below)
        left, right = from_columns(to_low, to_high)
        slab, normal, normed, rstd = normalise(
            k, slab, left, right, kernel, kernel_bias, norm_gain, norm_bias
        )
        weights = (weight_in, *fetched[:2], weight_out, *fetched[2:])
        current, top, bottom, act, slope, branch, full_in, full_out = mlp(
            k, place, current, normal, weights, bias_in, bias_out, layer_scale
        )
        saved.append((slab, act, normal, (branch, slope, normed, rstd, full_in, full_out)))
        if k == 0:
            later_in, later_out, _ = lax.optimization_barrier((weight_in, weight_out, normal))
            fetched = fetch_weights(core, later_in, later_out, 1)
    up = cotangent.reshape(PIX, CH)
    pieces = [None] * 2
    for k in (1, 0):
        seen, act, normal, rest = saved[k]
        low, gh, grads, top, bottom, channel, bias = backward(k, up, rest, norm_gain, layer_scale)
        above, below = from_rows(top, bottom)
        keep, give = weight_grads(place, normal, low, act, gh)
        got = swapped(give, "core")
        taps = tap_grads(seen, grads)
        pieces[k] = send_grads(keep, got, taps, channel, bias)
        slab, to_low, to_high = pack_edges(grads, above, below)
        left, right = from_columns(to_low, to_high)
        up = upstream(k, slab, left, right, kernel, up, F32 if k else BF16)
    copies = call(merge_body, [((32, 8, 2 * WIRE), BF16)], 2, 5_000_000)(*pieces)[0]
    whole = lax.all_to_all(copies, SPACE, 0, 0, tiled=True)
    mate = swapped(whole, "core")
    grad_in, grad_out = finish(place, whole, mate)
    grad_taps, grad_channel, grad_bias = finish_small(whole, mate)
    return (
        current.reshape(slides.shape),
        up.reshape(slides.shape),
        grad_in,
        grad_out,
        jnp.transpose(grad_taps, (2, 0, 1, 3)),
        jnp.transpose(grad_channel, (1, 0, 2)),
        grad_bias,
    )


def solution(mesh):
    fine = jax.sharding.Mesh(
        mesh.devices.reshape(2, 4, 2, 4, 2), ("xh", "y", "core", "z", "dp")
    )
    maps = P("dp", RANKS, "z", None)
    split_in, split_out = P(None, "dp", None), P(None, None, "dp")
    whole = P()
    return jax.shard_map(
        per_device,
        mesh=fine,
        in_specs=(
            maps, maps, whole, whole, whole, whole, split_in, whole, split_out, whole, whole,
        ),
        out_specs=(maps, maps, split_in, split_out, whole, whole, whole),
        check_vma=False,
    )
```

```python
import functools

import jax
import jax.numpy as jnp
from jax import lax
from jax.experimental import pallas as pl
from jax.experimental.pallas import tpu as pltpu
from jax.sharding import PartitionSpec as P

COEF = 0.7978845608028654
CUBIC = 0.044715
EPSILON = 1e-06

PIX = 512
CH = 512
FF = 2048
HALF = 1024
WIRE = FF + 128
ROWS, COLS = 16, 32
WIDE = 40
DEEP = 14
SLAB = DEEP * WIDE * 8
SPACE = ("xh", "y", "z")
F32, BF16 = jnp.float32, jnp.bfloat16

VM = pl.BlockSpec(memory_space=pltpu.VMEM)
SM = pl.BlockSpec(memory_space=pltpu.SMEM)


FAR = pl.BlockSpec(memory_space=pltpu.HBM)
DMA = pltpu.SemaphoreType.DMA


def call(body, outs, count, flops, scratch=(), scalars=0, grant=5, far=(), far_out=()):
    shapes = [
        pltpu.HBM(s, d) if n in far_out else jax.ShapeDtypeStruct(s, d)
        for n, (s, d) in enumerate(outs)
    ]
    made = pl.pallas_call(
        body,
        out_shape=shapes,
        in_specs=[
            SM if n < scalars else FAR if n in far else VM for n in range(count)
        ],
        out_specs=[FAR if n in far_out else VM for n in range(len(outs))],
        scratch_shapes=list(scratch),
        compiler_params=pltpu.CompilerParams(vmem_limit_bytes=grant * 1024 * 1024),
        cost_estimate=pl.CostEstimate(
            flops=flops, bytes_accessed=4_000_000, transcendentals=0
        ),
    )

    def run(*args):
        return made(
            *(
                pltpu.with_memory_space_constraint(arg, pltpu.HBM) if n in far else arg
                for n, arg in enumerate(args)
            )
        )

    return run


def started(source, target, sem):
    copy = pltpu.make_async_copy(source, target, sem)
    copy.start()
    return copy


def at(row, col):
    return (row * WIDE + col) * 8


def homes(row):
    found = []
    if row < DEEP:
        found.append((0, row))
    if row >= 8:
        found.append((1, row - 8))
    return found


def put_row(slab, row, line):
    for block, inner in homes(row):
        for group in range(4):
            slab[pl.ds(at(inner, 3) + block * 4 + group, COLS, stride=8), :] = line[
                :, group * 128 : (group + 1) * 128
            ]


def either(odd, a, b):
    return jnp.where(odd == 1, a, b)


def put_edges(slab, odd, near, far):
    for n in range(3):
        a = near[n * COLS : (n + 1) * COLS, :].astype(F32)
        b = far[n * COLS : (n + 1) * COLS, :].astype(F32)
        put_row(slab, n, either(odd, a, b))
        put_row(slab, 19 + n, either(odd, b, a))


def put_columns(slab, odd, near, far):
    for row in range(DEEP):
        a = near[row * 24 : (row + 1) * 24, :].astype(F32)
        b = far[row * 24 : (row + 1) * 24, :].astype(F32)
        slab[pl.ds(at(row, 0), 24), :] = either(odd, a, b)
        slab[pl.ds(at(row, 35), 24), :] = either(odd, b, a)


def give_columns(row, odd, low, high, near, far):
    near[row * 24 : (row + 1) * 24, :] = either(odd, low, high).astype(BF16)
    far[row * 24 : (row + 1) * 24, :] = either(odd, high, low).astype(BF16)


def spread(kernel, k, taps):
    for tap in range(49):
        line = kernel[tap // 7, tap % 7, k : k + 1, :]
        for part in range(8):
            group = part % 4
            taps[tap * 8 + part : tap * 8 + part + 1, :] = line[
                :, group * 128 : (group + 1) * 128
            ]


def filtered(slab, taps, store, turned):
    def step(n, carry):
        row = n // 4
        col = (n % 4) * 8
        sums = [None] * 8
        for p in range(7):
            base = pl.multiple_of(((row + p) * WIDE + col) * 8, 8)
            seen = [slab[pl.ds(base + 8 * k, 8), :] for k in range(14)]
            for q in range(7):
                tap = 48 - p * 7 - q if turned else p * 7 + q
                weight = taps[tap * 8 : tap * 8 + 8, :]
                for m in range(8):
                    term = seen[m + q] * weight
                    sums[m] = term if sums[m] is None else sums[m] + term
        base = pl.multiple_of((row * COLS + col) * 8, 8)
        for m in range(8):
            store[pl.ds(base + 8 * m, 8), :] = sums[m]
        return carry

    lax.fori_loop(0, 32, step, 0)


def line_of(store, row):
    block, inner = row // 8, row % 8
    return jnp.concatenate(
        [
            store[pl.ds(inner * COLS * 8 + block * 4 + group, COLS, stride=8), :]
            for group in range(4)
        ],
        axis=1,
    )


def strips_body(place, x, near, far):
    odd = place[0]
    near[...] = x[pl.ds(pl.multiple_of((1 - odd) * 416, 32), 96), :]
    far[...] = x[pl.ds(pl.multiple_of(odd * 416, 32), 96), :]


def pack_body(place, x, edge_near, edge_far, slab, near, far):
    for row in range(ROWS):
        put_row(slab, row + 3, x[row * COLS : (row + 1) * COLS, :].astype(F32))
    put_edges(slab, place[0], edge_near, edge_far)
    for row in range(DEEP):
        give_columns(
            row, place[3], slab[pl.ds(at(row, 3), 24), :], slab[pl.ds(at(row, 32), 24), :],
            near, far,
        )


def edge_body(place, slab, edge_near, edge_far, near, far, rim):
    put_edges(rim, place[0], edge_near, edge_far)
    upper = lax.broadcasted_iota(jnp.int32, (24, 128), 0) % 8 < 4
    for row in range(DEEP):
        found = []
        for col in (3, 32):
            value = slab[pl.ds(at(row, col), 24), :]
            if row < 3:
                value = jnp.where(upper, rim[pl.ds(at(row, col), 24), :], value)
            if row >= 11:
                value = jnp.where(upper, value, rim[pl.ds(at(row, col), 24), :])
            found.append(value)
        give_columns(row, place[3], *found, near, far)


def norm_body(
    k, place, old, near, far, kernel, bias, gain, shift, slab, normal, normed, rstd, store, taps
):
    one = slice(k, k + 1)
    spread(kernel, k, taps)
    slab[...] = old[...]
    put_columns(slab, place[3], near, far)
    filtered(slab, taps, store, False)
    for row in range(ROWS):
        a, b = row * COLS, (row + 1) * COLS
        mixed = line_of(store, row) + bias[one, :]
        center = mixed - jnp.mean(mixed, -1, keepdims=True)
        scale = lax.rsqrt(jnp.mean(center * center, -1, keepdims=True) + EPSILON)
        value = center * scale
        normed[a:b, :] = value
        rstd[a:b, :] = jnp.broadcast_to(scale, (COLS, 128))
        normal[a:b, :] = (value * gain[one, :] + shift[one, :]).astype(BF16)


def mlp_body(k, far, *refs):
    (
        place, a, normal, own_in, got_in, mate_in, own_out, got_out, mate_out,
        bias_in, bias_out, scale, out, edge_near, edge_far,
    ) = refs[:15]
    kept = refs[15:20]
    act, slope, branch, full_in, full_out = refs[20:25] if far else kept
    sems = refs[-1]
    copies = []

    def leave(which, span=slice(None)):
        if far:
            source = refs[20 + which].at[:, span] if span != slice(None) else refs[20 + which]
            target = kept[which].at[:, span] if span != slice(None) else kept[which]
            copies.append(started(source, target, sems.at[len(copies)]))

    one = slice(k, k + 1)
    core, part = place[0], place[1]
    mine = pl.multiple_of(part * 256, 256)
    theirs = pl.multiple_of((1 - part) * 256, 256)
    full_in[pl.ds(mine, 256), :] = own_in[k]
    full_in[pl.ds(pl.multiple_of(theirs + core * 128, 128), 128), :] = got_in[0]
    full_in[pl.ds(pl.multiple_of(theirs + (1 - core) * 128, 128), 128), :] = mate_in[0]
    leave(3)
    full_out[:, pl.ds(mine, 256)] = own_out[k]
    full_out[pl.ds(pl.multiple_of(core * HALF, HALF), HALF), pl.ds(theirs, 256)] = got_out[0]
    full_out[pl.ds(pl.multiple_of((1 - core) * HALF, HALF), HALF), pl.ds(theirs, 256)] = mate_out[0]
    leave(4)
    for c in range(8):
        cols = slice(c * 256, (c + 1) * 256)
        hidden = jnp.dot(normal[...], full_in[:, cols], preferred_element_type=F32)
        v = hidden + bias_in[one, cols]
        square = v * v
        tangent = jnp.tanh(v * (COEF + (COEF * CUBIC) * square))
        half = 0.5 * v
        act[:, cols] = (half + half * tangent).astype(BF16)
        slope[:, cols] = (
            0.5
            + 0.5 * tangent
            + half * (1.0 - tangent * tangent) * (COEF + (3.0 * COEF * CUBIC) * square)
        ).astype(BF16)
        if c % 2:
            leave(0, slice(c * 256 - 256, c * 256 + 256))
            leave(1, slice(c * 256 - 256, c * 256 + 256))
    for c in range(2):
        cols = slice(c * 256, (c + 1) * 256)
        value = jnp.dot(act[...], full_out[:, cols], preferred_element_type=F32)
        value = value + bias_out[one, cols]
        branch[:, cols] = value
        leave(2, cols)
        result = (a[:, cols].astype(F32) + scale[one, cols] * value).astype(BF16)
        out[:, cols] = result
        edge_near[:, cols] = either(core, result[:96, :], result[416:, :])
        edge_far[:, cols] = either(core, result[416:, :], result[:96, :])
    for copy in copies:
        copy.wait()


def back_body(
    k, place, u, branch, slope, normed, rstd, full_in, full_out, gain, scale,
    low, gh, slab, edge_near, edge_far, channel, bias, gn, rim,
):
    one = slice(k, k + 1)
    cols_last = (((1,), (1,)), ((), ()))
    up = u[...].astype(F32)
    channel[4:5, :] = jnp.sum(up * branch[...], 0, keepdims=True)
    gb = up * scale[one, :]
    channel[3:4, :] = jnp.sum(gb, 0, keepdims=True)
    low[...] = gb.astype(BF16)
    for c in range(8):
        cols = slice(c * 256, (c + 1) * 256)
        ga = lax.dot_general(
            low[...], full_out[cols, :], cols_last, preferred_element_type=F32
        )
        value = ga * slope[:, cols].astype(F32)
        bias[:, cols] = jnp.sum(value, 0, keepdims=True)
        gh[:, cols] = value.astype(BF16)
    for c in range(2):
        cols = slice(c * 256, (c + 1) * 256)
        gn[:, cols] = lax.dot_general(
            gh[...], full_in[cols, :], cols_last, preferred_element_type=F32
        )
    sums = [jnp.zeros((8, CH), F32) for _ in range(3)]

    def folded(value):
        return value[0:8] + value[8:16] + value[16:24] + value[24:32]

    for row in range(ROWS):
        a, b = row * COLS, (row + 1) * COLS
        grad = gn[a:b, :]
        value = normed[a:b, :]
        sums[1] += folded(grad * value)
        sums[2] += folded(grad)
        gs = grad * gain[one, :]
        gm = rstd[a:b, 0:1] * (
            gs
            - jnp.mean(gs, -1, keepdims=True)
            - value * jnp.mean(gs * value, -1, keepdims=True)
        )
        sums[0] += folded(gm)
        put_row(slab, row + 3, gm)
        if row < 3:
            rim[1 - place[0], a:b, :] = gm.astype(BF16)
        if row >= 13:
            rim[place[0], a - 416 : b - 416, :] = gm.astype(BF16)
    edge_near[...] = rim[0]
    edge_far[...] = rim[1]
    for n in range(3):
        channel[n : n + 1, :] = jnp.sum(sums[n], 0, keepdims=True)


def grads_body(place, normal, low, act, gh, keep, give):
    core = place[0]
    rows_first = (((0,), (0,)), ((), ()))
    for side, ref in ((1 - core, give), (core, keep)):
        for c in range(4):
            cols = pl.ds(pl.multiple_of(side * HALF + c * 256, 256), 256)
            ref[:, c * 256 : (c + 1) * 256] = lax.dot_general(
                normal[...], gh[:, cols], rows_first, preferred_element_type=F32
            ).astype(BF16)
            ref[:, HALF + c * 256 : HALF + (c + 1) * 256] = lax.dot_general(
                low[...], act[:, cols], rows_first, preferred_element_type=F32
            ).astype(BF16)


def taps_body(seen, grads, out):
    for p in range(7):

        def step(n, sums, p=p):
            row = n // 4
            col = (n % 4) * 8
            base = pl.multiple_of(((row + p) * WIDE + col) * 8, 8)
            home = pl.multiple_of(((row + 3) * WIDE + col + 3) * 8, 8)
            near = [seen[pl.ds(base + 8 * k, 8), :] for k in range(14)]
            sums = list(sums)
            for m in range(8):
                grad = grads[pl.ds(home + 8 * m, 8), :]
                for q in range(7):
                    sums[q] = sums[q] + near[m + q] * grad
            return tuple(sums)

        sums = lax.fori_loop(0, 32, step, tuple(jnp.zeros((8, 128), F32) for _ in range(7)))
        for q in range(7):
            out[(p * 7 + q) * 4 : (p * 7 + q + 1) * 4, :] = sums[q][0:4] + sums[q][4:8]


def up_body(
    k, count, place, old, edge_near, edge_far, near, far, kernel, u, *refs
):
    later, out, brought = refs[:count], refs[count], refs[count + 1 : 2 * count + 1]
    slab, store, taps, strips, edges, base, sems = refs[2 * count + 1 :]
    whole = started(old, slab, sems.at[0])
    copies = [
        started(edge_near, edges.at[0], sems.at[1]),
        started(edge_far, edges.at[1], sems.at[2]),
        started(near, strips.at[0], sems.at[3]),
        started(far, strips.at[1], sems.at[4]),
    ]
    last = started(u, base, sems.at[5])
    coming = [started(later[n], brought[n], sems.at[6 + n]) for n in range(count)]
    spread(kernel, k, taps)
    whole.wait()
    for copy in copies:
        copy.wait()
    put_edges(slab, place[0], edges.at[0], edges.at[1])
    put_columns(slab, place[3], strips.at[0], strips.at[1])
    filtered(slab, taps, store, True)
    last.wait()
    for row in range(ROWS):
        a, b = row * COLS, (row + 1) * COLS
        out[a:b, :] = (base[a:b, :].astype(F32) + line_of(store, row)).astype(out.dtype)
    for copy in coming:
        copy.wait()


def pair_body(keep, got, taps, channel, bias, far, out, lines, sems):
    lines[0:196, :] = taps[...]
    spot = 196
    for kind in range(5):
        for group in range(4):
            lines[spot : spot + 1, :] = channel[
                kind : kind + 1, group * 128 : (group + 1) * 128
            ]
            spot += 1
    for group in range(16):
        lines[spot : spot + 1, :] = bias[:, group * 128 : (group + 1) * 128]
        spot += 1
    lines[spot:256, :] = jnp.zeros((256 - spot, 128), F32)

    def step(n, carry):
        rows = pl.ds(pl.multiple_of(n * 32, 32), 32)
        total = keep[rows, :].astype(F32) + got[rows, :].astype(F32)
        out[pl.ds(n * 4, 4), :, :FF] = total.reshape(4, 8, FF).astype(BF16)
        rows = pl.ds(pl.multiple_of((n % 8) * 32, 32), 32)
        out[pl.ds(n * 4, 4), :, FF:] = lines[rows, :].reshape(4, 8, 128).astype(BF16)
        return carry

    copies = []
    for part in range(4):
        lax.fori_loop(part * 4, part * 4 + 4, step, 0)
        span = pl.ds(part * 16, 16)
        copies.append(started(out.at[span], far.at[span], sems.at[part]))
    for copy in copies:
        copy.wait()


def total_body(pieces, out):
    for a, b in ((0, 512), (512, 1024), (1024, 1536), (1536, WIRE)):

        def step(n, total, a=a, b=b):
            for m in range(4):
                total = total + pieces[n * 4 + m, :, a:b].astype(F32)
            return total

        total = lax.fori_loop(0, 16, step, jnp.zeros((8, b - a), F32))
        out[:, a:b] = total.astype(BF16)


def merge_body(other, pieces, far, out, sums, sems):
    total_body(pieces, sums)
    copies = []
    for part in range(4):
        for n in range(part * 8, part * 8 + 8):
            out[n, :, :WIRE] = sums[...]
            out[n, :, WIRE:] = other[...]
        span = pl.ds(part * 8, 8)
        copies.append(started(out.at[span], far.at[span], sems.at[part]))
    for copy in copies:
        copy.wait()


def small_body(whole0, whole1, mate0, mate1, taps, channel, bias, lines):
    for k, whole, mate in ((0, whole0, mate0), (1, whole1, mate1)):
        lines[0:256, :] = (whole[...].astype(F32) + mate[...].astype(F32)).reshape(256, 128)
        for group in range(4):
            cols = slice(group * 128, (group + 1) * 128)
            for tap in range(49):
                line = tap * 4 + group
                taps[tap // 7, tap % 7, k : k + 1, cols] = lines[line : line + 1, :]
            for kind in range(5):
                line = 196 + kind * 4 + group
                channel[kind, k : k + 1, cols] = lines[line : line + 1, :]
        for group in range(16):
            bias[k : k + 1, group * 128 : (group + 1) * 128] = lines[216 + group : 217 + group, :]


def finish_body(place, ref, *refs):
    grad_in, grad_out = refs[-2:]
    value = ref[:, :, :FF].astype(F32).reshape(128, FF)
    grad_in[0] = value[:, :HALF]
    grad_out[0] = value[:, HALF:].T


STORE = pltpu.VMEM((ROWS * COLS * 4 + 16, 128), F32)
TAPS = pltpu.VMEM((400, 128), F32)
STRIP = ((DEEP * 24, 128), BF16)
EDGE = ((96, CH), BF16)


def edge_strips(place, x):
    return call(strips_body, [EDGE, EDGE], 2, 1_000_000, scalars=1)(place, x)


def pack(place, x, near, far):
    outs = [((SLAB, 128), F32), STRIP, STRIP]
    return call(pack_body, outs, 4, 10_000_000, scalars=1)(place, x, near, far)


def pack_edges(place, slab, near, far):
    scratch = [pltpu.VMEM((SLAB, 128), F32)]
    return call(edge_body, [STRIP, STRIP], 4, 10_000_000, scratch, scalars=1)(
        place, slab, near, far
    )


def normalise(k, place, slab, near, far, kernel, bias, gain, shift):
    outs = [((SLAB, 128), F32), ((PIX, CH), BF16), ((PIX, CH), F32), ((PIX, 128), F32)]
    return call(
        functools.partial(norm_body, k), outs, 8, 40_000_000, [STORE, TAPS], scalars=1
    )(place, slab, near, far, kernel, bias, gain, shift)


def mlp(k, place, a, normal, weights, bias_in, bias_out, scale):
    kept = [
        ((PIX, FF), BF16), ((PIX, FF), BF16), ((PIX, CH), F32), ((CH, FF), BF16), ((FF, CH), BF16),
    ]
    outs = [((PIX, CH), BF16), EDGE, EDGE, *kept]
    far = k == 0
    scratch = [*(pltpu.VMEM(s, d) for s, d in kept), DMA((12,))] if far else [DMA((1,))]
    return call(
        functools.partial(mlp_body, k, far), outs, 12, 60_000_000, scratch, scalars=1,
        grant=14 if far else 5, far_out=range(3, 8) if far else (),
    )(place, a, normal, *weights, bias_in, bias_out, scale)


def backward(k, place, u, saved, gain, scale):
    outs = [
        ((PIX, CH), BF16), ((PIX, FF), BF16), ((SLAB, 128), F32), EDGE, EDGE,
        ((8, CH), F32), ((1, FF), F32),
    ]
    scratch = [pltpu.VMEM((PIX, CH), F32), pltpu.VMEM((2, *EDGE[0]), BF16)]
    return call(
        functools.partial(back_body, k), outs, 10, 60_000_000, scratch, scalars=1
    )(place, u, *saved, gain, scale)


def weight_grads(place, normal, low, act, gh):
    outs = [((CH, FF), BF16), ((CH, FF), BF16)]
    return call(grads_body, outs, 5, 50_000_000, scalars=1)(place, normal, low, act, gh)


def tap_grads(seen, grads):
    return call(taps_body, [((49 * 4, 128), F32)], 2, 40_000_000)(seen, grads)[0]


def upstream(k, place, slab, edge_near, edge_far, near, far, kernel, u, dtype, later=()):
    scratch = [
        pltpu.VMEM((SLAB, 128), F32), STORE, TAPS,
        pltpu.VMEM((2, *STRIP[0]), BF16), pltpu.VMEM((2, *EDGE[0]), BF16),
        pltpu.VMEM((PIX, CH), u.dtype), DMA((6 + len(later),)),
    ]
    outs = [((PIX, CH), dtype), *((x.shape, x.dtype) for x in later)]
    return call(
        functools.partial(up_body, k, len(later)), outs, 8 + len(later), 40_000_000, scratch,
        grant=8, far=(1, 2, 3, 4, 5, 7, *range(8, 8 + len(later))), scalars=1,
    )(place, slab, edge_near, edge_far, near, far, kernel, u, *later)


def finish(place, side, value, buffers):
    held = [pl.BlockSpec(memory_space=pl.ANY)] * len(buffers)
    return pl.pallas_call(
        finish_body,
        grid_spec=pltpu.PrefetchScalarGridSpec(
            num_scalar_prefetch=1,
            grid=(2, 2),
            in_specs=[pl.BlockSpec((16, 8, WIRE), lambda layer, i, s: (i, 0, layer)), *held],
            out_specs=[
                pl.BlockSpec((1, 128, HALF), lambda layer, i, s: (layer, i, s[side])),
                pl.BlockSpec((1, HALF, 128), lambda layer, i, s: (layer, s[side], i)),
            ],
        ),
        out_shape=[
            jax.ShapeDtypeStruct((2, 256, FF), F32),
            jax.ShapeDtypeStruct((2, FF, 256), F32),
        ],
        input_output_aliases={2: 0, 3: 1} if buffers else {},
        compiler_params=pltpu.CompilerParams(vmem_limit_bytes=10 * 1024 * 1024),
        cost_estimate=pl.CostEstimate(
            flops=5_000_000, bytes_accessed=6_000_000, transcendentals=0
        ),
    )(place, value, *buffers)


def finish_small(whole, mate):
    first = pl.BlockSpec((32, 8, 128), lambda i: (0, 0, FF // 128))
    second = pl.BlockSpec((32, 8, 128), lambda i: (0, 0, (WIRE + FF) // 128))
    shapes = [(7, 7, 2, CH), (5, 2, CH), (2, FF)]
    return pl.pallas_call(
        small_body,
        grid=(1,),
        out_shape=[jax.ShapeDtypeStruct(s, F32) for s in shapes],
        in_specs=[first, second, first, second],
        out_specs=[
            pl.BlockSpec((7, 7, 2, CH), lambda i: (0, 0, 0, 0)),
            pl.BlockSpec((5, 2, CH), lambda i: (0, 0, 0)),
            pl.BlockSpec((2, FF), lambda i: (0, 0)),
        ],
        scratch_shapes=[pltpu.VMEM((256 + 8, 128), F32)],
        compiler_params=pltpu.CompilerParams(vmem_limit_bytes=4 * 1024 * 1024),
        cost_estimate=pl.CostEstimate(
            flops=1_000_000, bytes_accessed=1_000_000, transcendentals=0
        ),
    )(whole, whole, mate, mate)


RANKS = ("xh", "y", "core")


def pairs(first, count):
    found = [(i, i + 1) for i in range(first, count - 1, 2)]
    return found + [(b, a) for a, b in found]


def from_rows(near, far):
    near = lax.ppermute(near, RANKS, pairs(0, 16))
    far = lax.ppermute(far, RANKS, pairs(1, 16))
    return near, far


def from_columns(near, far):
    near = lax.ppermute(near, "z", pairs(0, 4))
    far = lax.ppermute(far, "z", pairs(1, 4))
    return near, far


def swapped(value, axis):
    return lax.ppermute(value, axis, [(0, 1), (1, 0)])


def around_x(value, step):
    return lax.ppermute(value, ("xh", "dp"), [(i, (i + step) % 4) for i in range(4)])


def fetch_weights(core, weight_in, weight_out, k):
    half_in = lax.dynamic_slice(weight_in, (k, core * 128, 0), (1, 128, FF))
    half_out = lax.dynamic_slice(weight_out, (k, core * HALF, 0), (1, HALF, 256))
    got_in = around_x(half_in, 1)
    got_out = around_x(half_out, -1)
    mate_in = swapped(got_in, "core")
    mate_out = swapped(got_out, "core")
    return weight_in, got_in, mate_in, weight_out, got_out, mate_out


def send_grads(keep, got, taps, channel, bias):
    scratch = [pltpu.VMEM((64, 8, WIRE), BF16), pltpu.VMEM((256, 128), F32), DMA((4,))]
    pair = call(
        pair_body, [((64, 8, WIRE), BF16)], 5, 2_000_000, scratch, far_out=(0,)
    )(keep, got, taps, channel, bias)[0]
    return lax.all_to_all(pair, ("dp", *SPACE), 0, 0, tiled=True)


def per_device(
    slides,
    cotangent,
    kernel,
    kernel_bias,
    norm_gain,
    norm_bias,
    weight_in,
    bias_in,
    weight_out,
    bias_out,
    layer_scale,
):
    core, part = lax.axis_index("core"), lax.axis_index("dp")
    place = jnp.stack([core, part, 1 - core, lax.axis_index("z") % 2]).astype(jnp.int32)
    slides, place = lax.optimization_barrier((slides, place))
    kernel = jnp.transpose(kernel, (1, 2, 0, 3))
    current = slides.reshape(PIX, CH)
    edges = edge_strips(place, current)
    saved = []
    weights = [fetch_weights(core, weight_in, weight_out, k) for k in range(2)]
    for k in range(2):
        edges = from_rows(*edges)
        slab, *sides = pack(place, current, *edges)
        sides = from_columns(*sides)
        slab, normal, normed, rstd = normalise(
            k, place, slab, *sides, kernel, kernel_bias, norm_gain, norm_bias
        )
        current, *edges, act, slope, branch, full_in, full_out = mlp(
            k, place, current, normal, weights[k], bias_in, bias_out, layer_scale
        )
        saved.append((slab, act, normal, (branch, slope, normed, rstd, full_in, full_out)))
    up = cotangent.reshape(PIX, CH)
    pieces = [None] * 2
    for k in (1, 0):
        seen, act, normal, rest = saved[k]
        low, gh, grads, *edges, channel, bias = backward(k, place, up, rest, norm_gain, layer_scale)
        edges = from_rows(*edges)
        keep, give = weight_grads(place, normal, low, act, gh)
        got = swapped(give, "core")
        taps = tap_grads(seen, grads)
        pieces[k] = send_grads(keep, got, taps, channel, bias)
        sides = pack_edges(place, grads, *edges)
        sides = from_columns(*sides)
        later = saved[0][3] if k else ()
        up, *brought = upstream(
            k, place, grads, *edges, *sides, kernel, up, F32 if k else BF16, later
        )
        if k:
            saved[0] = (*saved[0][:3], brought)
    other = call(total_body, [((8, WIRE), BF16)], 1, 5_000_000)(pieces[1])[0]
    scratch = [
        pltpu.VMEM((32, 8, 2 * WIRE), BF16), pltpu.VMEM((8, WIRE), BF16), DMA((4,)),
    ]
    copies = call(
        merge_body, [((32, 8, 2 * WIRE), BF16)], 2, 5_000_000, scratch, grant=8, far_out=(0,)
    )(other, pieces[0])[0]
    whole = lax.all_to_all(copies, SPACE, 0, 0, tiled=True)
    mate = swapped(whole, "core")
    buffers = finish(place, 0, whole, ())
    grad_in, grad_out = finish(place, 2, mate, buffers)
    grad_taps, grad_channel, grad_bias = finish_small(whole, mate)
    return (
        current.reshape(slides.shape),
        up.reshape(slides.shape),
        grad_in,
        grad_out,
        jnp.transpose(grad_taps, (2, 0, 1, 3)),
        jnp.transpose(grad_channel, (1, 0, 2)),
        grad_bias,
    )


def solution(mesh):
    fine = jax.sharding.Mesh(
        mesh.devices.reshape(2, 4, 2, 4, 2), ("xh", "y", "core", "z", "dp")
    )
    maps = P("dp", RANKS, "z", None)
    split_in, split_out = P(None, "dp", None), P(None, None, "dp")
    whole = P()
    return jax.shard_map(
        per_device,
        mesh=fine,
        in_specs=(
            maps, maps, whole, whole, whole, whole, split_in, whole, split_out, whole, whole,
        ),
        out_specs=(maps, maps, split_in, split_out, whole, whole, whole),
        check_vma=False,
    )
```

```python
import functools

import jax
import jax.numpy as jnp
from jax import lax
from jax.experimental import pallas as pl
from jax.experimental.pallas import tpu as pltpu
from jax.sharding import PartitionSpec as P

COEF = 0.7978845608028654
CUBIC = 0.044715
EPSILON = 1e-06

PIX = 512
CH = 512
FF = 2048
HALF = 1024
WIRE = FF + 256
ROWS, COLS = 16, 32
WIDE = 40
DEEP = 14
SLAB = DEEP * WIDE * 8
SPACE = ("xh", "y", "z")
F32, BF16 = jnp.float32, jnp.bfloat16

VM = pl.BlockSpec(memory_space=pltpu.VMEM)
SM = pl.BlockSpec(memory_space=pltpu.SMEM)


FAR = pl.BlockSpec(memory_space=pltpu.HBM)
DMA = pltpu.SemaphoreType.DMA


def call(body, outs, count, flops, scratch=(), scalars=0, grant=5, far=(), far_out=()):
    shapes = [
        pltpu.HBM(s, d) if n in far_out else jax.ShapeDtypeStruct(s, d)
        for n, (s, d) in enumerate(outs)
    ]
    made = pl.pallas_call(
        body,
        out_shape=shapes,
        in_specs=[
            SM if n < scalars else FAR if n in far else VM for n in range(count)
        ],
        out_specs=[FAR if n in far_out else VM for n in range(len(outs))],
        scratch_shapes=list(scratch),
        compiler_params=pltpu.CompilerParams(vmem_limit_bytes=grant * 1024 * 1024),
        cost_estimate=pl.CostEstimate(
            flops=flops, bytes_accessed=4_000_000, transcendentals=0
        ),
    )

    def run(*args):
        return made(
            *(
                pltpu.with_memory_space_constraint(arg, pltpu.HBM) if n in far else arg
                for n, arg in enumerate(args)
            )
        )

    return run


def started(source, target, sem):
    copy = pltpu.make_async_copy(source, target, sem)
    copy.start()
    return copy


def at(row, col):
    return (row * WIDE + col) * 8


def homes(row):
    found = []
    if row < DEEP:
        found.append((0, row))
    if row >= 8:
        found.append((1, row - 8))
    return found


def put_row(slab, row, line):
    for block, inner in homes(row):
        for group in range(4):
            slab[pl.ds(at(inner, 3) + block * 4 + group, COLS, stride=8), :] = line[
                :, group * 128 : (group + 1) * 128
            ]


def either(odd, a, b):
    return jnp.where(odd == 1, a, b)


def put_edges(slab, odd, near, far):
    for n in range(3):
        a = near[n * COLS : (n + 1) * COLS, :].astype(F32)
        b = far[n * COLS : (n + 1) * COLS, :].astype(F32)
        put_row(slab, n, either(odd, a, b))
        put_row(slab, 19 + n, either(odd, b, a))


def put_columns(slab, odd, near, far):
    for row in range(DEEP):
        a = near[row * 24 : (row + 1) * 24, :].astype(F32)
        b = far[row * 24 : (row + 1) * 24, :].astype(F32)
        slab[pl.ds(at(row, 0), 24), :] = either(odd, a, b)
        slab[pl.ds(at(row, 35), 24), :] = either(odd, b, a)


def give_columns(row, odd, low, high, near, far):
    near[row * 24 : (row + 1) * 24, :] = either(odd, low, high).astype(BF16)
    far[row * 24 : (row + 1) * 24, :] = either(odd, high, low).astype(BF16)


def spread(kernel, k, taps):
    for tap in range(49):
        line = kernel[tap // 7, tap % 7, k : k + 1, :]
        for part in range(8):
            group = part % 4
            taps[tap * 8 + part : tap * 8 + part + 1, :] = line[
                :, group * 128 : (group + 1) * 128
            ]


def filtered(slab, taps, store, turned):
    def step(n, carry):
        row = n // 4
        col = (n % 4) * 8
        sums = [None] * 8
        for p in range(7):
            base = pl.multiple_of(((row + p) * WIDE + col) * 8, 8)
            seen = [slab[pl.ds(base + 8 * k, 8), :] for k in range(14)]
            for q in range(7):
                tap = 48 - p * 7 - q if turned else p * 7 + q
                weight = taps[tap * 8 : tap * 8 + 8, :]
                for m in range(8):
                    term = seen[m + q] * weight
                    sums[m] = term if sums[m] is None else sums[m] + term
        base = pl.multiple_of((row * COLS + col) * 8, 8)
        for m in range(8):
            store[pl.ds(base + 8 * m, 8), :] = sums[m]
        return carry

    lax.fori_loop(0, 32, step, 0)


def line_of(store, row):
    block, inner = row // 8, row % 8
    return jnp.concatenate(
        [
            store[pl.ds(inner * COLS * 8 + block * 4 + group, COLS, stride=8), :]
            for group in range(4)
        ],
        axis=1,
    )


def strips_body(place, x, near, far):
    odd = place[0]
    near[...] = x[pl.ds(pl.multiple_of((1 - odd) * 416, 32), 96), :]
    far[...] = x[pl.ds(pl.multiple_of(odd * 416, 32), 96), :]


def pack_body(place, x, edge_near, edge_far, slab, near, far):
    for row in range(ROWS):
        put_row(slab, row + 3, x[row * COLS : (row + 1) * COLS, :].astype(F32))
    put_edges(slab, place[0], edge_near, edge_far)
    for row in range(DEEP):
        give_columns(
            row, place[3], slab[pl.ds(at(row, 3), 24), :], slab[pl.ds(at(row, 32), 24), :],
            near, far,
        )


def edge_body(place, slab, edge_near, edge_far, near, far, rim):
    put_edges(rim, place[0], edge_near, edge_far)
    upper = lax.broadcasted_iota(jnp.int32, (24, 128), 0) % 8 < 4
    for row in range(DEEP):
        found = []
        for col in (3, 32):
            value = slab[pl.ds(at(row, col), 24), :]
            if row < 3:
                value = jnp.where(upper, rim[pl.ds(at(row, col), 24), :], value)
            if row >= 11:
                value = jnp.where(upper, value, rim[pl.ds(at(row, col), 24), :])
            found.append(value)
        give_columns(row, place[3], *found, near, far)


def norm_body(
    k, far, place, old, near, far_side, kernel, bias, gain, shift, slab, normal, normed, rstd,
    store, taps, *held,
):
    kept = slab, normed, rstd
    if far:
        slab, normed, rstd, sems = held
    one = slice(k, k + 1)
    spread(kernel, k, taps)
    slab[...] = old[...]
    put_columns(slab, place[3], near, far_side)
    copies = [started(slab, kept[0], sems.at[0])] if far else []
    filtered(slab, taps, store, False)
    for row in range(ROWS):
        a, b = row * COLS, (row + 1) * COLS
        mixed = line_of(store, row) + bias[one, :]
        center = mixed - jnp.mean(mixed, -1, keepdims=True)
        scale = lax.rsqrt(jnp.mean(center * center, -1, keepdims=True) + EPSILON)
        value = center * scale
        normed[a:b, :] = value
        rstd[a:b, :] = jnp.broadcast_to(scale, (COLS, 128))
        normal[a:b, :] = (value * gain[one, :] + shift[one, :]).astype(BF16)
        if far and row in (7, 15):
            span = pl.ds((row - 7) * COLS, 8 * COLS)
            half = row // 8
            copies.append(started(normed.at[span], kept[1].at[span], sems.at[1 + half]))
            copies.append(started(rstd.at[span], kept[2].at[span], sems.at[3 + half]))
    for copy in copies:
        copy.wait()


def mlp_body(k, far, *refs):
    (
        place, a, normal, own_in, got_in, mate_in, own_out, got_out, mate_out,
        bias_in, bias_out, scale, out, edge_near, edge_far,
    ) = refs[:15]
    kept = refs[15:20]
    act, slope, branch, full_in, full_out = refs[20:25] if far else kept
    sems = refs[-1]
    copies = []

    def leave(which, span=slice(None)):
        if far:
            source = refs[20 + which].at[:, span] if span != slice(None) else refs[20 + which]
            target = kept[which].at[:, span] if span != slice(None) else kept[which]
            copies.append(started(source, target, sems.at[len(copies)]))

    one = slice(k, k + 1)
    core, part = place[0], place[1]
    mine = pl.multiple_of(part * 256, 256)
    theirs = pl.multiple_of((1 - part) * 256, 256)
    full_in[pl.ds(mine, 256), :] = own_in[k]
    full_in[pl.ds(pl.multiple_of(theirs + core * 128, 128), 128), :] = got_in[0]
    full_in[pl.ds(pl.multiple_of(theirs + (1 - core) * 128, 128), 128), :] = mate_in[0]
    leave(3)
    full_out[:, pl.ds(mine, 256)] = own_out[k]
    full_out[pl.ds(pl.multiple_of(core * HALF, HALF), HALF), pl.ds(theirs, 256)] = got_out[0]
    full_out[pl.ds(pl.multiple_of((1 - core) * HALF, HALF), HALF), pl.ds(theirs, 256)] = mate_out[0]
    leave(4)
    for c in range(8):
        cols = slice(c * 256, (c + 1) * 256)
        hidden = jnp.dot(normal[...], full_in[:, cols], preferred_element_type=F32)
        v = hidden + bias_in[one, cols]
        square = v * v
        tangent = jnp.tanh(v * (COEF + (COEF * CUBIC) * square))
        half = 0.5 * v
        act[:, cols] = (half + half * tangent).astype(BF16)
        slope[:, cols] = (
            0.5
            + 0.5 * tangent
            + half * (1.0 - tangent * tangent) * (COEF + (3.0 * COEF * CUBIC) * square)
        ).astype(BF16)
        if c % 2:
            leave(0, slice(c * 256 - 256, c * 256 + 256))
            leave(1, slice(c * 256 - 256, c * 256 + 256))
    for c in range(2):
        cols = slice(c * 256, (c + 1) * 256)
        value = jnp.dot(act[...], full_out[:, cols], preferred_element_type=F32)
        value = value + bias_out[one, cols]
        branch[:, cols] = value
        leave(2, cols)
        result = (a[:, cols].astype(F32) + scale[one, cols] * value).astype(BF16)
        out[:, cols] = result
        edge_near[:, cols] = either(core, result[:96, :], result[416:, :])
        edge_far[:, cols] = either(core, result[416:, :], result[:96, :])
    for copy in copies:
        copy.wait()


def back_body(
    k, place, u, branch, slope, normed, rstd, full_in, full_out, gain, scale,
    low, gh, slab, edge_near, edge_far, channel, bias, gn, rim,
):
    one = slice(k, k + 1)
    cols_last = (((1,), (1,)), ((), ()))
    up = u[...].astype(F32)
    channel[4:5, :] = jnp.sum(up * branch[...], 0, keepdims=True)
    gb = up * scale[one, :]
    channel[3:4, :] = jnp.sum(gb, 0, keepdims=True)
    low[...] = gb.astype(BF16)
    for c in range(8):
        cols = slice(c * 256, (c + 1) * 256)
        ga = lax.dot_general(
            low[...], full_out[cols, :], cols_last, preferred_element_type=F32
        )
        value = ga * slope[:, cols].astype(F32)
        bias[:, cols] = jnp.sum(value, 0, keepdims=True)
        gh[:, cols] = value.astype(BF16)
    for c in range(2):
        cols = slice(c * 256, (c + 1) * 256)
        gn[:, cols] = lax.dot_general(
            gh[...], full_in[cols, :], cols_last, preferred_element_type=F32
        )
    sums = [jnp.zeros((8, CH), F32) for _ in range(3)]

    def folded(value):
        return value[0:8] + value[8:16] + value[16:24] + value[24:32]

    for row in range(ROWS):
        a, b = row * COLS, (row + 1) * COLS
        grad = gn[a:b, :]
        value = normed[a:b, :]
        sums[1] += folded(grad * value)
        sums[2] += folded(grad)
        gs = grad * gain[one, :]
        gm = rstd[a:b, 0:1] * (
            gs
            - jnp.mean(gs, -1, keepdims=True)
            - value * jnp.mean(gs * value, -1, keepdims=True)
        )
        sums[0] += folded(gm)
        put_row(slab, row + 3, gm)
        if row < 3:
            rim[1 - place[0], a:b, :] = gm.astype(BF16)
        if row >= 13:
            rim[place[0], a - 416 : b - 416, :] = gm.astype(BF16)
    edge_near[...] = rim[0]
    edge_far[...] = rim[1]
    for n in range(3):
        channel[n : n + 1, :] = jnp.sum(sums[n], 0, keepdims=True)


def grads_body(place, normal, low, act, gh, keep, give):
    core = place[0]
    rows_first = (((0,), (0,)), ((), ()))
    for side, ref in ((1 - core, give), (core, keep)):
        for c in range(4):
            cols = pl.ds(pl.multiple_of(side * HALF + c * 256, 256), 256)
            ref[:, c * 256 : (c + 1) * 256] = lax.dot_general(
                normal[...], gh[:, cols], rows_first, preferred_element_type=F32
            ).astype(BF16)
            ref[:, HALF + c * 256 : HALF + (c + 1) * 256] = lax.dot_general(
                low[...], act[:, cols], rows_first, preferred_element_type=F32
            ).astype(BF16)


def taps_body(seen, grads, out):
    for p in range(7):

        def step(n, sums, p=p):
            row = n // 4
            col = (n % 4) * 8
            base = pl.multiple_of(((row + p) * WIDE + col) * 8, 8)
            home = pl.multiple_of(((row + 3) * WIDE + col + 3) * 8, 8)
            near = [seen[pl.ds(base + 8 * k, 8), :] for k in range(14)]
            sums = list(sums)
            for m in range(8):
                grad = grads[pl.ds(home + 8 * m, 8), :]
                for q in range(7):
                    sums[q] = sums[q] + near[m + q] * grad
            return tuple(sums)

        sums = lax.fori_loop(0, 32, step, tuple(jnp.zeros((8, 128), F32) for _ in range(7)))
        for q in range(7):
            out[(p * 7 + q) * 4 : (p * 7 + q + 1) * 4, :] = sums[q][0:4] + sums[q][4:8]


def up_body(
    k, count, place, old, edge_near, edge_far, near, far, kernel, u, *refs
):
    later, out, brought = refs[:count], refs[count], refs[count + 1 : 2 * count + 1]
    slab, store, taps, strips, edges, base, sems = refs[2 * count + 1 :]
    whole = started(old, slab, sems.at[0])
    copies = [
        started(edge_near, edges.at[0], sems.at[1]),
        started(edge_far, edges.at[1], sems.at[2]),
        started(near, strips.at[0], sems.at[3]),
        started(far, strips.at[1], sems.at[4]),
    ]
    last = started(u, base, sems.at[5])
    coming = [started(later[n], brought[n], sems.at[6 + n]) for n in range(count)]
    spread(kernel, k, taps)
    whole.wait()
    for copy in copies:
        copy.wait()
    put_edges(slab, place[0], edges.at[0], edges.at[1])
    put_columns(slab, place[3], strips.at[0], strips.at[1])
    filtered(slab, taps, store, True)
    last.wait()
    for row in range(ROWS):
        a, b = row * COLS, (row + 1) * COLS
        out[a:b, :] = (base[a:b, :].astype(F32) + line_of(store, row)).astype(out.dtype)
    for copy in coming:
        copy.wait()


def pair_body(count, keep, got, *refs):
    parts, (far, out, *lines), sems = refs[: 3 * count], refs[3 * count : -1], refs[-1]
    for n in range(count):
        taps, channel, bias = parts[3 * n : 3 * n + 3]
        ref = lines[n]
        ref[0:196, :] = taps[...]
        spot = 196
        for kind in range(5):
            for group in range(4):
                ref[spot : spot + 1, :] = channel[
                    kind : kind + 1, group * 128 : (group + 1) * 128
                ]
                spot += 1
        for group in range(16):
            ref[spot : spot + 1, :] = bias[:, group * 128 : (group + 1) * 128]
            spot += 1
        ref[spot:256, :] = jnp.zeros((256 - spot, 128), F32)

    def step(n, carry):
        rows = pl.ds(pl.multiple_of(n * 32, 32), 32)
        total = keep[rows, :].astype(F32) + got[rows, :].astype(F32)
        out[pl.ds(n * 4, 4), :, :FF] = total.reshape(4, 8, FF).astype(BF16)
        rows = pl.ds(pl.multiple_of((n % 8) * 32, 32), 32)
        for m in range(count):
            out[pl.ds(n * 4, 4), :, FF + m * 128 : FF + (m + 1) * 128] = (
                lines[m][rows, :].reshape(4, 8, 128).astype(BF16)
            )
        return carry

    copies = []
    for part in range(4):
        lax.fori_loop(part * 4, part * 4 + 4, step, 0)
        span = pl.ds(part * 16, 16)
        copies.append(started(out.at[span], far.at[span], sems.at[part]))
    for copy in copies:
        copy.wait()


def total_body(pieces, out):
    width = pieces.shape[2]
    for a in range(0, width, 512):
        b = min(a + 512, width)

        def step(n, total, a=a, b=b):
            for m in range(4):
                total = total + pieces[n * 4 + m, :, a:b].astype(F32)
            return total

        total = lax.fori_loop(0, 16, step, jnp.zeros((8, b - a), F32))
        out[:, a:b] = total.astype(BF16)


def merge_body(other, pieces, far, out, sums, sems):
    for n in range(32):
        out[n, :, FF : 2 * FF] = other[...]
    copies = [started(out.at[:, :, FF : 2 * FF], far.at[:, :, FF : 2 * FF], sems.at[0])]
    total_body(pieces, sums)
    for part in range(2):
        for n in range(part * 16, part * 16 + 16):
            out[n, :, :FF] = sums[:, :FF]
            out[n, :, 2 * FF :] = sums[:, FF:]
        span = pl.ds(part * 16, 16)
        for m, cols in enumerate((slice(0, FF), slice(2 * FF, 2 * FF + 256))):
            copies.append(
                started(out.at[span, :, cols], far.at[span, :, cols], sems.at[1 + part * 2 + m])
            )
    for copy in copies:
        copy.wait()


def small_body(whole0, whole1, mate0, mate1, taps, channel, bias, lines):
    for k, whole, mate in ((0, whole0, mate0), (1, whole1, mate1)):
        lines[0:256, :] = (whole[...].astype(F32) + mate[...].astype(F32)).reshape(256, 128)
        for group in range(4):
            cols = slice(group * 128, (group + 1) * 128)
            for tap in range(49):
                line = tap * 4 + group
                taps[tap // 7, tap % 7, k : k + 1, cols] = lines[line : line + 1, :]
            for kind in range(5):
                line = 196 + kind * 4 + group
                channel[kind, k : k + 1, cols] = lines[line : line + 1, :]
        for group in range(16):
            bias[k : k + 1, group * 128 : (group + 1) * 128] = lines[216 + group : 217 + group, :]


def finish_body(place, ref, *refs):
    grad_in, grad_out = refs[-2:]
    value = ref[...].astype(F32).reshape(128, FF)
    grad_in[0] = value[:, :HALF]
    grad_out[0] = value[:, HALF:].T


STORE = pltpu.VMEM((ROWS * COLS * 4 + 16, 128), F32)
TAPS = pltpu.VMEM((400, 128), F32)
STRIP = ((DEEP * 24, 128), BF16)
EDGE = ((96, CH), BF16)


def edge_strips(place, x):
    return call(strips_body, [EDGE, EDGE], 2, 1_000_000, scalars=1)(place, x)


def pack(place, x, near, far):
    outs = [((SLAB, 128), F32), STRIP, STRIP]
    return call(pack_body, outs, 4, 10_000_000, scalars=1)(place, x, near, far)


def pack_edges(place, slab, near, far):
    scratch = [pltpu.VMEM((SLAB, 128), F32)]
    return call(edge_body, [STRIP, STRIP], 4, 10_000_000, scratch, scalars=1)(
        place, slab, near, far
    )


def normalise(k, place, slab, near, far_side, kernel, bias, gain, shift):
    outs = [((SLAB, 128), F32), ((PIX, CH), BF16), ((PIX, CH), F32), ((PIX, 128), F32)]
    far = k == 0
    scratch = [STORE, TAPS]
    if far:
        scratch += [pltpu.VMEM(*outs[n]) for n in (0, 2, 3)] + [DMA((5,))]
    return call(
        functools.partial(norm_body, k, far), outs, 8, 40_000_000, scratch, scalars=1,
        grant=8 if far else 5, far_out=(0, 2, 3) if far else (),
    )(place, slab, near, far_side, kernel, bias, gain, shift)


def mlp(k, place, a, normal, weights, bias_in, bias_out, scale):
    kept = [
        ((PIX, FF), BF16), ((PIX, FF), BF16), ((PIX, CH), F32), ((CH, FF), BF16), ((FF, CH), BF16),
    ]
    outs = [((PIX, CH), BF16), EDGE, EDGE, *kept]
    far = k == 0
    scratch = [*(pltpu.VMEM(s, d) for s, d in kept), DMA((12,))] if far else [DMA((1,))]
    return call(
        functools.partial(mlp_body, k, far), outs, 12, 60_000_000, scratch, scalars=1,
        grant=14 if far else 5, far_out=range(3, 8) if far else (),
    )(place, a, normal, *weights, bias_in, bias_out, scale)


def backward(k, place, u, saved, gain, scale):
    outs = [
        ((PIX, CH), BF16), ((PIX, FF), BF16), ((SLAB, 128), F32), EDGE, EDGE,
        ((8, CH), F32), ((1, FF), F32),
    ]
    scratch = [pltpu.VMEM((PIX, CH), F32), pltpu.VMEM((2, *EDGE[0]), BF16)]
    return call(
        functools.partial(back_body, k), outs, 10, 60_000_000, scratch, scalars=1
    )(place, u, *saved, gain, scale)


def weight_grads(place, normal, low, act, gh):
    outs = [((CH, FF), BF16), ((CH, FF), BF16)]
    return call(grads_body, outs, 5, 50_000_000, scalars=1)(place, normal, low, act, gh)


def tap_grads(seen, grads):
    return call(taps_body, [((49 * 4, 128), F32)], 2, 40_000_000)(seen, grads)[0]


def upstream(k, place, slab, edge_near, edge_far, near, far, kernel, u, dtype, later=()):
    scratch = [
        pltpu.VMEM((SLAB, 128), F32), STORE, TAPS,
        pltpu.VMEM((2, *STRIP[0]), BF16), pltpu.VMEM((2, *EDGE[0]), BF16),
        pltpu.VMEM((PIX, CH), u.dtype), DMA((6 + len(later),)),
    ]
    outs = [((PIX, CH), dtype), *((x.shape, x.dtype) for x in later)]
    return call(
        functools.partial(up_body, k, len(later)), outs, 8 + len(later), 40_000_000, scratch,
        grant=8, far=(1, 2, 3, 4, 5, 7, *range(8, 8 + len(later))), scalars=1,
    )(place, slab, edge_near, edge_far, near, far, kernel, u, *later)


def finish(place, side, value, buffers):
    held = [pl.BlockSpec(memory_space=pl.ANY)] * len(buffers)
    return pl.pallas_call(
        finish_body,
        grid_spec=pltpu.PrefetchScalarGridSpec(
            num_scalar_prefetch=1,
            grid=(2, 2),
            in_specs=[pl.BlockSpec((16, 8, FF), lambda layer, i, s: (i, 0, layer)), *held],
            out_specs=[
                pl.BlockSpec((1, 128, HALF), lambda layer, i, s: (layer, i, s[side])),
                pl.BlockSpec((1, HALF, 128), lambda layer, i, s: (layer, s[side], i)),
            ],
        ),
        out_shape=[
            jax.ShapeDtypeStruct((2, 256, FF), F32),
            jax.ShapeDtypeStruct((2, FF, 256), F32),
        ],
        input_output_aliases={2: 0, 3: 1} if buffers else {},
        compiler_params=pltpu.CompilerParams(vmem_limit_bytes=10 * 1024 * 1024),
        cost_estimate=pl.CostEstimate(
            flops=5_000_000, bytes_accessed=6_000_000, transcendentals=0
        ),
    )(place, value, *buffers)


def finish_small(whole, mate):
    first = pl.BlockSpec((32, 8, 128), lambda i: (0, 0, 2 * FF // 128))
    second = pl.BlockSpec((32, 8, 128), lambda i: (0, 0, 2 * FF // 128 + 1))
    shapes = [(7, 7, 2, CH), (5, 2, CH), (2, FF)]
    return pl.pallas_call(
        small_body,
        grid=(1,),
        out_shape=[jax.ShapeDtypeStruct(s, F32) for s in shapes],
        in_specs=[first, second, first, second],
        out_specs=[
            pl.BlockSpec((7, 7, 2, CH), lambda i: (0, 0, 0, 0)),
            pl.BlockSpec((5, 2, CH), lambda i: (0, 0, 0)),
            pl.BlockSpec((2, FF), lambda i: (0, 0)),
        ],
        scratch_shapes=[pltpu.VMEM((256 + 8, 128), F32)],
        compiler_params=pltpu.CompilerParams(vmem_limit_bytes=4 * 1024 * 1024),
        cost_estimate=pl.CostEstimate(
            flops=1_000_000, bytes_accessed=1_000_000, transcendentals=0
        ),
    )(whole, whole, mate, mate)


RANKS = ("xh", "y", "core")


def pairs(first, count):
    found = [(i, i + 1) for i in range(first, count - 1, 2)]
    return found + [(b, a) for a, b in found]


def from_rows(near, far):
    near = lax.ppermute(near, RANKS, pairs(0, 16))
    far = lax.ppermute(far, RANKS, pairs(1, 16))
    return near, far


def from_columns(near, far):
    near = lax.ppermute(near, "z", pairs(0, 4))
    far = lax.ppermute(far, "z", pairs(1, 4))
    return near, far


def swapped(value, axis):
    return lax.ppermute(value, axis, [(0, 1), (1, 0)])


def around_x(value, step):
    return lax.ppermute(value, ("xh", "dp"), [(i, (i + step) % 4) for i in range(4)])


def fetch_weights(core, weight_in, weight_out, k):
    half_in = lax.dynamic_slice(weight_in, (k, core * 128, 0), (1, 128, FF))
    half_out = lax.dynamic_slice(weight_out, (k, core * HALF, 0), (1, HALF, 256))
    got_in = around_x(half_in, 1)
    got_out = around_x(half_out, -1)
    mate_in = swapped(got_in, "core")
    mate_out = swapped(got_out, "core")
    return weight_in, got_in, mate_in, weight_out, got_out, mate_out


def send_grads(keep, got, small):
    count = len(small) // 3
    shape = (64, 8, FF + 128 * count)
    scratch = [
        pltpu.VMEM(shape, BF16), *[pltpu.VMEM((256, 128), F32)] * count, DMA((4,)),
    ]
    pair = call(
        functools.partial(pair_body, count), [(shape, BF16)], 2 + len(small), 2_000_000,
        scratch, far_out=(0,),
    )(keep, got, *small)[0]
    return lax.all_to_all(pair, ("dp", *SPACE), 0, 0, tiled=True)


def per_device(
    slides,
    cotangent,
    kernel,
    kernel_bias,
    norm_gain,
    norm_bias,
    weight_in,
    bias_in,
    weight_out,
    bias_out,
    layer_scale,
):
    core, part = lax.axis_index("core"), lax.axis_index("dp")
    place = jnp.stack([core, part, 1 - core, lax.axis_index("z") % 2]).astype(jnp.int32)
    slides, place = lax.optimization_barrier((slides, place))
    kernel = jnp.transpose(kernel, (1, 2, 0, 3))
    current = slides.reshape(PIX, CH)
    edges = edge_strips(place, current)
    saved = []
    weights = [fetch_weights(core, weight_in, weight_out, k) for k in range(2)]
    for k in range(2):
        edges = from_rows(*edges)
        slab, *sides = pack(place, current, *edges)
        sides = from_columns(*sides)
        slab, normal, normed, rstd = normalise(
            k, place, slab, *sides, kernel, kernel_bias, norm_gain, norm_bias
        )
        current, *edges, act, slope, branch, full_in, full_out = mlp(
            k, place, current, normal, weights[k], bias_in, bias_out, layer_scale
        )
        saved.append((slab, act, normal, (branch, slope, normed, rstd, full_in, full_out)))
    up = cotangent.reshape(PIX, CH)
    pieces = [None] * 2
    small = []
    for k in (1, 0):
        seen, act, normal, rest = saved[k]
        low, gh, grads, *edges, channel, bias = backward(k, place, up, rest, norm_gain, layer_scale)
        edges = from_rows(*edges)
        keep, give = weight_grads(place, normal, low, act, gh)
        got = swapped(give, "core")
        taps = tap_grads(seen, grads)
        small = [taps, channel, bias, *small]
        pieces[k] = send_grads(keep, got, () if k else small)
        sides = pack_edges(place, grads, *edges)
        sides = from_columns(*sides)
        later = saved[0][3] if k else ()
        up, *brought = upstream(
            k, place, grads, *edges, *sides, kernel, up, F32 if k else BF16, later
        )
        if k:
            saved[0] = (*saved[0][:3], brought)
    other = call(total_body, [((8, FF), BF16)], 1, 5_000_000)(pieces[1])[0]
    scratch = [
        pltpu.VMEM((32, 8, FF + WIRE), BF16), pltpu.VMEM((8, WIRE), BF16), DMA((5,)),
    ]
    copies = call(
        merge_body, [((32, 8, FF + WIRE), BF16)], 2, 5_000_000, scratch, grant=8, far_out=(0,)
    )(other, pieces[0])[0]
    whole = lax.all_to_all(copies, SPACE, 0, 0, tiled=True)
    mate = swapped(whole, "core")
    buffers = finish(place, 0, whole, ())
    grad_in, grad_out = finish(place, 2, mate, buffers)
    grad_taps, grad_channel, grad_bias = finish_small(whole, mate)
    return (
        current.reshape(slides.shape),
        up.reshape(slides.shape),
        grad_in,
        grad_out,
        jnp.transpose(grad_taps, (2, 0, 1, 3)),
        jnp.transpose(grad_channel, (1, 0, 2)),
        grad_bias,
    )


def solution(mesh):
    fine = jax.sharding.Mesh(
        mesh.devices.reshape(2, 4, 2, 4, 2), ("xh", "y", "core", "z", "dp")
    )
    maps = P("dp", RANKS, "z", None)
    split_in, split_out = P(None, "dp", None), P(None, None, "dp")
    whole = P()
    return jax.shard_map(
        per_device,
        mesh=fine,
        in_specs=(
            maps, maps, whole, whole, whole, whole, split_in, whole, split_out, whole, whole,
        ),
        out_specs=(maps, maps, split_in, split_out, whole, whole, whole),
        check_vma=False,
    )
```

```python
import functools

import jax
import jax.numpy as jnp
from jax import lax
from jax.experimental import pallas as pl
from jax.experimental.pallas import tpu as pltpu
from jax.sharding import PartitionSpec as P

COEF = 0.7978845608028654
CUBIC = 0.044715
EPSILON = 1e-06

PIX = 512
CH = 512
FF = 2048
HALF = 1024
WIRE = FF + 256
ROWS, COLS = 16, 32
WIDE = 40
DEEP = 14
SLAB = DEEP * WIDE * 8
SPACE = ("xh", "y", "z")
F32, BF16 = jnp.float32, jnp.bfloat16

VM = pl.BlockSpec(memory_space=pltpu.VMEM)
SM = pl.BlockSpec(memory_space=pltpu.SMEM)


FAR = pl.BlockSpec(memory_space=pltpu.HBM)
DMA = pltpu.SemaphoreType.DMA


def call(body, outs, count, flops, scratch=(), scalars=0, grant=5, far=(), far_out=()):
    shapes = [
        pltpu.HBM(s, d) if n in far_out else jax.ShapeDtypeStruct(s, d)
        for n, (s, d) in enumerate(outs)
    ]
    made = pl.pallas_call(
        body,
        out_shape=shapes,
        in_specs=[
            SM if n < scalars else FAR if n in far else VM for n in range(count)
        ],
        out_specs=[FAR if n in far_out else VM for n in range(len(outs))],
        scratch_shapes=list(scratch),
        compiler_params=pltpu.CompilerParams(vmem_limit_bytes=grant * 1024 * 1024),
        cost_estimate=pl.CostEstimate(
            flops=flops, bytes_accessed=4_000_000, transcendentals=0
        ),
    )

    def run(*args):
        return made(
            *(
                pltpu.with_memory_space_constraint(arg, pltpu.HBM) if n in far else arg
                for n, arg in enumerate(args)
            )
        )

    return run


def started(source, target, sem):
    copy = pltpu.make_async_copy(source, target, sem)
    copy.start()
    return copy


def at(row, col):
    return (row * WIDE + col) * 8


def homes(row):
    found = []
    if row < DEEP:
        found.append((0, row))
    if row >= 8:
        found.append((1, row - 8))
    return found


def put_row(slab, row, line):
    for block, inner in homes(row):
        for group in range(4):
            slab[pl.ds(at(inner, 3) + block * 4 + group, COLS, stride=8), :] = line[
                :, group * 128 : (group + 1) * 128
            ]


def either(odd, a, b):
    return jnp.where(odd == 1, a, b)


def put_edges(slab, odd, near, far):
    for n in range(3):
        a = near[n * COLS : (n + 1) * COLS, :].astype(F32)
        b = far[n * COLS : (n + 1) * COLS, :].astype(F32)
        put_row(slab, n, either(odd, a, b))
        put_row(slab, 19 + n, either(odd, b, a))


def put_columns(slab, odd, near, far):
    for row in range(DEEP):
        a = near[row * 24 : (row + 1) * 24, :].astype(F32)
        b = far[row * 24 : (row + 1) * 24, :].astype(F32)
        slab[pl.ds(at(row, 0), 24), :] = either(odd, a, b)
        slab[pl.ds(at(row, 35), 24), :] = either(odd, b, a)


def give_columns(row, odd, low, high, near, far):
    near[row * 24 : (row + 1) * 24, :] = either(odd, low, high).astype(BF16)
    far[row * 24 : (row + 1) * 24, :] = either(odd, high, low).astype(BF16)


def spread(kernel, k, taps):
    for tap in range(49):
        line = kernel[tap // 7, tap % 7, k : k + 1, :]
        for part in range(8):
            group = part % 4
            taps[tap * 8 + part : tap * 8 + part + 1, :] = line[
                :, group * 128 : (group + 1) * 128
            ]


def filtered(slab, taps, store, turned):
    def step(n, carry):
        row = n // 4
        col = (n % 4) * 8
        sums = [None] * 8
        for p in range(7):
            base = pl.multiple_of(((row + p) * WIDE + col) * 8, 8)
            seen = [slab[pl.ds(base + 8 * k, 8), :] for k in range(14)]
            for q in range(7):
                tap = 48 - p * 7 - q if turned else p * 7 + q
                weight = taps[tap * 8 : tap * 8 + 8, :]
                for m in range(8):
                    term = seen[m + q] * weight
                    sums[m] = term if sums[m] is None else sums[m] + term
        base = pl.multiple_of((row * COLS + col) * 8, 8)
        for m in range(8):
            store[pl.ds(base + 8 * m, 8), :] = sums[m]
        return carry

    lax.fori_loop(0, 32, step, 0)


def line_of(store, row):
    block, inner = row // 8, row % 8
    return jnp.concatenate(
        [
            store[pl.ds(inner * COLS * 8 + block * 4 + group, COLS, stride=8), :]
            for group in range(4)
        ],
        axis=1,
    )


def strips_body(place, x, near, far):
    odd = place[0]
    near[...] = x[pl.ds(pl.multiple_of((1 - odd) * 416, 32), 96), :]
    far[...] = x[pl.ds(pl.multiple_of(odd * 416, 32), 96), :]


def pack_body(place, x, edge_near, edge_far, slab, near, far):
    for row in range(ROWS):
        put_row(slab, row + 3, x[row * COLS : (row + 1) * COLS, :].astype(F32))
    put_edges(slab, place[0], edge_near, edge_far)
    for row in range(DEEP):
        give_columns(
            row, place[3], slab[pl.ds(at(row, 3), 24), :], slab[pl.ds(at(row, 32), 24), :],
            near, far,
        )


def edge_body(place, slab, edge_near, edge_far, near, far, rim):
    put_edges(rim, place[0], edge_near, edge_far)
    upper = lax.broadcasted_iota(jnp.int32, (24, 128), 0) % 8 < 4
    for row in range(DEEP):
        found = []
        for col in (3, 32):
            value = slab[pl.ds(at(row, col), 24), :]
            if row < 3:
                value = jnp.where(upper, rim[pl.ds(at(row, col), 24), :], value)
            if row >= 11:
                value = jnp.where(upper, value, rim[pl.ds(at(row, col), 24), :])
            found.append(value)
        give_columns(row, place[3], *found, near, far)


def norm_body(
    k, far, place, old, near, far_side, kernel, bias, gain, shift, slab, normal, normed, rstd,
    store, taps, *held,
):
    kept = slab, normed, rstd
    if far:
        slab, normed, rstd, sems = held
    one = slice(k, k + 1)
    spread(kernel, k, taps)
    slab[...] = old[...]
    put_columns(slab, place[3], near, far_side)
    copies = [started(slab, kept[0], sems.at[0])] if far else []
    filtered(slab, taps, store, False)
    for row in range(ROWS):
        a, b = row * COLS, (row + 1) * COLS
        mixed = line_of(store, row) + bias[one, :]
        center = mixed - jnp.mean(mixed, -1, keepdims=True)
        scale = lax.rsqrt(jnp.mean(center * center, -1, keepdims=True) + EPSILON)
        value = center * scale
        normed[a:b, :] = value
        rstd[a:b, :] = jnp.broadcast_to(scale, (COLS, 128))
        normal[a:b, :] = (value * gain[one, :] + shift[one, :]).astype(BF16)
        if far and row in (7, 15):
            span = pl.ds((row - 7) * COLS, 8 * COLS)
            half = row // 8
            copies.append(started(normed.at[span], kept[1].at[span], sems.at[1 + half]))
            copies.append(started(rstd.at[span], kept[2].at[span], sems.at[3 + half]))
    for copy in copies:
        copy.wait()


def mlp_body(k, far, *refs):
    (
        place, a, normal, own_in, got_in, mate_in, own_out, got_out, mate_out,
        bias_in, bias_out, scale, out, edge_near, edge_far,
    ) = refs[:15]
    kept = refs[15:20]
    act, slope, branch, full_in, full_out = refs[20:25] if far else kept
    sems = refs[-1]
    copies = []

    def leave(which, span=slice(None)):
        if far:
            source = refs[20 + which].at[:, span] if span != slice(None) else refs[20 + which]
            target = kept[which].at[:, span] if span != slice(None) else kept[which]
            copies.append(started(source, target, sems.at[len(copies)]))

    one = slice(k, k + 1)
    core, part = place[0], place[1]
    mine = pl.multiple_of(part * 256, 256)
    theirs = pl.multiple_of((1 - part) * 256, 256)
    full_in[pl.ds(mine, 256), :] = own_in[k]
    full_in[pl.ds(pl.multiple_of(theirs + core * 128, 128), 128), :] = got_in[0]
    full_in[pl.ds(pl.multiple_of(theirs + (1 - core) * 128, 128), 128), :] = mate_in[0]
    leave(3)
    full_out[:, pl.ds(mine, 256)] = own_out[k]
    full_out[pl.ds(pl.multiple_of(core * HALF, HALF), HALF), pl.ds(theirs, 256)] = got_out[0]
    full_out[pl.ds(pl.multiple_of((1 - core) * HALF, HALF), HALF), pl.ds(theirs, 256)] = mate_out[0]
    leave(4)
    for c in range(8):
        cols = slice(c * 256, (c + 1) * 256)
        hidden = jnp.dot(normal[...], full_in[:, cols], preferred_element_type=F32)
        v = hidden + bias_in[one, cols]
        square = v * v
        tangent = jnp.tanh(v * (COEF + (COEF * CUBIC) * square))
        half = 0.5 * v
        act[:, cols] = (half + half * tangent).astype(BF16)
        slope[:, cols] = (
            0.5
            + 0.5 * tangent
            + half * (1.0 - tangent * tangent) * (COEF + (3.0 * COEF * CUBIC) * square)
        ).astype(BF16)
        if c % 2:
            leave(0, slice(c * 256 - 256, c * 256 + 256))
            leave(1, slice(c * 256 - 256, c * 256 + 256))
    for c in range(2):
        cols = slice(c * 256, (c + 1) * 256)
        value = jnp.dot(act[...], full_out[:, cols], preferred_element_type=F32)
        value = value + bias_out[one, cols]
        branch[:, cols] = value
        leave(2, cols)
        result = (a[:, cols].astype(F32) + scale[one, cols] * value).astype(BF16)
        out[:, cols] = result
        edge_near[:, cols] = either(core, result[:96, :], result[416:, :])
        edge_far[:, cols] = either(core, result[416:, :], result[:96, :])
    for copy in copies:
        copy.wait()


def back_body(
    k, place, u, branch, slope, normed, rstd, full_in, full_out, gain, scale,
    low, gh, slab, edge_near, edge_far, channel, bias, gn, rim,
):
    one = slice(k, k + 1)
    cols_last = (((1,), (1,)), ((), ()))
    up = u[...].astype(F32)
    channel[4:5, :] = jnp.sum(up * branch[...], 0, keepdims=True)
    gb = up * scale[one, :]
    channel[3:4, :] = jnp.sum(gb, 0, keepdims=True)
    low[...] = gb.astype(BF16)
    for c in range(8):
        cols = slice(c * 256, (c + 1) * 256)
        ga = lax.dot_general(
            low[...], full_out[cols, :], cols_last, preferred_element_type=F32
        )
        value = ga * slope[:, cols].astype(F32)
        bias[:, cols] = jnp.sum(value, 0, keepdims=True)
        gh[:, cols] = value.astype(BF16)
    for c in range(2):
        cols = slice(c * 256, (c + 1) * 256)
        gn[:, cols] = lax.dot_general(
            gh[...], full_in[cols, :], cols_last, preferred_element_type=F32
        )
    sums = [jnp.zeros((8, CH), F32) for _ in range(3)]

    def folded(value):
        return value[0:8] + value[8:16] + value[16:24] + value[24:32]

    for row in range(ROWS):
        a, b = row * COLS, (row + 1) * COLS
        grad = gn[a:b, :]
        value = normed[a:b, :]
        sums[1] += folded(grad * value)
        sums[2] += folded(grad)
        gs = grad * gain[one, :]
        gm = rstd[a:b, 0:1] * (
            gs
            - jnp.mean(gs, -1, keepdims=True)
            - value * jnp.mean(gs * value, -1, keepdims=True)
        )
        sums[0] += folded(gm)
        put_row(slab, row + 3, gm)
        if row < 3:
            rim[1 - place[0], a:b, :] = gm.astype(BF16)
        if row >= 13:
            rim[place[0], a - 416 : b - 416, :] = gm.astype(BF16)
    edge_near[...] = rim[0]
    edge_far[...] = rim[1]
    for n in range(3):
        channel[n : n + 1, :] = jnp.sum(sums[n], 0, keepdims=True)


def grads_body(place, normal, low, act, gh, keep, give):
    core = place[0]
    rows_first = (((0,), (0,)), ((), ()))
    for side, ref in ((1 - core, give), (core, keep)):
        for c in range(4):
            cols = pl.ds(pl.multiple_of(side * HALF + c * 256, 256), 256)
            ref[:, c * 256 : (c + 1) * 256] = lax.dot_general(
                normal[...], gh[:, cols], rows_first, preferred_element_type=F32
            ).astype(BF16)
            ref[:, HALF + c * 256 : HALF + (c + 1) * 256] = lax.dot_general(
                low[...], act[:, cols], rows_first, preferred_element_type=F32
            ).astype(BF16)


def taps_body(seen, grads, out, wide):
    def line(p, carry):
        def step(row, sums):
            sums = list(sums)
            for part in range(4):
                col = part * 8
                base = pl.multiple_of(((row + p) * WIDE + col) * 8, 8)
                home = pl.multiple_of(((row + 3) * WIDE + col + 3) * 8, 8)
                near = [seen[pl.ds(base + 8 * k, 8), :] for k in range(14)]
                for m in range(8):
                    grad = grads[pl.ds(home + 8 * m, 8), :]
                    for q in range(7):
                        spot = q + 7 * (m % 2)
                        sums[spot] = sums[spot] + near[m + q] * grad
            return tuple(sums)

        zero = jnp.zeros((8, 128), F32)
        sums = lax.fori_loop(0, 8, step, (zero,) * 14)
        base = pl.multiple_of(p * 56, 8)
        for q in range(7):
            wide[pl.ds(base + 8 * q, 8), :] = sums[q] + sums[q + 7]
        return carry

    lax.fori_loop(0, 7, line, 0)
    for tap in range(49):
        total = wide[tap * 8 : tap * 8 + 8, :]
        out[tap * 4 : tap * 4 + 4, :] = total[0:4] + total[4:8]


def up_body(
    k, count, place, old, edge_near, edge_far, near, far, kernel, u, *refs
):
    later, out, brought = refs[:count], refs[count], refs[count + 1 : 2 * count + 1]
    slab, store, taps, strips, edges, base, sems = refs[2 * count + 1 :]
    whole = started(old, slab, sems.at[0])
    copies = [
        started(edge_near, edges.at[0], sems.at[1]),
        started(edge_far, edges.at[1], sems.at[2]),
        started(near, strips.at[0], sems.at[3]),
        started(far, strips.at[1], sems.at[4]),
    ]
    last = started(u, base, sems.at[5])
    coming = [started(later[n], brought[n], sems.at[6 + n]) for n in range(count)]
    spread(kernel, k, taps)
    whole.wait()
    for copy in copies:
        copy.wait()
    put_edges(slab, place[0], edges.at[0], edges.at[1])
    put_columns(slab, place[3], strips.at[0], strips.at[1])
    filtered(slab, taps, store, True)
    last.wait()
    for row in range(ROWS):
        a, b = row * COLS, (row + 1) * COLS
        out[a:b, :] = (base[a:b, :].astype(F32) + line_of(store, row)).astype(out.dtype)
    for copy in coming:
        copy.wait()


def pair_body(count, keep, got, *refs):
    parts, (far, out, *lines), sems = refs[: 3 * count], refs[3 * count : -1], refs[-1]
    for n in range(count):
        taps, channel, bias = parts[3 * n : 3 * n + 3]
        ref = lines[n]
        ref[0:196, :] = taps[...]
        spot = 196
        for kind in range(5):
            for group in range(4):
                ref[spot : spot + 1, :] = channel[
                    kind : kind + 1, group * 128 : (group + 1) * 128
                ]
                spot += 1
        for group in range(16):
            ref[spot : spot + 1, :] = bias[:, group * 128 : (group + 1) * 128]
            spot += 1
        ref[spot:256, :] = jnp.zeros((256 - spot, 128), F32)

    def step(n, carry):
        rows = pl.ds(pl.multiple_of(n * 32, 32), 32)
        total = keep[rows, :].astype(F32) + got[rows, :].astype(F32)
        out[pl.ds(n * 4, 4), :, :FF] = total.reshape(4, 8, FF).astype(BF16)
        rows = pl.ds(pl.multiple_of((n % 8) * 32, 32), 32)
        for m in range(count):
            out[pl.ds(n * 4, 4), :, FF + m * 128 : FF + (m + 1) * 128] = (
                lines[m][rows, :].reshape(4, 8, 128).astype(BF16)
            )
        return carry

    copies = []
    for part in range(4):
        lax.fori_loop(part * 4, part * 4 + 4, step, 0)
        span = pl.ds(part * 16, 16)
        copies.append(started(out.at[span], far.at[span], sems.at[part]))
    for copy in copies:
        copy.wait()


def total_body(pieces, out):
    width = pieces.shape[2]
    for a in range(0, width, 512):
        b = min(a + 512, width)

        def step(n, total, a=a, b=b):
            for m in range(4):
                total = total + pieces[n * 4 + m, :, a:b].astype(F32)
            return total

        total = lax.fori_loop(0, 16, step, jnp.zeros((8, b - a), F32))
        out[:, a:b] = total.astype(BF16)


def merge_body(other, pieces, far, out, sums, sems):
    for n in range(32):
        out[n, :, FF : 2 * FF] = other[...]
    copies = [started(out.at[:, :, FF : 2 * FF], far.at[:, :, FF : 2 * FF], sems.at[0])]
    total_body(pieces, sums)
    for part in range(2):
        for n in range(part * 16, part * 16 + 16):
            out[n, :, :FF] = sums[:, :FF]
            out[n, :, 2 * FF :] = sums[:, FF:]
        span = pl.ds(part * 16, 16)
        for m, cols in enumerate((slice(0, FF), slice(2 * FF, 2 * FF + 256))):
            copies.append(
                started(out.at[span, :, cols], far.at[span, :, cols], sems.at[1 + part * 2 + m])
            )
    for copy in copies:
        copy.wait()


def small_body(whole0, whole1, mate0, mate1, taps, channel, bias, lines):
    for k, whole, mate in ((0, whole0, mate0), (1, whole1, mate1)):
        lines[0:256, :] = (whole[...].astype(F32) + mate[...].astype(F32)).reshape(256, 128)
        for group in range(4):
            cols = slice(group * 128, (group + 1) * 128)
            for tap in range(49):
                line = tap * 4 + group
                taps[tap // 7, tap % 7, k : k + 1, cols] = lines[line : line + 1, :]
            for kind in range(5):
                line = 196 + kind * 4 + group
                channel[kind, k : k + 1, cols] = lines[line : line + 1, :]
        for group in range(16):
            bias[k : k + 1, group * 128 : (group + 1) * 128] = lines[216 + group : 217 + group, :]


def finish_body(place, ref, *refs):
    grad_in, grad_out = refs[-2:]
    value = ref[...].astype(F32).reshape(128, FF)
    grad_in[0] = value[:, :HALF]
    grad_out[0] = value[:, HALF:].T


STORE = pltpu.VMEM((ROWS * COLS * 4 + 16, 128), F32)
TAPS = pltpu.VMEM((400, 128), F32)
STRIP = ((DEEP * 24, 128), BF16)
EDGE = ((96, CH), BF16)


def edge_strips(place, x):
    return call(strips_body, [EDGE, EDGE], 2, 1_000_000, scalars=1)(place, x)


def pack(place, x, near, far):
    outs = [((SLAB, 128), F32), STRIP, STRIP]
    return call(pack_body, outs, 4, 10_000_000, scalars=1)(place, x, near, far)


def pack_edges(place, slab, near, far):
    scratch = [pltpu.VMEM((SLAB, 128), F32)]
    return call(edge_body, [STRIP, STRIP], 4, 10_000_000, scratch, scalars=1)(
        place, slab, near, far
    )


def normalise(k, place, slab, near, far_side, kernel, bias, gain, shift):
    outs = [((SLAB, 128), F32), ((PIX, CH), BF16), ((PIX, CH), F32), ((PIX, 128), F32)]
    far = k == 0
    scratch = [STORE, TAPS]
    if far:
        scratch += [pltpu.VMEM(*outs[n]) for n in (0, 2, 3)] + [DMA((5,))]
    return call(
        functools.partial(norm_body, k, far), outs, 8, 40_000_000, scratch, scalars=1,
        grant=8 if far else 5, far_out=(0, 2, 3) if far else (),
    )(place, slab, near, far_side, kernel, bias, gain, shift)


def mlp(k, place, a, normal, weights, bias_in, bias_out, scale):
    kept = [
        ((PIX, FF), BF16), ((PIX, FF), BF16), ((PIX, CH), F32), ((CH, FF), BF16), ((FF, CH), BF16),
    ]
    outs = [((PIX, CH), BF16), EDGE, EDGE, *kept]
    far = k == 0
    scratch = [*(pltpu.VMEM(s, d) for s, d in kept), DMA((12,))] if far else [DMA((1,))]
    return call(
        functools.partial(mlp_body, k, far), outs, 12, 60_000_000, scratch, scalars=1,
        grant=14 if far else 5, far_out=range(3, 8) if far else (),
    )(place, a, normal, *weights, bias_in, bias_out, scale)


def backward(k, place, u, saved, gain, scale):
    outs = [
        ((PIX, CH), BF16), ((PIX, FF), BF16), ((SLAB, 128), F32), EDGE, EDGE,
        ((8, CH), F32), ((1, FF), F32),
    ]
    scratch = [pltpu.VMEM((PIX, CH), F32), pltpu.VMEM((2, *EDGE[0]), BF16)]
    return call(
        functools.partial(back_body, k), outs, 10, 60_000_000, scratch, scalars=1
    )(place, u, *saved, gain, scale)


def weight_grads(place, normal, low, act, gh):
    outs = [((CH, FF), BF16), ((CH, FF), BF16)]
    return call(grads_body, outs, 5, 50_000_000, scalars=1)(place, normal, low, act, gh)


def tap_grads(seen, grads):
    return call(taps_body, [((49 * 4, 128), F32)], 2, 40_000_000, [TAPS])(
        seen, grads
    )[0]


def upstream(k, place, slab, edge_near, edge_far, near, far, kernel, u, dtype, later=()):
    scratch = [
        pltpu.VMEM((SLAB, 128), F32), STORE, TAPS,
        pltpu.VMEM((2, *STRIP[0]), BF16), pltpu.VMEM((2, *EDGE[0]), BF16),
        pltpu.VMEM((PIX, CH), u.dtype), DMA((6 + len(later),)),
    ]
    outs = [((PIX, CH), dtype), *((x.shape, x.dtype) for x in later)]
    return call(
        functools.partial(up_body, k, len(later)), outs, 8 + len(later), 40_000_000, scratch,
        grant=8, far=(1, 2, 3, 4, 5, 7, *range(8, 8 + len(later))), scalars=1,
    )(place, slab, edge_near, edge_far, near, far, kernel, u, *later)


def finish(place, side, value, buffers):
    held = [pl.BlockSpec(memory_space=pl.ANY)] * len(buffers)
    return pl.pallas_call(
        finish_body,
        grid_spec=pltpu.PrefetchScalarGridSpec(
            num_scalar_prefetch=1,
            grid=(2, 2),
            in_specs=[pl.BlockSpec((16, 8, FF), lambda layer, i, s: (i, 0, layer)), *held],
            out_specs=[
                pl.BlockSpec((1, 128, HALF), lambda layer, i, s: (layer, i, s[side])),
                pl.BlockSpec((1, HALF, 128), lambda layer, i, s: (layer, s[side], i)),
            ],
        ),
        out_shape=[
            jax.ShapeDtypeStruct((2, 256, FF), F32),
            jax.ShapeDtypeStruct((2, FF, 256), F32),
        ],
        input_output_aliases={2: 0, 3: 1} if buffers else {},
        compiler_params=pltpu.CompilerParams(vmem_limit_bytes=10 * 1024 * 1024),
        cost_estimate=pl.CostEstimate(
            flops=5_000_000, bytes_accessed=6_000_000, transcendentals=0
        ),
    )(place, value, *buffers)


def finish_small(whole, mate):
    first = pl.BlockSpec((32, 8, 128), lambda i: (0, 0, 2 * FF // 128))
    second = pl.BlockSpec((32, 8, 128), lambda i: (0, 0, 2 * FF // 128 + 1))
    shapes = [(7, 7, 2, CH), (5, 2, CH), (2, FF)]
    return pl.pallas_call(
        small_body,
        grid=(1,),
        out_shape=[jax.ShapeDtypeStruct(s, F32) for s in shapes],
        in_specs=[first, second, first, second],
        out_specs=[
            pl.BlockSpec((7, 7, 2, CH), lambda i: (0, 0, 0, 0)),
            pl.BlockSpec((5, 2, CH), lambda i: (0, 0, 0)),
            pl.BlockSpec((2, FF), lambda i: (0, 0)),
        ],
        scratch_shapes=[pltpu.VMEM((256 + 8, 128), F32)],
        compiler_params=pltpu.CompilerParams(vmem_limit_bytes=4 * 1024 * 1024),
        cost_estimate=pl.CostEstimate(
            flops=1_000_000, bytes_accessed=1_000_000, transcendentals=0
        ),
    )(whole, whole, mate, mate)


RANKS = ("xh", "y", "core")


def pairs(first, count):
    found = [(i, i + 1) for i in range(first, count - 1, 2)]
    return found + [(b, a) for a, b in found]


def from_rows(near, far):
    near = lax.ppermute(near, RANKS, pairs(0, 16))
    far = lax.ppermute(far, RANKS, pairs(1, 16))
    return near, far


def from_columns(near, far):
    near = lax.ppermute(near, "z", pairs(0, 4))
    far = lax.ppermute(far, "z", pairs(1, 4))
    return near, far


def swapped(value, axis):
    return lax.ppermute(value, axis, [(0, 1), (1, 0)])


def around_x(value, step):
    return lax.ppermute(value, ("xh", "dp"), [(i, (i + step) % 4) for i in range(4)])


def fetch_weights(core, weight_in, weight_out, k):
    half_in = lax.dynamic_slice(weight_in, (k, core * 128, 0), (1, 128, FF))
    half_out = lax.dynamic_slice(weight_out, (k, core * HALF, 0), (1, HALF, 256))
    got_in = around_x(half_in, 1)
    got_out = around_x(half_out, -1)
    mate_in = swapped(got_in, "core")
    mate_out = swapped(got_out, "core")
    return weight_in, got_in, mate_in, weight_out, got_out, mate_out


def send_grads(keep, got, small):
    count = len(small) // 3
    shape = (64, 8, FF + 128 * count)
    scratch = [
        pltpu.VMEM(shape, BF16), *[pltpu.VMEM((256, 128), F32)] * count, DMA((4,)),
    ]
    pair = call(
        functools.partial(pair_body, count), [(shape, BF16)], 2 + len(small), 2_000_000,
        scratch, far_out=(0,),
    )(keep, got, *small)[0]
    return lax.all_to_all(pair, ("dp", *SPACE), 0, 0, tiled=True)


def per_device(
    slides,
    cotangent,
    kernel,
    kernel_bias,
    norm_gain,
    norm_bias,
    weight_in,
    bias_in,
    weight_out,
    bias_out,
    layer_scale,
):
    core, part = lax.axis_index("core"), lax.axis_index("dp")
    place = jnp.stack([core, part, 1 - core, lax.axis_index("z") % 2]).astype(jnp.int32)
    slides, place = lax.optimization_barrier((slides, place))
    kernel = jnp.transpose(kernel, (1, 2, 0, 3))
    current = slides.reshape(PIX, CH)
    edges = edge_strips(place, current)
    saved = []
    weights = [fetch_weights(core, weight_in, weight_out, k) for k in range(2)]
    for k in range(2):
        edges = from_rows(*edges)
        slab, *sides = pack(place, current, *edges)
        sides = from_columns(*sides)
        slab, normal, normed, rstd = normalise(
            k, place, slab, *sides, kernel, kernel_bias, norm_gain, norm_bias
        )
        current, *edges, act, slope, branch, full_in, full_out = mlp(
            k, place, current, normal, weights[k], bias_in, bias_out, layer_scale
        )
        saved.append((slab, act, normal, (branch, slope, normed, rstd, full_in, full_out)))
    up = cotangent.reshape(PIX, CH)
    pieces = [None] * 2
    small = []
    for k in (1, 0):
        seen, act, normal, rest = saved[k]
        low, gh, grads, *edges, channel, bias = backward(k, place, up, rest, norm_gain, layer_scale)
        edges = from_rows(*edges)
        keep, give = weight_grads(place, normal, low, act, gh)
        got = swapped(give, "core")
        taps = tap_grads(seen, grads)
        small = [taps, channel, bias, *small]
        pieces[k] = send_grads(keep, got, () if k else small)
        sides = pack_edges(place, grads, *edges)
        sides = from_columns(*sides)
        later = saved[0][3] if k else ()
        up, *brought = upstream(
            k, place, grads, *edges, *sides, kernel, up, F32 if k else BF16, later
        )
        if k:
            saved[0] = (*saved[0][:3], brought)
    other = call(total_body, [((8, FF), BF16)], 1, 5_000_000)(pieces[1])[0]
    scratch = [
        pltpu.VMEM((32, 8, FF + WIRE), BF16), pltpu.VMEM((8, WIRE), BF16), DMA((5,)),
    ]
    copies = call(
        merge_body, [((32, 8, FF + WIRE), BF16)], 2, 5_000_000, scratch, grant=8, far_out=(0,)
    )(other, pieces[0])[0]
    whole = lax.all_to_all(copies, SPACE, 0, 0, tiled=True)
    mate = swapped(whole, "core")
    buffers = finish(place, 0, whole, ())
    grad_in, grad_out = finish(place, 2, mate, buffers)
    grad_taps, grad_channel, grad_bias = finish_small(whole, mate)
    return (
        current.reshape(slides.shape),
        up.reshape(slides.shape),
        grad_in,
        grad_out,
        jnp.transpose(grad_taps, (2, 0, 1, 3)),
        jnp.transpose(grad_channel, (1, 0, 2)),
        grad_bias,
    )


def solution(mesh):
    fine = jax.sharding.Mesh(
        mesh.devices.reshape(2, 4, 2, 4, 2), ("xh", "y", "core", "z", "dp")
    )
    maps = P("dp", RANKS, "z", None)
    split_in, split_out = P(None, "dp", None), P(None, None, "dp")
    whole = P()
    return jax.shard_map(
        per_device,
        mesh=fine,
        in_specs=(
            maps, maps, whole, whole, whole, whole, split_in, whole, split_out, whole, whole,
        ),
        out_specs=(maps, maps, split_in, split_out, whole, whole, whole),
        check_vma=False,
    )
```

```python
import functools

import jax
import jax.numpy as jnp
from jax import lax
from jax.experimental import pallas as pl
from jax.experimental.pallas import tpu as pltpu
from jax.sharding import PartitionSpec as P

COEF = 0.7978845608028654
CUBIC = 0.044715
EPSILON = 1e-06

PIX = 512
CH = 512
FF = 2048
HALF = 1024
WIRE = FF + 256
ROWS, COLS = 16, 32
WIDE = 40
DEEP = 14
SLAB = DEEP * WIDE * 8
SPACE = ("xh", "y", "z")
F32, BF16 = jnp.float32, jnp.bfloat16

VM = pl.BlockSpec(memory_space=pltpu.VMEM)
SM = pl.BlockSpec(memory_space=pltpu.SMEM)


FAR = pl.BlockSpec(memory_space=pltpu.HBM)
DMA = pltpu.SemaphoreType.DMA


def call(body, outs, count, flops, scratch=(), scalars=0, grant=5, far=(), far_out=()):
    shapes = [
        pltpu.HBM(s, d) if n in far_out else jax.ShapeDtypeStruct(s, d)
        for n, (s, d) in enumerate(outs)
    ]
    made = pl.pallas_call(
        body,
        out_shape=shapes,
        in_specs=[
            SM if n < scalars else FAR if n in far else VM for n in range(count)
        ],
        out_specs=[FAR if n in far_out else VM for n in range(len(outs))],
        scratch_shapes=list(scratch),
        compiler_params=pltpu.CompilerParams(vmem_limit_bytes=grant * 1024 * 1024),
        cost_estimate=pl.CostEstimate(
            flops=flops, bytes_accessed=4_000_000, transcendentals=0
        ),
    )

    def run(*args):
        return made(
            *(
                pltpu.with_memory_space_constraint(arg, pltpu.HBM) if n in far else arg
                for n, arg in enumerate(args)
            )
        )

    return run


def started(source, target, sem):
    copy = pltpu.make_async_copy(source, target, sem)
    copy.start()
    return copy


def at(row, col):
    return (row * WIDE + col) * 8


def homes(row):
    found = []
    if row < DEEP:
        found.append((0, row))
    if row >= 8:
        found.append((1, row - 8))
    return found


def put_row(slab, row, line):
    for block, inner in homes(row):
        for group in range(4):
            slab[pl.ds(at(inner, 3) + block * 4 + group, COLS, stride=8), :] = line[
                :, group * 128 : (group + 1) * 128
            ]


def either(odd, a, b):
    return jnp.where(odd == 1, a, b)


def put_edges(slab, odd, near, far):
    for n in range(3):
        a = near[n * COLS : (n + 1) * COLS, :].astype(F32)
        b = far[n * COLS : (n + 1) * COLS, :].astype(F32)
        put_row(slab, n, either(odd, a, b))
        put_row(slab, 19 + n, either(odd, b, a))


def put_columns(slab, odd, near, far):
    for row in range(DEEP):
        a = near[row * 24 : (row + 1) * 24, :].astype(F32)
        b = far[row * 24 : (row + 1) * 24, :].astype(F32)
        slab[pl.ds(at(row, 0), 24), :] = either(odd, a, b)
        slab[pl.ds(at(row, 35), 24), :] = either(odd, b, a)


def give_columns(row, odd, low, high, near, far):
    near[row * 24 : (row + 1) * 24, :] = either(odd, low, high).astype(BF16)
    far[row * 24 : (row + 1) * 24, :] = either(odd, high, low).astype(BF16)


def spread(kernel, k, taps):
    for tap in range(49):
        line = kernel[tap // 7, tap % 7, k : k + 1, :]
        for part in range(8):
            group = part % 4
            taps[tap * 8 + part : tap * 8 + part + 1, :] = line[
                :, group * 128 : (group + 1) * 128
            ]


def filtered(slab, taps, store, turned):
    def step(n, carry):
        row = n // 4
        col = (n % 4) * 8
        sums = [None] * 8
        for p in range(7):
            base = pl.multiple_of(((row + p) * WIDE + col) * 8, 8)
            seen = [slab[pl.ds(base + 8 * k, 8), :] for k in range(14)]
            for q in range(7):
                tap = 48 - p * 7 - q if turned else p * 7 + q
                weight = taps[tap * 8 : tap * 8 + 8, :]
                for m in range(8):
                    term = seen[m + q] * weight
                    sums[m] = term if sums[m] is None else sums[m] + term
        base = pl.multiple_of((row * COLS + col) * 8, 8)
        for m in range(8):
            store[pl.ds(base + 8 * m, 8), :] = sums[m]
        return carry

    lax.fori_loop(0, 32, step, 0)


def line_of(store, row):
    block, inner = row // 8, row % 8
    return jnp.concatenate(
        [
            store[pl.ds(inner * COLS * 8 + block * 4 + group, COLS, stride=8), :]
            for group in range(4)
        ],
        axis=1,
    )


def strips_body(place, x, near, far):
    odd = place[0]
    near[...] = x[pl.ds(pl.multiple_of((1 - odd) * 416, 32), 96), :]
    far[...] = x[pl.ds(pl.multiple_of(odd * 416, 32), 96), :]


def pack_body(place, x, edge_near, edge_far, slab, near, far):
    for row in range(ROWS):
        put_row(slab, row + 3, x[row * COLS : (row + 1) * COLS, :].astype(F32))
    put_edges(slab, place[0], edge_near, edge_far)
    for row in range(DEEP):
        give_columns(
            row, place[3], slab[pl.ds(at(row, 3), 24), :], slab[pl.ds(at(row, 32), 24), :],
            near, far,
        )


def edge_body(place, slab, edge_near, edge_far, near, far, rim):
    put_edges(rim, place[0], edge_near, edge_far)
    upper = lax.broadcasted_iota(jnp.int32, (24, 128), 0) % 8 < 4
    for row in range(DEEP):
        found = []
        for col in (3, 32):
            value = slab[pl.ds(at(row, col), 24), :]
            if row < 3:
                value = jnp.where(upper, rim[pl.ds(at(row, col), 24), :], value)
            if row >= 11:
                value = jnp.where(upper, value, rim[pl.ds(at(row, col), 24), :])
            found.append(value)
        give_columns(row, place[3], *found, near, far)


def norm_body(
    k, far, place, old, near, far_side, kernel, bias, gain, shift, slab, normal, normed, rstd,
    store, taps, *held,
):
    kept = slab, normed, rstd
    slab, sems = held[0], held[-1]
    if far:
        normed, rstd = held[1:3]
    one = slice(k, k + 1)
    spread(kernel, k, taps)
    slab[...] = old[...]
    put_columns(slab, place[3], near, far_side)
    copies = [started(slab, kept[0], sems.at[0])]
    filtered(slab, taps, store, False)
    for row in range(ROWS):
        a, b = row * COLS, (row + 1) * COLS
        mixed = line_of(store, row) + bias[one, :]
        center = mixed - jnp.mean(mixed, -1, keepdims=True)
        scale = lax.rsqrt(jnp.mean(center * center, -1, keepdims=True) + EPSILON)
        value = center * scale
        normed[a:b, :] = value
        rstd[a:b, :] = jnp.broadcast_to(scale, (COLS, 128))
        normal[a:b, :] = (value * gain[one, :] + shift[one, :]).astype(BF16)
        if far and row in (7, 15):
            span = pl.ds((row - 7) * COLS, 8 * COLS)
            half = row // 8
            copies.append(started(normed.at[span], kept[1].at[span], sems.at[1 + half]))
            copies.append(started(rstd.at[span], kept[2].at[span], sems.at[3 + half]))
    for copy in copies:
        copy.wait()


def mlp_body(k, far, *refs):
    (
        place, a, normal, own_in, got_in, mate_in, own_out, got_out, mate_out,
        bias_in, bias_out, scale, out, edge_near, edge_far,
    ) = refs[:15]
    kept = refs[15:20]
    act, slope, branch, full_in, full_out = refs[20:25] if far else kept
    sems = refs[-1]
    copies = []

    def leave(which, span=slice(None)):
        if far:
            source = refs[20 + which].at[:, span] if span != slice(None) else refs[20 + which]
            target = kept[which].at[:, span] if span != slice(None) else kept[which]
            copies.append(started(source, target, sems.at[len(copies)]))

    one = slice(k, k + 1)
    core, part = place[0], place[1]
    mine = pl.multiple_of(part * 256, 256)
    theirs = pl.multiple_of((1 - part) * 256, 256)
    full_in[pl.ds(mine, 256), :] = own_in[k]
    full_in[pl.ds(pl.multiple_of(theirs + core * 128, 128), 128), :] = got_in[0]
    full_in[pl.ds(pl.multiple_of(theirs + (1 - core) * 128, 128), 128), :] = mate_in[0]
    leave(3)
    full_out[:, pl.ds(mine, 256)] = own_out[k]
    full_out[pl.ds(pl.multiple_of(core * HALF, HALF), HALF), pl.ds(theirs, 256)] = got_out[0]
    full_out[pl.ds(pl.multiple_of((1 - core) * HALF, HALF), HALF), pl.ds(theirs, 256)] = mate_out[0]
    leave(4)
    for c in range(8):
        cols = slice(c * 256, (c + 1) * 256)
        hidden = jnp.dot(normal[...], full_in[:, cols], preferred_element_type=F32)
        v = hidden + bias_in[one, cols]
        square = v * v
        tangent = jnp.tanh(v * (COEF + (COEF * CUBIC) * square))
        half = 0.5 * v
        act[:, cols] = (half + half * tangent).astype(BF16)
        slope[:, cols] = (
            0.5
            + 0.5 * tangent
            + half * (1.0 - tangent * tangent) * (COEF + (3.0 * COEF * CUBIC) * square)
        ).astype(BF16)
        if c % 2:
            leave(0, slice(c * 256 - 256, c * 256 + 256))
            leave(1, slice(c * 256 - 256, c * 256 + 256))
    for c in range(2):
        cols = slice(c * 256, (c + 1) * 256)
        value = jnp.dot(act[...], full_out[:, cols], preferred_element_type=F32)
        value = value + bias_out[one, cols]
        branch[:, cols] = value
        leave(2, cols)
        result = (a[:, cols].astype(F32) + scale[one, cols] * value).astype(BF16)
        out[:, cols] = result
        edge_near[:, cols] = either(core, result[:96, :], result[416:, :])
        edge_far[:, cols] = either(core, result[416:, :], result[:96, :])
    for copy in copies:
        copy.wait()


def back_body(
    k, place, u, branch, slope, normed, rstd, full_in, full_out, gain, scale,
    low, gh, slab, edge_near, edge_far, channel, bias, gn, rim,
):
    one = slice(k, k + 1)
    cols_last = (((1,), (1,)), ((), ()))
    up = u[...].astype(F32)
    channel[4:5, :] = jnp.sum(up * branch[...], 0, keepdims=True)
    gb = up * scale[one, :]
    channel[3:4, :] = jnp.sum(gb, 0, keepdims=True)
    low[...] = gb.astype(BF16)
    for c in range(8):
        cols = slice(c * 256, (c + 1) * 256)
        ga = lax.dot_general(
            low[...], full_out[cols, :], cols_last, preferred_element_type=F32
        )
        value = ga * slope[:, cols].astype(F32)
        bias[:, cols] = jnp.sum(value, 0, keepdims=True)
        gh[:, cols] = value.astype(BF16)
    for c in range(2):
        cols = slice(c * 256, (c + 1) * 256)
        gn[:, cols] = lax.dot_general(
            gh[...], full_in[cols, :], cols_last, preferred_element_type=F32
        )
    sums = [jnp.zeros((8, CH), F32) for _ in range(3)]

    def folded(value):
        return value[0:8] + value[8:16] + value[16:24] + value[24:32]

    for row in range(ROWS):
        a, b = row * COLS, (row + 1) * COLS
        grad = gn[a:b, :]
        value = normed[a:b, :]
        sums[1] += folded(grad * value)
        sums[2] += folded(grad)
        gs = grad * gain[one, :]
        gm = rstd[a:b, 0:1] * (
            gs
            - jnp.mean(gs, -1, keepdims=True)
            - value * jnp.mean(gs * value, -1, keepdims=True)
        )
        sums[0] += folded(gm)
        put_row(slab, row + 3, gm)
        if row < 3:
            rim[1 - place[0], a:b, :] = gm.astype(BF16)
        if row >= 13:
            rim[place[0], a - 416 : b - 416, :] = gm.astype(BF16)
    edge_near[...] = rim[0]
    edge_far[...] = rim[1]
    for n in range(3):
        channel[n : n + 1, :] = jnp.sum(sums[n], 0, keepdims=True)


def grads_body(place, normal, low, act, gh, keep, give):
    core = place[0]
    rows_first = (((0,), (0,)), ((), ()))
    for side, ref in ((1 - core, give), (core, keep)):
        for c in range(4):
            cols = pl.ds(pl.multiple_of(side * HALF + c * 256, 256), 256)
            ref[:, c * 256 : (c + 1) * 256] = lax.dot_general(
                normal[...], gh[:, cols], rows_first, preferred_element_type=F32
            ).astype(BF16)
            ref[:, HALF + c * 256 : HALF + (c + 1) * 256] = lax.dot_general(
                low[...], act[:, cols], rows_first, preferred_element_type=F32
            ).astype(BF16)


def taps_body(seen, grads, out, wide):
    def line(p, carry):
        def step(row, sums):
            sums = list(sums)
            for part in range(4):
                col = part * 8
                base = pl.multiple_of(((row + p) * WIDE + col) * 8, 8)
                home = pl.multiple_of(((row + 3) * WIDE + col + 3) * 8, 8)
                near = [seen[pl.ds(base + 8 * k, 8), :] for k in range(14)]
                for m in range(8):
                    grad = grads[pl.ds(home + 8 * m, 8), :]
                    for q in range(7):
                        spot = q + 7 * (m % 2)
                        sums[spot] = sums[spot] + near[m + q] * grad
            return tuple(sums)

        zero = jnp.zeros((8, 128), F32)
        sums = lax.fori_loop(0, 8, step, (zero,) * 14)
        base = pl.multiple_of(p * 56, 8)
        for q in range(7):
            wide[pl.ds(base + 8 * q, 8), :] = sums[q] + sums[q + 7]
        return carry

    lax.fori_loop(0, 7, line, 0)
    for tap in range(49):
        total = wide[tap * 8 : tap * 8 + 8, :]
        out[tap * 4 : tap * 4 + 4, :] = total[0:4] + total[4:8]


def up_body(
    k, count, place, old, edge_near, edge_far, near, far, kernel, u, *refs
):
    later, out, brought = refs[:count], refs[count], refs[count + 1 : 2 * count + 1]
    slab, store, taps, strips, edges, base, sems = refs[2 * count + 1 :]
    whole = started(old, slab, sems.at[0])
    copies = [
        started(edge_near, edges.at[0], sems.at[1]),
        started(edge_far, edges.at[1], sems.at[2]),
        started(near, strips.at[0], sems.at[3]),
        started(far, strips.at[1], sems.at[4]),
    ]
    last = started(u, base, sems.at[5])
    coming = [started(later[n], brought[n], sems.at[6 + n]) for n in range(count)]
    spread(kernel, k, taps)
    whole.wait()
    for copy in copies:
        copy.wait()
    put_edges(slab, place[0], edges.at[0], edges.at[1])
    put_columns(slab, place[3], strips.at[0], strips.at[1])
    filtered(slab, taps, store, True)
    last.wait()
    for row in range(ROWS):
        a, b = row * COLS, (row + 1) * COLS
        out[a:b, :] = (base[a:b, :].astype(F32) + line_of(store, row)).astype(out.dtype)
    for copy in coming:
        copy.wait()


def pair_body(count, keep, got, *refs):
    parts, (far, out, *lines), sems = refs[: 3 * count], refs[3 * count : -1], refs[-1]
    for n in range(count):
        taps, channel, bias = parts[3 * n : 3 * n + 3]
        ref = lines[n]
        ref[0:196, :] = taps[...]
        spot = 196
        for kind in range(5):
            for group in range(4):
                ref[spot : spot + 1, :] = channel[
                    kind : kind + 1, group * 128 : (group + 1) * 128
                ]
                spot += 1
        for group in range(16):
            ref[spot : spot + 1, :] = bias[:, group * 128 : (group + 1) * 128]
            spot += 1
        ref[spot:256, :] = jnp.zeros((256 - spot, 128), F32)

    def step(n, carry):
        rows = pl.ds(pl.multiple_of(n * 32, 32), 32)
        total = keep[rows, :].astype(F32) + got[rows, :].astype(F32)
        out[pl.ds(n * 4, 4), :, :FF] = total.reshape(4, 8, FF).astype(BF16)
        rows = pl.ds(pl.multiple_of((n % 8) * 32, 32), 32)
        for m in range(count):
            out[pl.ds(n * 4, 4), :, FF + m * 128 : FF + (m + 1) * 128] = (
                lines[m][rows, :].reshape(4, 8, 128).astype(BF16)
            )
        return carry

    copies = []
    for part in range(4):
        lax.fori_loop(part * 4, part * 4 + 4, step, 0)
        span = pl.ds(part * 16, 16)
        copies.append(started(out.at[span], far.at[span], sems.at[part]))
    for copy in copies:
        copy.wait()


def total_body(pieces, out):
    width = pieces.shape[2]
    for a in range(0, width, 512):
        b = min(a + 512, width)

        def step(n, total, a=a, b=b):
            for m in range(4):
                total = total + pieces[n * 4 + m, :, a:b].astype(F32)
            return total

        total = lax.fori_loop(0, 16, step, jnp.zeros((8, b - a), F32))
        out[:, a:b] = total.astype(BF16)


def merge_body(other, pieces, far, out, sums, sems):
    for n in range(32):
        out[n, :, FF : 2 * FF] = other[...]
    copies = [started(out.at[:, :, FF : 2 * FF], far.at[:, :, FF : 2 * FF], sems.at[0])]
    total_body(pieces, sums)
    for part in range(2):
        for n in range(part * 16, part * 16 + 16):
            out[n, :, :FF] = sums[:, :FF]
            out[n, :, 2 * FF :] = sums[:, FF:]
        span = pl.ds(part * 16, 16)
        for m, cols in enumerate((slice(0, FF), slice(2 * FF, 2 * FF + 256))):
            copies.append(
                started(out.at[span, :, cols], far.at[span, :, cols], sems.at[1 + part * 2 + m])
            )
    for copy in copies:
        copy.wait()


def small_body(whole0, whole1, mate0, mate1, taps, channel, bias, lines):
    for k, whole, mate in ((0, whole0, mate0), (1, whole1, mate1)):
        lines[0:256, :] = (whole[...].astype(F32) + mate[...].astype(F32)).reshape(256, 128)
        for group in range(4):
            cols = slice(group * 128, (group + 1) * 128)
            for tap in range(49):
                line = tap * 4 + group
                taps[tap // 7, tap % 7, k : k + 1, cols] = lines[line : line + 1, :]
            for kind in range(5):
                line = 196 + kind * 4 + group
                channel[kind, k : k + 1, cols] = lines[line : line + 1, :]
        for group in range(16):
            bias[k : k + 1, group * 128 : (group + 1) * 128] = lines[216 + group : 217 + group, :]


def finish_body(place, ref, *refs):
    grad_in, grad_out = refs[-2:]
    value = ref[...].astype(F32).reshape(128, FF)
    grad_in[0] = value[:, :HALF]
    grad_out[0] = value[:, HALF:].T


STORE = pltpu.VMEM((ROWS * COLS * 4 + 16, 128), F32)
TAPS = pltpu.VMEM((400, 128), F32)
STRIP = ((DEEP * 24, 128), BF16)
EDGE = ((96, CH), BF16)


def edge_strips(place, x):
    return call(strips_body, [EDGE, EDGE], 2, 1_000_000, scalars=1)(place, x)


def pack(place, x, near, far):
    outs = [((SLAB, 128), F32), STRIP, STRIP]
    return call(pack_body, outs, 4, 10_000_000, scalars=1)(place, x, near, far)


def pack_edges(place, slab, near, far):
    scratch = [pltpu.VMEM((SLAB, 128), F32)]
    return call(edge_body, [STRIP, STRIP], 4, 10_000_000, scratch, scalars=1)(
        place, slab, near, far
    )


def normalise(k, place, slab, near, far_side, kernel, bias, gain, shift):
    outs = [((SLAB, 128), F32), ((PIX, CH), BF16), ((PIX, CH), F32), ((PIX, 128), F32)]
    far = k == 0
    leaving = (0, 2, 3) if far else (0,)
    scratch = [STORE, TAPS, *(pltpu.VMEM(*outs[n]) for n in leaving), DMA((5,))]
    return call(
        functools.partial(norm_body, k, far), outs, 8, 40_000_000, scratch, scalars=1,
        grant=8, far_out=leaving,
    )(place, slab, near, far_side, kernel, bias, gain, shift)


def mlp(k, place, a, normal, weights, bias_in, bias_out, scale):
    kept = [
        ((PIX, FF), BF16), ((PIX, FF), BF16), ((PIX, CH), F32), ((CH, FF), BF16), ((FF, CH), BF16),
    ]
    outs = [((PIX, CH), BF16), EDGE, EDGE, *kept]
    far = k == 0
    scratch = [*(pltpu.VMEM(s, d) for s, d in kept), DMA((12,))] if far else [DMA((1,))]
    return call(
        functools.partial(mlp_body, k, far), outs, 12, 60_000_000, scratch, scalars=1,
        grant=14 if far else 5, far_out=range(3, 8) if far else (),
    )(place, a, normal, *weights, bias_in, bias_out, scale)


def backward(k, place, u, saved, gain, scale):
    outs = [
        ((PIX, CH), BF16), ((PIX, FF), BF16), ((SLAB, 128), F32), EDGE, EDGE,
        ((8, CH), F32), ((1, FF), F32),
    ]
    scratch = [pltpu.VMEM((PIX, CH), F32), pltpu.VMEM((2, *EDGE[0]), BF16)]
    return call(
        functools.partial(back_body, k), outs, 10, 60_000_000, scratch, scalars=1
    )(place, u, *saved, gain, scale)


def weight_grads(place, normal, low, act, gh):
    outs = [((CH, FF), BF16), ((CH, FF), BF16)]
    return call(grads_body, outs, 5, 50_000_000, scalars=1)(place, normal, low, act, gh)


def tap_grads(seen, grads):
    return call(taps_body, [((49 * 4, 128), F32)], 2, 40_000_000, [TAPS])(
        seen, grads
    )[0]


def upstream(k, place, slab, edge_near, edge_far, near, far, kernel, u, dtype, later=()):
    scratch = [
        pltpu.VMEM((SLAB, 128), F32), STORE, TAPS,
        pltpu.VMEM((2, *STRIP[0]), BF16), pltpu.VMEM((2, *EDGE[0]), BF16),
        pltpu.VMEM((PIX, CH), u.dtype), DMA((6 + len(later),)),
    ]
    outs = [((PIX, CH), dtype), *((x.shape, x.dtype) for x in later)]
    return call(
        functools.partial(up_body, k, len(later)), outs, 8 + len(later), 40_000_000, scratch,
        grant=8, far=(1, 2, 3, 4, 5, 7, *range(8, 8 + len(later))), scalars=1,
    )(place, slab, edge_near, edge_far, near, far, kernel, u, *later)


def finish(place, side, value, buffers):
    held = [pl.BlockSpec(memory_space=pl.ANY)] * len(buffers)
    return pl.pallas_call(
        finish_body,
        grid_spec=pltpu.PrefetchScalarGridSpec(
            num_scalar_prefetch=1,
            grid=(2, 2),
            in_specs=[pl.BlockSpec((16, 8, FF), lambda layer, i, s: (i, 0, layer)), *held],
            out_specs=[
                pl.BlockSpec((1, 128, HALF), lambda layer, i, s: (layer, i, s[side])),
                pl.BlockSpec((1, HALF, 128), lambda layer, i, s: (layer, s[side], i)),
            ],
        ),
        out_shape=[
            jax.ShapeDtypeStruct((2, 256, FF), F32),
            jax.ShapeDtypeStruct((2, FF, 256), F32),
        ],
        input_output_aliases={2: 0, 3: 1} if buffers else {},
        compiler_params=pltpu.CompilerParams(vmem_limit_bytes=10 * 1024 * 1024),
        cost_estimate=pl.CostEstimate(
            flops=5_000_000, bytes_accessed=6_000_000, transcendentals=0
        ),
    )(place, value, *buffers)


def finish_small(whole, mate):
    first = pl.BlockSpec((32, 8, 128), lambda i: (0, 0, 2 * FF // 128))
    second = pl.BlockSpec((32, 8, 128), lambda i: (0, 0, 2 * FF // 128 + 1))
    shapes = [(7, 7, 2, CH), (5, 2, CH), (2, FF)]
    return pl.pallas_call(
        small_body,
        grid=(1,),
        out_shape=[jax.ShapeDtypeStruct(s, F32) for s in shapes],
        in_specs=[first, second, first, second],
        out_specs=[
            pl.BlockSpec((7, 7, 2, CH), lambda i: (0, 0, 0, 0)),
            pl.BlockSpec((5, 2, CH), lambda i: (0, 0, 0)),
            pl.BlockSpec((2, FF), lambda i: (0, 0)),
        ],
        scratch_shapes=[pltpu.VMEM((256 + 8, 128), F32)],
        compiler_params=pltpu.CompilerParams(vmem_limit_bytes=4 * 1024 * 1024),
        cost_estimate=pl.CostEstimate(
            flops=1_000_000, bytes_accessed=1_000_000, transcendentals=0
        ),
    )(whole, whole, mate, mate)


RANKS = ("xh", "y", "core")


def pairs(first, count):
    found = [(i, i + 1) for i in range(first, count - 1, 2)]
    return found + [(b, a) for a, b in found]


def from_rows(near, far):
    near = lax.ppermute(near, RANKS, pairs(0, 16))
    far = lax.ppermute(far, RANKS, pairs(1, 16))
    return near, far


def from_columns(near, far):
    near = lax.ppermute(near, "z", pairs(0, 4))
    far = lax.ppermute(far, "z", pairs(1, 4))
    return near, far


def swapped(value, axis):
    return lax.ppermute(value, axis, [(0, 1), (1, 0)])


def around_x(value, step):
    return lax.ppermute(value, ("xh", "dp"), [(i, (i + step) % 4) for i in range(4)])


def fetch_weights(core, weight_in, weight_out, k):
    half_in = lax.dynamic_slice(weight_in, (k, core * 128, 0), (1, 128, FF))
    half_out = lax.dynamic_slice(weight_out, (k, core * HALF, 0), (1, HALF, 256))
    got_in = around_x(half_in, 1)
    got_out = around_x(half_out, -1)
    mate_in = swapped(got_in, "core")
    mate_out = swapped(got_out, "core")
    return weight_in, got_in, mate_in, weight_out, got_out, mate_out


def send_grads(keep, got, small):
    count = len(small) // 3
    shape = (64, 8, FF + 128 * count)
    scratch = [
        pltpu.VMEM(shape, BF16), *[pltpu.VMEM((256, 128), F32)] * count, DMA((4,)),
    ]
    pair = call(
        functools.partial(pair_body, count), [(shape, BF16)], 2 + len(small), 2_000_000,
        scratch, far_out=(0,),
    )(keep, got, *small)[0]
    return lax.all_to_all(pair, ("dp", *SPACE), 0, 0, tiled=True)


def per_device(
    slides,
    cotangent,
    kernel,
    kernel_bias,
    norm_gain,
    norm_bias,
    weight_in,
    bias_in,
    weight_out,
    bias_out,
    layer_scale,
):
    core, part = lax.axis_index("core"), lax.axis_index("dp")
    place = jnp.stack([core, part, 1 - core, lax.axis_index("z") % 2]).astype(jnp.int32)
    slides, place = lax.optimization_barrier((slides, place))
    kernel = jnp.transpose(kernel, (1, 2, 0, 3))
    current = slides.reshape(PIX, CH)
    edges = edge_strips(place, current)
    saved = []
    weights = [fetch_weights(core, weight_in, weight_out, k) for k in range(2)]
    for k in range(2):
        edges = from_rows(*edges)
        slab, *sides = pack(place, current, *edges)
        sides = from_columns(*sides)
        slab, normal, normed, rstd = normalise(
            k, place, slab, *sides, kernel, kernel_bias, norm_gain, norm_bias
        )
        current, *edges, act, slope, branch, full_in, full_out = mlp(
            k, place, current, normal, weights[k], bias_in, bias_out, layer_scale
        )
        saved.append((slab, act, normal, (branch, slope, normed, rstd, full_in, full_out)))
    up = cotangent.reshape(PIX, CH)
    pieces = [None] * 2
    small = []
    for k in (1, 0):
        seen, act, normal, rest = saved[k]
        low, gh, grads, *edges, channel, bias = backward(k, place, up, rest, norm_gain, layer_scale)
        edges = from_rows(*edges)
        keep, give = weight_grads(place, normal, low, act, gh)
        got = swapped(give, "core")
        taps = tap_grads(seen, grads)
        small = [taps, channel, bias, *small]
        pieces[k] = send_grads(keep, got, () if k else small)
        sides = pack_edges(place, grads, *edges)
        sides = from_columns(*sides)
        later = saved[0][3] if k else ()
        up, *brought = upstream(
            k, place, grads, *edges, *sides, kernel, up, F32 if k else BF16, later
        )
        if k:
            saved[0] = (*saved[0][:3], brought)
    other = call(total_body, [((8, FF), BF16)], 1, 5_000_000)(pieces[1])[0]
    scratch = [
        pltpu.VMEM((32, 8, FF + WIRE), BF16), pltpu.VMEM((8, WIRE), BF16), DMA((5,)),
    ]
    copies = call(
        merge_body, [((32, 8, FF + WIRE), BF16)], 2, 5_000_000, scratch, grant=8, far_out=(0,)
    )(other, pieces[0])[0]
    whole = lax.all_to_all(copies, SPACE, 0, 0, tiled=True)
    mate = swapped(whole, "core")
    buffers = finish(place, 0, whole, ())
    grad_in, grad_out = finish(place, 2, mate, buffers)
    grad_taps, grad_channel, grad_bias = finish_small(whole, mate)
    return (
        current.reshape(slides.shape),
        up.reshape(slides.shape),
        grad_in,
        grad_out,
        jnp.transpose(grad_taps, (2, 0, 1, 3)),
        jnp.transpose(grad_channel, (1, 0, 2)),
        grad_bias,
    )


def solution(mesh):
    fine = jax.sharding.Mesh(
        mesh.devices.reshape(2, 4, 2, 4, 2), ("xh", "y", "core", "z", "dp")
    )
    maps = P("dp", RANKS, "z", None)
    split_in, split_out = P(None, "dp", None), P(None, None, "dp")
    whole = P()
    return jax.shard_map(
        per_device,
        mesh=fine,
        in_specs=(
            maps, maps, whole, whole, whole, whole, split_in, whole, split_out, whole, whole,
        ),
        out_specs=(maps, maps, split_in, split_out, whole, whole, whole),
        check_vma=False,
    )
```
